256 devices in a mesh: seq: 32 (over y, x, core), head: 8 (over z).
Axes of the slice: x: 4, y: 4, z: 8, core: 2. Of those that a mesh axis runs over, the one named last changes fastest.
Arguments:
- inputs: bfloat16 [8192, 4096], P('seq', 'head'), may hold values from -6 to 6
- gates: bfloat16 [8192, 4096], P('seq', 'head'), may hold values from -6 to 6
- b_proj: bfloat16 [8192, 128], P('seq'), may hold values from -6 to 6
- c_proj: bfloat16 [8192, 128], P('seq'), may hold values from -6 to 6
- step_size: float32 [64, 8192], P('head', 'seq'), may hold values from 0 to 2
- decay_rate: float32 [64], P('head'), may hold values from 0.5 to 2
- norm_gain: float32 [4096], P('head'), may hold values from 0.5 to 1.5
- out_weight: bfloat16 [4096, 4096], P('seq', 'head'), may hold values from -0.09375 to 0.09375
- grad_out: bfloat16 [8192, 4096], P('seq', 'head'), may hold values from -6 to 6
Outputs:
- grad_inputs: bfloat16 [8192, 4096], P('seq', 'head')
- grad_gates: bfloat16 [8192, 4096], P('seq', 'head')
- grad_b: float32 [8192, 128], P('seq')
- grad_c: float32 [8192, 128], P('seq')
- grad_step: float32 [64, 8192], P('head', 'seq')
- grad_rate: float32 [64], P('head')
- grad_gain: float32 [4096], P('head')
- grad_weight: float32 [4096, 4096], P('seq', 'head')
The draws below stay inside these ranges and needn't reach their ends.
All inputs are finite; a program needn't handle non-finite values.
Results may differ from the reference program's by a relative error of at most 0.0042.
Values may be sent and summed in bfloat16 or wider, within the bound.
A program may use at most 64 MiB of HBM per device.

```python
import jax
import jax.numpy as jnp
from jax import lax

D = 4096
HEADS = 64
HEAD_DIM = 64
STATE = 128
TOK_DEV = 256
STREAM_WORDS = 8192
N_SEQ = 32


def rates_and_steps(key):
    stochastic_seeds = jax.random.split(jax.random.fold_in(key, 11), 8)
    rate = jnp.exp(jax.random.uniform(stochastic_seeds[0], (HEADS,), jnp.float32, jnp.log(0.5), jnp.log(2.0)))
    share = 0.5
    quick = jax.random.uniform(stochastic_seeds[1], (HEADS,), jnp.float32) < share
    quick_step = jax.random.uniform(stochastic_seeds[2], (HEADS,), jnp.float32, 1.0 / 50.0, 1.0 / 30.0)
    slow_step = jax.random.uniform(stochastic_seeds[3], (HEADS,), jnp.float32, 0.1, 0.5) / STREAM_WORDS
    single_update_expense = jnp.where(quick, quick_step, slow_step)
    blocks = STREAM_WORDS // TOK_DEV
    tile_factor = jnp.exp(jax.random.uniform(stochastic_seeds[4], (HEADS, blocks), jnp.float32, jnp.log(0.5), jnp.log(2.0)))
    tile_factor = jnp.repeat(tile_factor, TOK_DEV, axis=1)
    approximate_guess = jax.random.uniform(stochastic_seeds[5], (HEADS, STREAM_WORDS), jnp.float32, 0.5, 1.5)
    span_extent = jax.random.uniform(stochastic_seeds[6], (STREAM_WORDS,), jnp.float32) < 3.0 / STREAM_WORDS
    objective_number = jax.random.uniform(stochastic_seeds[7], (HEADS, STREAM_WORDS), jnp.float32, 0.22, 0.69)
    overall_tally = single_update_expense[:, None] * tile_factor * approximate_guess + jnp.where(span_extent[None, :], objective_number, 0.0)
    return (rate, overall_tally / rate[:, None])


def draw_decay_rate(key, part):
    return rates_and_steps(key)[0]


def draw_step_size(key, part):
    return rates_and_steps(key)[1]


def with_spikes(result, key, source, target, blocks, factor):
    owner, partner = [(jnp.arange(result.shape[axis_at]) // (result.shape[axis_at] // blocks)).reshape([-1 if axis == axis_at else 1 for axis in range(result.ndim)]) for axis_at in (source, target)]
    chosen = jax.random.permutation(key, blocks)[partner]
    strong = (owner == chosen) | (owner == (partner + blocks // 2) % blocks)
    return jnp.where(strong, factor * result, result)


def shard_levels(rng, dims, pieces, least, high):
    def one(dim, blocks):
        heights = jax.random.uniform(jax.random.fold_in(jax.random.fold_in(rng, 6), dim), (blocks,), jnp.float32, least / len(pieces), high / len(pieces))
        return jnp.repeat(jnp.exp(heights), dims[dim] // blocks).reshape((-1,) + (1,) * (len(dims) - dim - 1))

    loudness = one(*pieces[0])
    for cut in pieces[1:]:
        loudness = loudness * one(*cut)
    return loudness


def centred(stream_key, extent, deviation, bound, shards=(), held_as=jnp.bfloat16):
    drawn = jax.random.normal(stream_key, extent, jnp.float32) * deviation
    if len(shards) > 0:
        drawn = shard_levels(stream_key, extent, shards, -0.22, 0.18) * drawn
    return jnp.clip(drawn, min=-bound, max=bound).astype(held_as)


def heavy_noise(stream_key, extent, deviation, reach, pieces, heavy, dtype=jnp.bfloat16):
    drawn = deviation * jax.random.normal(stream_key, extent, jnp.float32)
    if pieces:
        drawn = drawn * shard_levels(stream_key, extent, pieces, -0.22, 0.18)
    return jnp.clip(with_spikes(drawn, jax.random.fold_in(stream_key, 3), *heavy), -reach, reach).astype(dtype)


def setup_inputs(seed: int = 0) -> dict:
    key_list = jax.random.split(jax.random.key(seed), 10)
    return {
        "inputs": centred(key_list[0], (STREAM_WORDS, HEADS * HEAD_DIM), 1.0, 6.0, ((0, 32), (1, 8))),
        "gates": centred(key_list[1], (STREAM_WORDS, HEADS * HEAD_DIM), 1.0, 6.0, ((0, 32), (1, 8))),
        "b_proj": centred(key_list[2], (STREAM_WORDS, STATE), 1.0, 6.0, ((0, 32),)),
        "c_proj": centred(key_list[3], (STREAM_WORDS, STATE), 1.0, 6.0, ((0, 32),)),
        "step_size": draw_step_size(jax.random.fold_in(key_list[9], 71), 0),
        "decay_rate": draw_decay_rate(jax.random.fold_in(key_list[9], 71), 0),
        "norm_gain": jnp.clip(1.0 + 0.1 * jax.random.normal(key_list[6], (HEADS * HEAD_DIM,), jnp.float32), 0.5, 1.5),
        "out_weight": centred(key_list[7], (D, HEADS * HEAD_DIM), (HEADS * HEAD_DIM) ** -0.5, 0.09375, ((0, 32), (1, 8))),
        "grad_out": heavy_noise(key_list[8], (STREAM_WORDS, D), 1.0, 6.0, ((0, 32), (1, 8)), (0, 1, 32, 2.75)),
    }


EPSILON = 1e-05

def dot_high(left, right):
    return jnp.dot(left, right, precision=lax.Precision.HIGHEST, preferred_element_type=jnp.float32)

def dot_inner(left, right):
    return lax.dot_general(left, right, (((0,), (0,)), ((), ())), precision=lax.Precision.HIGHEST, preferred_element_type=jnp.float32)

def decay_table(step, rate):
    logs = -jnp.cumsum(rate * step)
    count = step.shape[0]
    later = lax.broadcasted_iota(jnp.int32, (count, count), 0)
    earlier = lax.broadcasted_iota(jnp.int32, (count, count), 1)
    spread = jnp.minimum(logs[:, None] - logs[None, :], 0.0)
    table = jnp.where(later >= earlier, jnp.exp(spread), 0.0)
    return (logs, table)

def span_summary(step, rate, values, keys_b):
    logs = -jnp.cumsum(rate * step)
    tail = jnp.exp(logs[-1] - logs)
    return (jnp.exp(logs[-1]), dot_inner(keys_b * (step * tail)[:, None], values))

def span_output(step, rate, values, keys_b, queries_c, state_in):
    logs, table = decay_table(step, rate)
    scores = dot_high(queries_c, keys_b.T)
    mixing = table * scores * step[None, :]
    return dot_high(mixing, values) + jnp.exp(logs)[:, None] * dot_high(queries_c, state_in)

def adjoint_summary(step, rate, queries_c, grads):
    logs = -jnp.cumsum(rate * step)
    return (jnp.exp(logs[-1]), dot_inner(queries_c * jnp.exp(logs)[:, None], grads))

def span_backward(step, rate, values, keys_b, queries_c, grads, state_in, adjoint_in):
    logs, table = decay_table(step, rate)
    tail = jnp.exp(logs[-1] - logs)
    front = jnp.exp(logs)
    scores = dot_high(queries_c, keys_b.T)
    inner = dot_high(grads, values.T)
    weighted = table * inner
    mixing = table * scores * step[None, :]
    keys_adjoint = dot_high(keys_b, adjoint_in)
    grad_values = dot_inner(mixing, grads) + (step * tail)[:, None] * keys_adjoint
    grad_keys = step[:, None] * (dot_inner(weighted, queries_c) + tail[:, None] * dot_high(values, adjoint_in.T))
    grad_queries = dot_high(weighted * step[None, :], keys_b) + front[:, None] * dot_high(grads, state_in.T)
    carried = tail * lax.optimization_barrier(jnp.sum(keys_adjoint * values, axis=1))
    q_terms = lax.optimization_barrier(jnp.sum(weighted * scores, axis=0)) + carried
    row_part = lax.optimization_barrier(jnp.sum(mixing * inner, axis=1)) + front * lax.optimization_barrier(jnp.sum(dot_high(queries_c, state_in) * grads, axis=1))
    drive = row_part - step * q_terms
    state_end = jnp.exp(logs[-1]) * state_in + dot_inner(keys_b * (step * tail)[:, None], values)
    boundary = jnp.sum(adjoint_in * state_end)
    log_grad = jnp.flip(jnp.cumsum(jnp.flip(drive))) + boundary
    grad_step = q_terms - rate * log_grad
    rate_part = -jnp.sum(step * log_grad)
    return (grad_values, grad_keys, grad_queries, grad_step, rate_part)

def reference(inputs, gates, b_proj, c_proj, step_size, decay_rate, norm_gain, out_weight, grad_out):
    spans = N_SEQ
    length = TOK_DEV
    width = HEADS * HEAD_DIM
    grad_normed = jnp.dot(grad_out, out_weight, preferred_element_type=jnp.float32)
    values = inputs.astype(jnp.float32).reshape(spans, length, HEADS, HEAD_DIM).transpose(0, 2, 1, 3)
    keys_b = b_proj.astype(jnp.float32).reshape(spans, length, STATE)
    queries_c = c_proj.astype(jnp.float32).reshape(spans, length, STATE)
    steps = step_size.reshape(HEADS, spans, length).transpose(1, 0, 2)

    def forward_step(state, items):
        span_values, span_keys, span_queries, span_steps = items
        outputs = jax.vmap(span_output, in_axes=(0, 0, 0, None, None, 0))(span_steps, decay_rate, span_values, span_keys, span_queries, state)
        decays, local = jax.vmap(span_summary, in_axes=(0, 0, 0, None))(span_steps, decay_rate, span_values, span_keys)
        return (decays[:, None, None] * state + local, (outputs, state))
    start = jnp.zeros((HEADS, STATE, HEAD_DIM), jnp.float32)
    _, (outputs, states_in) = lax.scan(forward_step, start, (values, keys_b, queries_c, steps))
    ssd_out = outputs.transpose(0, 2, 1, 3).reshape(STREAM_WORDS, width)
    gate_values = gates.astype(jnp.float32)
    sigmoid_gate = jax.nn.sigmoid(gate_values)
    gated = ssd_out * gate_values * sigmoid_gate
    inv_rms = lax.rsqrt(lax.optimization_barrier(jnp.mean(gated * gated, axis=1)) + EPSILON)
    normed = (gated * inv_rms[:, None] * norm_gain[None, :]).astype(jnp.bfloat16)
    grad_weight = lax.dot_general(grad_out, normed, (((0,), (0,)), ((), ())), preferred_element_type=jnp.float32)
    grad_gain = lax.optimization_barrier(jnp.sum(grad_normed * gated * inv_rms[:, None], axis=0))
    scaled = grad_normed * norm_gain[None, :]
    cross_mean = lax.optimization_barrier(jnp.mean(scaled * gated, axis=1))
    grad_gated = inv_rms[:, None] * (scaled - gated * (inv_rms * inv_rms * cross_mean)[:, None])
    grad_ssd = grad_gated * gate_values * sigmoid_gate
    grad_gates = (grad_gated * ssd_out * sigmoid_gate * (1.0 + gate_values * (1.0 - sigmoid_gate))).astype(jnp.bfloat16)
    grads = grad_ssd.reshape(spans, length, HEADS, HEAD_DIM).transpose(0, 2, 1, 3)

    def backward_step(adjoint, items):
        span_values, span_keys, span_queries, span_steps, span_grads, state_in = items
        parts = jax.vmap(span_backward, in_axes=(0, 0, 0, None, None, 0, 0, 0))(span_steps, decay_rate, span_values, span_keys, span_queries, span_grads, state_in, adjoint)
        decays, local = jax.vmap(adjoint_summary, in_axes=(0, 0, None, 0))(span_steps, decay_rate, span_queries, span_grads)
        return (local + decays[:, None, None] * adjoint, parts)
    _, parts = lax.scan(backward_step, start, (values, keys_b, queries_c, steps, grads, states_in), reverse=True)
    grad_values, grad_keys, grad_queries, grad_steps, rate_parts = parts
    grad_inputs = grad_values.transpose(0, 2, 1, 3).reshape(STREAM_WORDS, width).astype(jnp.bfloat16)
    grad_b = lax.optimization_barrier(jnp.sum(grad_keys, axis=1)).reshape(STREAM_WORDS, STATE)
    grad_c = lax.optimization_barrier(jnp.sum(grad_queries, axis=1)).reshape(STREAM_WORDS, STATE)
    grad_step = grad_steps.transpose(1, 0, 2).reshape(HEADS, STREAM_WORDS)
    grad_rate = lax.optimization_barrier(jnp.sum(rate_parts, axis=0))
    return (grad_inputs, grad_gates, grad_b, grad_c, grad_step, grad_rate, grad_gain, grad_weight)
```

```python
import jax
import jax.numpy as jnp
from jax import lax
from jax.experimental import pallas as pl
from jax.experimental.pallas import tpu as pltpu
from jax.sharding import Mesh
from jax.sharding import PartitionSpec as P

SEQ = ("seq_0", "seq_1", "seq_2")
EPSILON = 1e-05
MESH = pl.DeviceIdType.MESH
BF = jnp.bfloat16
F32 = jnp.float32


def mm(a, b):
    return jnp.dot(a, b, preferred_element_type=F32)


def nt(a, b):
    return lax.dot_general(a, b, (((1,), (1,)), ((), ())), preferred_element_type=F32)


def split2(v):
    hi = v.astype(BF)
    return hi, (v - hi.astype(F32)).astype(BF)


def split3(v):
    hi = v.astype(BF)
    rest = v - hi.astype(F32)
    mid = rest.astype(BF)
    return hi, mid, (rest - mid.astype(F32)).astype(BF)


def lanes(*parts):
    return jnp.concatenate(parts, axis=1)


def rows(*parts):
    return jnp.concatenate(parts, axis=0)


def kernel(
    x_ref, z_ref, b_ref, c_ref, step_ref, rate_ref, gain_ref, w_ref, g_ref,
    gx_ref, gz_ref, gb_ref, gc_ref, gs_ref, gr_ref, gg_ref, gw_ref,
    gfull, wbuf, dec_src, dec_all, st_send, st_recv, st_pref, st_in,
    ad_send, ad_recv, ad_pref, ad_in, stat_src, stat_all,
    pt_own, pt_send, pt_recv, rs_o, rs_p, rs_m, buf_p, buf_m, fin,
    tot, t_o, t_p, t_m, tbuf_p, tbuf_m, tfin,
    cpart, crecv, csum, call_, bpart, brecv, bsum, ball,
    gg_src, gg_all, rt_src, rt_all,
    rate_c, lg, lgt, stept, fr, stl, xs2, sc, sct, mix_t, mix_b, ybuf, ycs, gn,
    nb, ntr, ehi, elo, ef2, rprod, colst, ws, qcol, rowp, gxi, mixw, pprod,
    zs, zr, w1s, w1r, w2s, w2r, wds, wdr, des, der, a1s, a1r, a2s, a2r,
    b1s, b1r, b2s, b2r, sts, str_, d0s, d0r, r1s, r1r, r2s, r2r,
    c1s, c1r, c2s, c2r, k1s, k1r, k2s, k2r, ggs, ggr, rts, rtr,
):
    y = lax.axis_index("seq_0")
    x = lax.axis_index("seq_1")
    c = lax.axis_index("seq_2")
    z = lax.axis_index("head")
    me = (y * 4 + x) * 2 + c
    oc = 1 - c
    q = x * oc + y * c
    p = y * oc + x * c
    group = y * 4 + x

    def at_seq(k):
        return (k // 8, (k // 2) % 4, k % 2, z)

    def at_head(k):
        return (y, x, c, k)

    def first(d):
        return ((y + d * c) % 4, (x + d * oc) % 4, c, z)

    def second(d):
        return ((y + d * oc) % 4, (x + d * c) % 4, c, z)

    partner = (y, x, oc, z)

    def copy(src, dst, ssem, rsem, dev):
        return pltpu.make_async_remote_copy(
            src_ref=src, dst_ref=dst, send_sem=ssem, recv_sem=rsem,
            device_id=dev, device_id_type=MESH,
        )

    def got(ref, sem):
        copy(ref, ref, sem, sem, partner).wait_recv()

    sent = []

    def send(src, dst, ssem, rsem, dev):
        d = copy(src, dst, ssem, rsem, dev)
        d.start()
        sent.append(d)

    def to_seq(make):
        def one(d, carry):
            k = (me + d) % 32
            make(k).start()
            return carry

        lax.fori_loop(1, 32, one, 0)

    def to_head(make):
        for d in range(1, 8):
            make((z + d) % 8).start()

    barrier = pltpu.get_barrier_semaphore()

    def greet(d, carry):
        pl.semaphore_signal(barrier, inc=1, device_id=at_seq((me + d) % 32), device_id_type=MESH)
        return carry

    lax.fori_loop(1, 32, greet, 0)
    for d in range(1, 8):
        pl.semaphore_signal(barrier, inc=1, device_id=at_head((z + d) % 8), device_id_type=MESH)

    i8 = lax.broadcasted_iota(jnp.int32, (8, 8), 0)
    j8 = lax.broadcasted_iota(jnp.int32, (8, 8), 1)
    rate = jnp.sum(jnp.where(i8 == j8, jnp.broadcast_to(rate_ref[...], (8, 8)), 0.0), axis=1, keepdims=True)
    rate_c[...] = jnp.broadcast_to(rate, (8, 128))
    step = step_ref[...]
    ia = lax.broadcasted_iota(jnp.int32, (256, 256), 0)
    ib = lax.broadcasted_iota(jnp.int32, (256, 256), 1)
    tri_u = jnp.where(ia <= ib, 1.0, 0.0).astype(BF)
    v1, v2, v3 = split3(rate * step)
    logs = -(mm(v1, tri_u) + mm(v2, tri_u) + mm(v3, tri_u))
    lg[...] = logs
    logs_t = jnp.transpose(logs)
    step_t = jnp.transpose(step)
    lgt[:, 0:8] = logs_t
    stept[:, 0:8] = step_t
    e8 = jnp.where(
        lax.broadcasted_iota(jnp.int32, (8, 512), 0)
        == lax.broadcasted_iota(jnp.int32, (8, 512), 1) // 64, 1.0, 0.0,
    ).astype(BF)

    def spread_heads(v):
        a1, a2, a3 = split3(v)
        return mm(a1, e8) + mm(a2, e8) + mm(a3, e8)

    fr[...] = spread_heads(jnp.exp(logs_t))
    stl[...] = spread_heads(step_t * jnp.exp(logs_t[255:256, :] - logs_t))
    dec_src[0] = fr[255:256, :]
    dec_all[me] = fr[255:256, :]
    bt = b_ref[...].T
    ct = c_ref[...].T
    for r in range(4):
        rs = slice(64 * r, 64 * r + 64)
        hi, lo = split2(x_ref[rs, :].astype(F32) * stl[rs, :])
        xs2[rs, :] = hi
        xs2[64 * r + 256 : 64 * r + 320, :] = lo
    st_send[...] = mm(lanes(bt, bt), xs2[...])

    pl.semaphore_wait(barrier, 38)

    for k in range(2):
        rk = pl.ds(128 * k, 128)
        for side, d in ((0, 1), (1, 7)):
            send(g_ref.at[rk], gfull.at[z, rk], zs.at[side, 0, k], zr.at[side, 0, k], at_head((z + d) % 8))
    for side, d in ((0, 1), (1, 3)):
        send(w_ref, wbuf.at[c, p, q], w1s.at[side], w1r.at[side], first(d))
    to_seq(lambda k: copy(dec_src.at[0], dec_all.at[me], des, der, at_seq(k)))

    def slab(ref, k):
        return ref.at[
            pl.ds(pl.multiple_of(8 * (k // 2), 8), 8),
            pl.ds(pl.multiple_of(256 * (k % 2), 256), 256),
        ]

    to_seq(lambda k: copy(slab(st_send, k), st_recv.at[me], a1s, a1r, at_seq(k)))
    st_recv[me] = slab(st_send, me)[...]
    gfull[z] = g_ref[...]
    wbuf[c, p, q] = w_ref[...]

    iota_i = lax.broadcasted_iota(jnp.int32, (64, 256), 0)
    iota_j = lax.broadcasted_iota(jnp.int32, (64, 256), 1)
    raw = mm(c_ref[...], bt)
    for r in range(4):
        rs = slice(64 * r, 64 * r + 64)
        sc[rs, :] = jnp.where(iota_i + 64 * r >= iota_j, raw[rs, :], 0.0)
    sct[...] = mm(b_ref[...], ct)

    qm, qp, q2 = (q + 3) % 4, (q + 1) % 4, (q + 2) % 4
    pm, pp, p2 = (p + 3) % 4, (p + 1) % 4, (p + 2) % 4
    got(wbuf.at[c, p, qm], w1r.at[0])
    top = pl.ds(0, 64)
    send(wbuf.at[c, p, qm, top], wbuf.at[c, p, qm, top], w1s.at[2], w1r.at[2], first(1))
    got(wbuf.at[c, p, qp], w1r.at[1])
    low = pl.ds(64, 64)
    send(wbuf.at[c, p, qp, low], wbuf.at[c, p, qp, low], w1s.at[3], w1r.at[3], first(3))

    half = lax.broadcasted_iota(jnp.int32, (1, 128), 1)
    keep = (
        jnp.where(half < 64, 1.0, 0.0).astype(BF),
        jnp.where(half < 64, 0.0, 1.0).astype(BF),
    )

    def inside(hp):
        ls = slice(128 * hp, 128 * hp + 128)
        mt, mb = mix_t.at[hp % 2], mix_b.at[hp % 2]
        xp = x_ref[:, ls]
        x0, x1 = xp * keep[0], xp * keep[1]
        for k in range(2):
            h = 2 * hp + k
            for r in range(4):
                rs = slice(64 * r, 64 * r + 64)
                wd = 128 if r < 2 else 256
                t = jnp.exp(jnp.minimum(lgt[rs, h : h + 1] - lg[h : h + 1, 0:wd], 0.0))
                hi, lo = split2(t * (sc[rs, 0:wd] * step_ref[h : h + 1, 0:wd]))
                dst = mt if r < 2 else mb
                rr = slice(64 * (r % 2), 64 * (r % 2) + 64)
                dst[rr, 2 * k * wd : (2 * k + 1) * wd] = hi
                dst[rr, (2 * k + 1) * wd : (2 * k + 2) * wd] = lo
        ybuf[0:128, ls] = mm(mt[...], rows(x0[0:128], x0[0:128], x1[0:128], x1[0:128]))
        ybuf[128:256, ls] = mm(mb[...], rows(x0, x0, x1, x1))

    def z_block(side, j):
        return (z + 8 - j) % 8 if side == 0 else (z + j) % 8

    def z_forward(j):
        for k in range(2):
            rk = pl.ds(128 * k, 128)
            for side, d in ((0, 1), (1, 7)):
                blk = gfull.at[z_block(side, j), rk]
                got(blk, zr.at[side, j - 1, k])
                if j < 3 or k == side:
                    send(blk, blk, zs.at[side, j, k], zr.at[side, j, k], at_head((z + d) % 8))

    def scan(recv, pref, back):
        s = jnp.zeros((8, 256), F32)
        for k in reversed(range(32)) if back else range(32):
            pref[k] = s
            s = s * dec_all[k, :, pl.ds(pl.multiple_of(256 * c, 256), 256)] + recv[k]

    many = pl.ds(0, 31)

    inside(0)
    inside(1)
    got(dec_all.at[many], der)
    got(st_recv.at[many], a1r)
    scan(st_recv, st_pref, False)
    to_seq(lambda k: copy(st_pref.at[k], slab(st_in, me), a2s, a2r, at_seq(k)))
    slab(st_in, me)[...] = st_pref[me]

    got(wbuf.at[c, p, q2, top], w1r.at[2])
    got(wbuf.at[c, p, q2, low], w1r.at[3])
    mine = wbuf.at[c, p]
    for side, d in ((0, 1), (1, 3)):
        send(mine, mine, w2s.at[side], w2r.at[side], second(d))
    send(mine, mine, wds.at[0], wdr.at[0], partner)
    inside(2)
    z_forward(1)
    inside(3)

    got(st_recv.at[many], a2r)
    s_hi, s_lo = split2(st_in[...])
    cc = lanes(c_ref[...], c_ref[...])
    for r in range(4):
        rs = slice(64 * r, 64 * r + 64)
        v = fr[rs, :] * mm(cc[rs, :], rows(s_hi, s_lo))
        ycs[rs, :] = v
        ybuf[rs, :] = ybuf[rs, :] + v
    z_forward(2)

    ab, cd = pl.ds(0, 2), pl.ds(2, 2)
    got(wbuf.at[c, pm], w2r.at[0])
    send(wbuf.at[c, pm, ab], wbuf.at[c, pm, ab], w2s.at[2], w2r.at[2], second(1))
    send(wbuf.at[c, pm], wbuf.at[c, pm], wds.at[1], wdr.at[1], partner)
    got(wbuf.at[c, pp], w2r.at[1])
    send(wbuf.at[c, pp, cd], wbuf.at[c, pp, cd], w2s.at[3], w2r.at[3], second(3))
    send(wbuf.at[c, pp], wbuf.at[c, pp], wds.at[2], wdr.at[2], partner)
    z_forward(3)
    got(wbuf.at[c, p2, ab], w2r.at[2])
    send(wbuf.at[c, p2, ab], wbuf.at[c, p2, ab], wds.at[3], wdr.at[3], partner)
    got(wbuf.at[c, p2, cd], w2r.at[3])
    send(wbuf.at[c, p2, cd], wbuf.at[c, p2, cd], wds.at[4], wdr.at[4], partner)
    for side in range(2):
        got(gfull.at[z_block(side, 4), pl.ds(128 * side, 128)], zr.at[side, 3, side])
    for n in range(3):
        got(wbuf.at[oc, p], wdr.at[n])
    got(wbuf.at[oc, p, ab], wdr.at[3])
    got(wbuf.at[oc, p, cd], wdr.at[4])

    for r in range(2):
        rs = slice(128 * r, 128 * r + 128)
        acc = None
        for cp in range(2):
            for i2 in range(4):
                parts = []
                for i1 in range(4):
                    yy, xx = (i2, i1) if cp == 0 else (i1, i2)
                    off = (xx % 2) * 256 + cp * 128
                    parts.append(gfull[2 * yy + xx // 2, rs, off : off + 128])
                part = mm(lanes(*parts), wbuf[cp, i2].reshape(512, 512))
                acc = part if acc is None else acc + part
        gn[rs, :] = acc

    gain = gain_ref[...]

    def folded(v):
        return v[:, 0:128] + v[:, 128:256] + v[:, 256:384] + v[:, 384:512]

    for r in range(4):
        rs = slice(64 * r, 64 * r + 64)
        zf = z_ref[rs, :].astype(F32)
        u = ybuf[rs, :] * (zf / (1.0 + jnp.exp(-zf)))
        pprod[rs, 0:128] = folded(u * u)
        pprod[rs, 128:256] = folded(gn[rs, :] * gain * u)
    stat_src[0:1, :] = jnp.sum(jnp.transpose(pprod[:, 0:128]), axis=0, keepdims=True)
    stat_src[1:2, :] = jnp.sum(jnp.transpose(pprod[:, 128:256]), axis=0, keepdims=True)
    stat_all[z] = stat_src[...]
    to_head(lambda k: copy(stat_src, stat_all.at[z], sts, str_, at_head(k)))
    got(stat_all.at[pl.ds(0, 7)], str_)
    stats = jnp.sum(stat_all[...], axis=0)
    inv_row = lax.rsqrt(stats[0:1, :] / 4096.0 + EPSILON)
    coef_row = inv_row * inv_row * (stats[1:2, :] / 4096.0)
    colst[:, 0:8] = jnp.transpose(rows(inv_row, coef_row, jnp.zeros((6, 256), F32)))

    gg_acc = jnp.zeros((8, 512), F32)
    for r in range(8):
        rs = slice(32 * r, 32 * r + 32)
        inv, coef = colst[rs, 0:1], colst[rs, 1:2]
        zf = z_ref[rs, :].astype(F32)
        s = 1.0 / (1.0 + jnp.exp(-zf))
        sil = zf * s
        yv = ybuf[rs, :]
        gnv = gn[rs, :]
        ui = yv * sil * inv
        nb[rs, :] = (ui * gain).astype(BF)
        gg_acc = gg_acc + jnp.sum((gnv * ui).reshape(4, 8, 512), axis=0)
        gu = inv * (gnv * gain - yv * sil * coef)
        e = gu * sil
        gz_ref[rs, :] = (gu * yv * s * (1.0 + zf * (1.0 - s))).astype(BF)
        hi, lo = split2(e)
        ehi[rs, :] = hi
        elo[rs, :] = lo
        hi, lo = split2(e * fr[rs, :])
        ef2[rs, :] = hi
        ef2[256 + 32 * r : 288 + 32 * r, :] = lo
        hi, lo = split2(e * ycs[rs, :])
        rprod[rs, 0:512] = hi
        rprod[rs, 512:1024] = lo
    ad_send[...] = mm(lanes(ct, ct), ef2[...])
    to_seq(lambda k: copy(slab(ad_send, k), ad_recv.at[me], b1s, b1r, at_seq(k)))
    ad_recv[me] = slab(ad_send, me)[...]
    gg_src[0] = jnp.sum(gg_acc, axis=0, keepdims=True)
    gg_all[me] = gg_src[0]
    to_seq(lambda k: copy(gg_src.at[0], gg_all.at[me], ggs, ggr, at_seq(k)))

    ntr[...] = nb[...].T

    def one_chip(i, carry):
        yy, xx = i // 4, i % 4
        blk = 2 * yy + xx // 2
        base = (xx % 2) * 256
        left = gfull[blk, :, pl.ds(pl.multiple_of(base + 128 * c, 128), 128)]
        right = gfull[blk, :, pl.ds(pl.multiple_of(base + 128 * oc, 128), 128)]
        both = mm(ntr[...], lanes(left, right))
        own1, own2 = xx * oc + yy * c, yy * oc + xx * c
        pt_own[own2, own1] = both[:, 0:128]
        pt_send[own1, own2] = both[:, 128:256].astype(BF)
        return carry

    lax.fori_loop(0, 16, one_chip, 0)
    order = (2, 1, 3, 0)
    for n in range(4):
        i2 = (q + order[n]) % 4
        send(pt_send.at[i2], pt_recv.at[i2], d0s.at[n], d0r.at[n], partner)

    mask_t = (iota_j >= iota_i, iota_j >= iota_i + 64)
    mask_b = (iota_j[:, 0:128] >= iota_i[:, 0:128], iota_j[:, 0:128] >= iota_i[:, 0:128] + 64)

    def inside_back(hp):
        ls = slice(128 * hp, 128 * hp + 128)
        mw = mixw.at[hp % 2]
        xp = x_ref[:, ls]
        eh, el = ehi[:, ls], elo[:, ls]
        e2 = lanes(eh, el)
        for k in range(2):
            h = 2 * hp + k
            xk = xp * keep[k]
            x2 = lanes(xk, xk)
            inner_t = nt(x2[0:128], e2)
            inner_b = nt(x2[128:256], e2[128:256])
            racc_l = jnp.zeros((1, 128), F32)
            racc_r = jnp.zeros((1, 128), F32)
            for r in range(4):
                rs = slice(64 * r, 64 * r + 64)
                rr = slice(64 * (r % 2), 64 * (r % 2) + 64)
                cs = slice(0, 256) if r < 2 else slice(128, 256)
                t = jnp.exp(jnp.minimum(lg[h : h + 1, cs] - lgt[rs, h : h + 1], 0.0))
                tab = jnp.where(mask_t[r] if r < 2 else mask_b[r - 2], t, 0.0)
                inner = inner_t[rr] if r < 2 else inner_b[rr]
                st = sct[rs, cs]
                sj = stept[rs, h : h + 1]
                w = tab * inner
                sw = w * sj
                if r < 2:
                    mw[rr, 256 * k : 256 * k + 256] = (tab * st * sj).astype(BF)
                else:
                    mw[128 + 64 * (r - 2) : 192 + 64 * (r - 2), 128 * k : 128 * k + 128] = (tab * st * sj).astype(BF)
                qcol[rs, h : h + 1] = jnp.sum(w * st, axis=1, keepdims=True)
                if h == 0:
                    ws[rs, cs] = sw
                else:
                    ws[rs, cs] = ws[rs, cs] + sw
                rsum = jnp.sum(sw * st, axis=0, keepdims=True)
                if r < 2:
                    racc_l = racc_l + rsum[:, 0:128]
                    racc_r = racc_r + rsum[:, 128:256]
                else:
                    racc_r = racc_r + rsum
            rowp[h : h + 1, 0:128] = racc_l
            rowp[h : h + 1, 128:256] = racc_r
        em0, em1 = lanes(eh * keep[0], el * keep[0]), lanes(eh * keep[1], el * keep[1])
        v = mm(mw[0:128, :], rows(em0, em1))
        gxi[0:128, ls] = v[:, 0:128] + v[:, 128:256]
        v = mm(mw[128:256, 0:256], rows(em0[128:256], em1[128:256]))
        gxi[128:256, ls] = v[:, 0:128] + v[:, 128:256]

    inside_back(0)
    got(pt_recv.at[p2], d0r.at[0])
    for i in range(4):
        rs_o[i] = (pt_own[p2, i] + pt_recv[p2, i].astype(F32)).astype(BF)
    send(rs_o.at[ab], buf_p, r1s.at[0], r1r.at[0], second(1))
    send(rs_o.at[cd], buf_m, r1s.at[1], r1r.at[1], second(3))
    inside_back(1)
    inside_back(2)
    inside_back(3)

    got(ad_recv.at[many], b1r)
    scan(ad_recv, ad_pref, True)
    to_seq(lambda k: copy(ad_pref.at[k], slab(ad_in, me), b2s, b2r, at_seq(k)))
    slab(ad_in, me)[...] = ad_pref[me]

    got(pt_recv.at[pp], d0r.at[1])
    for i in range(4):
        v = pt_own[pp, i] + pt_recv[pp, i].astype(F32)
        if i < 2:
            pt_own[pp, i] = v
        else:
            rs_p[i] = v.astype(BF)
    send(rs_p.at[cd], fin.at[0, cd], r1s.at[2], r1r.at[2], second(1))
    got(pt_recv.at[pm], d0r.at[2])
    for i in range(4):
        v = pt_own[pm, i] + pt_recv[pm, i].astype(F32)
        if i < 2:
            rs_m[i] = v.astype(BF)
        else:
            pt_own[pm, i] = v
    send(rs_m.at[ab], fin.at[1, ab], r1s.at[3], r1r.at[3], second(3))

    ws[128:256, 0:128] = jnp.zeros((128, 128), F32)
    w_hi, w_lo = split2(jnp.transpose(ws[...]))
    gq = mm(lanes(w_hi, w_lo), rows(b_ref[...], b_ref[...]))
    gq = gq + nt(lanes(ef2[0:256], ef2[256:512], ef2[0:256]), lanes(s_hi, s_hi, s_lo))
    for k in range(8):
        cpart[k] = gq[32 * k : 32 * k + 32]
    crecv[z] = cpart[z]
    to_head(lambda k: copy(cpart.at[k], crecv.at[z], c1s, c1r, at_head(k)))
    w_hi, w_lo = split2(ws[...])
    gk = mm(lanes(w_hi, w_lo), rows(c_ref[...], c_ref[...]))

    got(pt_recv.at[p], d0r.at[3])
    for i in range(4):
        pt_own[p, i] = pt_own[p, i] + pt_recv[p, i].astype(F32)

    got(buf_p, r1r.at[0])
    for i in range(2):
        rs_p[i] = (pt_own[pp, i] + buf_p[i].astype(F32)).astype(BF)
    send(rs_p.at[ab], fin.at[0, ab], r2s.at[0], r2r.at[0], second(1))
    got(buf_m, r1r.at[1])
    for i in range(2):
        rs_m[2 + i] = (pt_own[pm, 2 + i] + buf_m[i].astype(F32)).astype(BF)
    send(rs_m.at[cd], fin.at[1, cd], r2s.at[1], r2r.at[1], second(3))

    got(ad_recv.at[many], b2r)
    a_hi, a_lo = split2(ad_in[...])
    gk = gk + nt(lanes(xs2[0:256], xs2[256:512], xs2[0:256]), lanes(a_hi, a_hi, a_lo))
    for k in range(8):
        bpart[k] = gk[32 * k : 32 * k + 32]
    brecv[z] = bpart[z]
    to_head(lambda k: copy(bpart.at[k], brecv.at[z], k1s, k1r, at_head(k)))
    got(crecv.at[pl.ds(0, 7)], c1r)
    csum[...] = jnp.sum(crecv[...], axis=0)
    call_[z] = csum[...]
    to_head(lambda k: copy(csum, call_.at[z], c2s, c2r, at_head(k)))

    bb = lanes(b_ref[...], b_ref[...])
    for r in range(4):
        rs = slice(64 * r, 64 * r + 64)
        ka = mm(bb[rs, :], rows(a_hi, a_lo))
        gx_ref[rs, :] = (gxi[rs, :] + stl[rs, :] * ka).astype(BF)
        hi, lo = split2(x_ref[rs, :].astype(F32) * ka)
        pprod[rs, 0:512] = hi.astype(F32)
        pprod[rs, 512:1024] = lo.astype(F32)
    e16 = lanes(e8, e8)
    carr = nt(e16, pprod[...].astype(BF))
    rstate = nt(e16, rprod[...])
    held = jnp.sum((ad_in[...] * st_in[...]).reshape(16, 8, 512), axis=0)
    h_hi, h_lo = split2(held)
    held8 = jnp.sum(nt(e16, lanes(h_hi, h_lo)), axis=1, keepdims=True)
    logs = lg[...]
    step = step_ref[...]
    rate = rate_c[:, 0:1]
    tail = jnp.exp(logs[:, 255:256] - logs)
    q_in = jnp.transpose(qcol[...])[0:8, :]
    tc = tail * carr
    q_terms = q_in + tc
    drive = rowp[...] + rstate - step * q_terms
    boundary = jnp.exp(logs[:, 255:256]) * held8 + jnp.sum(step * tc, axis=1, keepdims=True)
    tri_l = jnp.where(ia >= ib, 1.0, 0.0).astype(BF)
    v1, v2, v3 = split3(drive)
    log_grad = mm(v1, tri_l) + mm(v2, tri_l) + mm(v3, tri_l) + boundary
    gs_ref[...] = q_terms - rate * log_grad
    rp = -jnp.sum(step * log_grad, axis=1, keepdims=True)
    d0 = lax.broadcasted_iota(jnp.int32, (8, 128), 0)
    d1 = lax.broadcasted_iota(jnp.int32, (8, 128), 1)
    rt_src[0] = jnp.sum(jnp.where(d0 == d1, rp, 0.0), axis=0, keepdims=True)
    rt_all[me] = rt_src[0]
    to_seq(lambda k: copy(rt_src.at[0], rt_all.at[me], rts, rtr, at_seq(k)))

    got(fin.at[0, cd], r1r.at[2])
    got(fin.at[1, ab], r1r.at[3])
    got(fin.at[0, ab], r2r.at[0])
    got(fin.at[1, cd], r2r.at[1])

    def total(i):
        return pt_own[p, i] + fin[0, i].astype(F32) + fin[1, i].astype(F32)

    hi_rows, lo_rows = pl.ds(0, 256), pl.ds(256, 256)
    t_o[...] = total(q2).astype(BF)
    send(t_o.at[hi_rows], tbuf_p, r1s.at[4], r1r.at[4], first(1))
    send(t_o.at[lo_rows], tbuf_m, r1s.at[5], r1r.at[5], first(3))
    v = total(qp)
    tot[0] = v[0:256]
    t_p[256:512, :] = v[256:512].astype(BF)
    send(t_p.at[lo_rows], tfin.at[0, lo_rows], r1s.at[6], r1r.at[6], first(1))
    v = total(qm)
    tot[1] = v[256:512]
    t_m[0:256, :] = v[0:256].astype(BF)
    send(t_m.at[hi_rows], tfin.at[1, hi_rows], r1s.at[7], r1r.at[7], first(3))

    got(brecv.at[pl.ds(0, 7)], k1r)
    bsum[...] = jnp.sum(brecv[...], axis=0)
    ball[z] = bsum[...]
    to_head(lambda k: copy(bsum, ball.at[z], k2s, k2r, at_head(k)))

    mine_w = total(q)
    got(tbuf_p, r1r.at[4])
    t_p[0:256, :] = (tot[0] + tbuf_p[...].astype(F32)).astype(BF)
    send(t_p.at[hi_rows], tfin.at[0, hi_rows], r2s.at[2], r2r.at[2], first(1))
    got(tbuf_m, r1r.at[5])
    t_m[256:512, :] = (tot[1] + tbuf_m[...].astype(F32)).astype(BF)
    send(t_m.at[lo_rows], tfin.at[1, lo_rows], r2s.at[3], r2r.at[3], first(3))

    got(gg_all.at[many], ggr)
    gg_ref[...] = jnp.sum(gg_all[...], axis=0)
    got(call_.at[pl.ds(0, 7)], c2r)
    for k in range(8):
        gc_ref[32 * k : 32 * k + 32, :] = call_[k]
    got(rt_all.at[many], rtr)
    gr_ref[...] = jnp.sum(rt_all[...], axis=0)[:, 0:8]

    got(tfin.at[0, lo_rows], r1r.at[6])
    got(tfin.at[1, hi_rows], r1r.at[7])
    got(tfin.at[0, hi_rows], r2r.at[2])
    got(tfin.at[1, lo_rows], r2r.at[3])
    gw_ref[...] = jnp.transpose(mine_w + tfin[0].astype(F32) + tfin[1].astype(F32))
    got(ball.at[pl.ds(0, 7)], k2r)
    for k in range(8):
        gb_ref[32 * k : 32 * k + 32, :] = ball[k]

    def left(ref, sem):
        copy(ref, ref, sem, sem, partner).wait_send()

    for d in sent:
        d.wait_send()
    for ref, sem in (
        (dec_all, des), (st_recv, a1s), (st_recv, a2s), (ad_recv, b1s), (ad_recv, b2s),
        (gg_all, ggs), (rt_all, rts),
    ):
        left(ref.at[many], sem)
    for ref, sem in ((stat_all, sts), (crecv, c1s), (call_, c2s), (brecv, k1s), (ball, k2s)):
        left(ref.at[pl.ds(0, 7)], sem)


def on_device(
    inputs, gates, b_proj, c_proj, step_size, decay_rate, norm_gain, out_weight, grad_out
):
    V = pltpu.VMEM
    dma = pltpu.SemaphoreType.DMA
    scratch = [
        V((8, 256, 512), BF), V((2, 4, 4, 128, 512), BF),
        V((1, 1, 512), F32), V((32, 1, 512), F32),
        V((128, 512), F32), V((32, 8, 256), F32), V((32, 8, 256), F32), V((128, 512), F32),
        V((128, 512), F32), V((32, 8, 256), F32), V((32, 8, 256), F32), V((128, 512), F32),
        V((2, 256), F32), V((8, 2, 256), F32),
        V((4, 4, 512, 128), F32), V((4, 4, 512, 128), BF), V((4, 4, 512, 128), BF),
        V((4, 512, 128), BF), V((4, 512, 128), BF), V((4, 512, 128), BF),
        V((2, 512, 128), BF), V((2, 512, 128), BF), V((2, 4, 512, 128), BF),
        V((2, 256, 128), F32), V((512, 128), BF), V((512, 128), BF), V((512, 128), BF),
        V((256, 128), BF), V((256, 128), BF), V((2, 512, 128), BF),
        V((8, 32, 128), F32), V((8, 32, 128), F32), V((32, 128), F32), V((8, 32, 128), F32),
        V((8, 32, 128), F32), V((8, 32, 128), F32), V((32, 128), F32), V((8, 32, 128), F32),
        V((1, 1, 512), F32), V((32, 1, 512), F32), V((1, 1, 128), F32), V((32, 1, 128), F32),
        V((8, 128), F32), V((8, 256), F32), V((256, 128), F32), V((256, 128), F32),
        V((256, 512), F32), V((256, 512), F32), V((512, 512), BF),
        V((256, 256), F32), V((256, 256), F32),
        V((2, 128, 512), BF), V((2, 128, 1024), BF),
        V((256, 512), F32), V((256, 512), F32), V((256, 512), F32),
        V((256, 512), BF), V((512, 256), BF),
        V((256, 512), BF), V((256, 512), BF), V((512, 512), BF), V((256, 1024), BF),
        V((256, 128), F32), V((256, 256), F32), V((256, 128), F32), V((8, 256), F32),
        V((256, 512), F32), V((2, 256, 512), BF), V((256, 1024), F32),
        dma((2, 4, 2)), dma((2, 4, 2)), dma((4,)), dma((4,)), dma((4,)), dma((4,)),
        dma((5,)), dma((5,)),
        dma, dma, dma, dma, dma, dma, dma, dma, dma, dma, dma, dma,
        dma((4,)), dma((4,)), dma((8,)), dma((8,)), dma((4,)), dma((4,)),
        dma, dma, dma, dma, dma, dma, dma, dma, dma, dma, dma, dma,
    ]
    outs = (
        jax.ShapeDtypeStruct((256, 512), BF),
        jax.ShapeDtypeStruct((256, 512), BF),
        jax.ShapeDtypeStruct((256, 128), F32),
        jax.ShapeDtypeStruct((256, 128), F32),
        jax.ShapeDtypeStruct((8, 256), F32),
        jax.ShapeDtypeStruct((1, 8), F32),
        jax.ShapeDtypeStruct((1, 512), F32),
        jax.ShapeDtypeStruct((128, 512), F32),
    )
    spec = pl.BlockSpec(memory_space=pltpu.VMEM)
    gx, gz, gb, gc, gs, gr, gg, gw = pl.pallas_call(
        kernel,
        out_shape=outs,
        in_specs=[spec] * 9,
        out_specs=[spec] * 8,
        scratch_shapes=scratch,
        compiler_params=pltpu.CompilerParams(
            collective_id=0, has_side_effects=True, vmem_limit_bytes=60 * 1024 * 1024
        ),
    )(
        inputs, gates, b_proj, c_proj, step_size, decay_rate.reshape(1, 8),
        norm_gain.reshape(1, 512), out_weight, grad_out,
    )
    return gx, gz, gb, gc, gs, gr.reshape(8), gg.reshape(512), gw


def solution(mesh):
    split = Mesh(
        mesh.devices.reshape(4, 4, 2, mesh.shape["head"]), ("seq_0", "seq_1", "seq_2", "head")
    )
    return jax.shard_map(
        on_device,
        mesh=split,
        in_specs=(
            P(SEQ, "head"), P(SEQ, "head"), P(SEQ, None), P(SEQ, None), P("head", SEQ),
            P("head"), P("head"), P(SEQ, "head"), P(SEQ, "head"),
        ),
        out_specs=(
            P(SEQ, "head"), P(SEQ, "head"), P(SEQ, None), P(SEQ, None), P("head", SEQ),
            P("head"), P("head"), P(SEQ, "head"),
        ),
        check_vma=False,
    )
```

```python
import jax
import jax.numpy as jnp
from jax import lax
from jax.experimental import pallas as pl
from jax.experimental.pallas import tpu as pltpu
from jax.sharding import Mesh
from jax.sharding import PartitionSpec as P

SEQ = ("seq_0", "seq_1", "seq_2")
EPSILON = 1e-05
MESH = pl.DeviceIdType.MESH
BF = jnp.bfloat16
F32 = jnp.float32


def mm(a, b):
    return jnp.dot(a, b, preferred_element_type=F32)


def nt(a, b):
    return lax.dot_general(a, b, (((1,), (1,)), ((), ())), preferred_element_type=F32)


def split2(v):
    hi = v.astype(BF)
    return hi, (v - hi.astype(F32)).astype(BF)


def split3(v):
    hi = v.astype(BF)
    rest = v - hi.astype(F32)
    mid = rest.astype(BF)
    return hi, mid, (rest - mid.astype(F32)).astype(BF)


def lanes(*parts):
    return jnp.concatenate(parts, axis=1)


def rows(*parts):
    return jnp.concatenate(parts, axis=0)


ORDER = (2, 1, 3, 0)


def kernel(
    x_hbm, z_hbm, b_hbm, c_hbm, step_hbm, rate_hbm, gain_hbm, w_hbm, g_hbm,
    gx_hbm, gz_hbm, gb_hbm, gc_hbm, gs_hbm, gr_hbm, gg_hbm, gw_hbm,
    gx_ref, gz_ref, gb_ref, gc_ref, gs_ref, gr_ref, gg_ref, gw_ref, outs,
    x_ref, z_ref, b_ref, c_ref, step_ref, rate_ref, gain_ref, w_ref, g_ref,
    gfull, wbuf, dec_src, dec_all, st_send, st_recv, st_pref, st_in,
    ad_send, ad_recv, ad_pref, ad_in, sq_src, sq_all, cr_src, cr_all,
    pt_own, pt_send, pt_recv, rs_o, rs_p, rs_m, buf_p, buf_m, fin,
    tot, t_o, t_p, t_m, tbuf_p, tbuf_m, tfin,
    cpart, crecv, csum, call_, bpart, brecv, bsum, ball,
    gg_src, gg_all, rt_src, rt_all,
    rate_c, lg, lgt, stept, fr, stl, xs2, sc, sct, mix_t, mix_b, ybuf, ycs, gn,
    ubuf, silb, ydb, nb, ntr, ehi, elo, ef2, rprod, colst, ws, qcol, rowp, gxi, mixw, pprod,
    ins, zs, zr, w1s, w1r, w2s, w2r, wfs, wfr, wds, wdr, des, der, a1s, a1r, a2s, a2r,
    b1s, b1r, b2s, b2r, sqs, sqr, crs, crr, d0s, d0r, r1s, r1r, r2s, r2r,
    c1s, c1r, c2s, c2r, k1s, k1r, k2s, k2r, ggs, ggr, rts, rtr,
):
    y = lax.axis_index("seq_0")
    x = lax.axis_index("seq_1")
    c = lax.axis_index("seq_2")
    z = lax.axis_index("head")
    me = (y * 4 + x) * 2 + c
    oc = 1 - c
    q = x * oc + y * c
    p = y * oc + x * c
    rem, div = lax.rem, lax.div

    def at_seq(k):
        return (div(k, 8), rem(div(k, 2), 4), rem(k, 2), z)

    def at_head(k):
        return (y, x, c, k)

    def first(d):
        return (rem(y + d * c, 4), rem(x + d * oc, 4), c, z)

    def second(d):
        return (rem(y + d * oc, 4), rem(x + d * c, 4), c, z)

    partner = (y, x, oc, z)

    def copy(src, dst, ssem, rsem, dev):
        return pltpu.make_async_remote_copy(
            src_ref=src, dst_ref=dst, send_sem=ssem, recv_sem=rsem,
            device_id=dev, device_id_type=MESH,
        )

    def got(ref, sem):
        copy(ref, ref, sem, sem, partner).wait_recv()

    sent, stored = [], []

    def store(src, dst):
        one = pltpu.make_async_copy(src, dst, outs.at[len(stored)])
        one.start()
        stored.append(one)

    def send(src, dst, ssem, rsem, dev):
        d = copy(src, dst, ssem, rsem, dev)
        d.start()
        sent.append(d)

    def to_seq(make):
        def one(d, carry):
            make(rem(me + d, 32)).start()
            return carry

        lax.fori_loop(1, 32, one, 0)

    def to_head(make):
        for d in (4, 3, 5, 2, 6, 1, 7):
            make(rem(z + d, 8)).start()

    barrier = pltpu.get_barrier_semaphore()
    for d in (4, 3, 5, 2, 6, 1, 7):
        pl.semaphore_signal(barrier, inc=1, device_id=at_head(rem(z + d, 8)), device_id_type=MESH)

    def greet(d, carry):
        pl.semaphore_signal(barrier, inc=1, device_id=at_seq(rem(me + d, 32)), device_id_type=MESH)
        return carry

    lax.fori_loop(1, 32, greet, 0)
    fetches = [
        pltpu.make_async_copy(src, dst, ins.at[i])
        for i, (src, dst) in enumerate((
            (step_hbm, step_ref), (rate_hbm, rate_ref), (gain_hbm, gain_ref), (b_hbm, b_ref),
            (x_hbm, x_ref), (c_hbm, c_ref), (g_hbm, g_ref), (w_hbm, w_ref), (z_hbm, z_ref),
        ))
    ]
    for f in fetches:
        f.start()
    for f in fetches[:4]:
        f.wait()

    i8 = lax.broadcasted_iota(jnp.int32, (8, 8), 0)
    j8 = lax.broadcasted_iota(jnp.int32, (8, 8), 1)
    rate = jnp.sum(jnp.where(i8 == j8, jnp.broadcast_to(rate_ref[...], (8, 8)), 0.0), axis=1, keepdims=True)
    rate_c[...] = jnp.broadcast_to(rate, (8, 128))
    step = step_ref[...]
    ia = lax.broadcasted_iota(jnp.int32, (256, 256), 0)
    ib = lax.broadcasted_iota(jnp.int32, (256, 256), 1)
    tri_u = jnp.where(ia <= ib, 1.0, 0.0).astype(BF)
    v1, v2, v3 = split3(rate * step)
    logs = -(mm(v1, tri_u) + mm(v2, tri_u) + mm(v3, tri_u))
    lg[...] = logs
    logs_t = jnp.transpose(logs)
    step_t = jnp.transpose(step)
    lgt[:, 0:8] = logs_t
    stept[:, 0:8] = step_t
    e8 = jnp.where(
        lax.broadcasted_iota(jnp.int32, (8, 512), 0)
        == lax.broadcasted_iota(jnp.int32, (8, 512), 1) // 64, 1.0, 0.0,
    ).astype(BF)

    def spread_heads(v):
        a1, a2, a3 = split3(v)
        return mm(a1, e8) + mm(a2, e8) + mm(a3, e8)

    fr[...] = spread_heads(jnp.exp(logs_t))
    stl[...] = spread_heads(step_t * jnp.exp(logs_t[255:256, :] - logs_t))
    dec_src[0] = fr[255:256, :]
    dec_all[me] = fr[255:256, :]
    bt = b_ref[...].T
    fetches[4].wait()
    for r in range(4):
        rs = slice(64 * r, 64 * r + 64)
        hi, lo = split2(x_ref[rs, :].astype(F32) * stl[rs, :])
        xs2[rs, :] = hi
        xs2[64 * r + 256 : 64 * r + 320, :] = lo
    st_send[...] = mm(lanes(bt, bt), xs2[...])
    for f in fetches[5:]:
        f.wait()

    pl.semaphore_wait(barrier, 38)

    qm, qp, q2 = rem(q + 3, 4), rem(q + 1, 4), rem(q + 2, 4)
    pm, pp, p2 = rem(p + 3, 4), rem(p + 1, 4), rem(p + 2, 4)
    top, low = pl.ds(0, 64), pl.ds(64, 64)
    both_z, both_4 = ((0, 1), (1, 7)), ((0, 1), (1, 3))
    for k in range(2):
        rk = pl.ds(128 * k, 128)
        for side, d in both_z:
            send(g_ref.at[rk], gfull.at[z, rk], zs.at[side, 0, k], zr.at[side, 0, k], at_head(rem(z + d, 8)))
    for side, d in both_4:
        send(w_ref, wbuf.at[c, p, q], w1s.at[side], w1r.at[side], first(d))
    to_seq(lambda k: copy(dec_src.at[0], dec_all.at[me], des, der, at_seq(k)))

    def slab(ref, k):
        return ref.at[
            pl.ds(pl.multiple_of(8 * div(k, 2), 8), 8),
            pl.ds(pl.multiple_of(256 * rem(k, 2), 256), 256),
        ]

    to_seq(lambda k: copy(slab(st_send, k), st_recv.at[me], a1s, a1r, at_seq(k)))
    for side, d in both_4:
        send(w_ref, wbuf.at[c, p, q], w2s.at[side, 0], w2r.at[side, 0], second(d))
    st_recv[me] = slab(st_send, me)[...]
    gfull[z] = g_ref[...]
    wbuf[c, p, q] = w_ref[...]

    iota_i = lax.broadcasted_iota(jnp.int32, (64, 256), 0)
    iota_j = lax.broadcasted_iota(jnp.int32, (64, 256), 1)
    ct = c_ref[...].T
    raw = mm(c_ref[...], bt)
    for r in range(4):
        rs = slice(64 * r, 64 * r + 64)
        sc[rs, :] = jnp.where(iota_i + 64 * r >= iota_j, raw[rs, :], 0.0)
    sct[...] = mm(b_ref[...], ct)

    got(wbuf.at[c, p, qm], w1r.at[0])
    send(wbuf.at[c, p, qm, top], wbuf.at[c, p, qm, top], w1s.at[2], w1r.at[2], first(1))
    for side, d in both_4:
        send(wbuf.at[c, p, qm], wbuf.at[c, p, qm], w2s.at[side, 1], w2r.at[side, 1], second(d))
    got(wbuf.at[c, p, qp], w1r.at[1])
    send(wbuf.at[c, p, qp, low], wbuf.at[c, p, qp, low], w1s.at[3], w1r.at[3], first(3))
    for side, d in both_4:
        send(wbuf.at[c, p, qp], wbuf.at[c, p, qp], w2s.at[side, 2], w2r.at[side, 2], second(d))

    half = lax.broadcasted_iota(jnp.int32, (1, 128), 1)
    keep = (
        jnp.where(half < 64, 1.0, 0.0).astype(BF),
        jnp.where(half < 64, 0.0, 1.0).astype(BF),
    )

    def inside(hp):
        ls = slice(128 * hp, 128 * hp + 128)
        mt, mb = mix_t.at[hp % 2], mix_b.at[hp % 2]
        xp = x_ref[:, ls]
        x0, x1 = xp * keep[0], xp * keep[1]
        for k in range(2):
            h = 2 * hp + k
            for r in range(4):
                rs = slice(64 * r, 64 * r + 64)
                wd = 128 if r < 2 else 256
                t = jnp.exp(jnp.minimum(lgt[rs, h : h + 1] - lg[h : h + 1, 0:wd], 0.0))
                hi, lo = split2(t * (sc[rs, 0:wd] * step_ref[h : h + 1, 0:wd]))
                dst = mt if r < 2 else mb
                rr = slice(64 * (r % 2), 64 * (r % 2) + 64)
                dst[rr, 2 * k * wd : (2 * k + 1) * wd] = hi
                dst[rr, (2 * k + 1) * wd : (2 * k + 2) * wd] = lo
        ybuf[0:128, ls] = mm(mt[...], rows(x0[0:128], x0[0:128], x1[0:128], x1[0:128]))
        ybuf[128:256, ls] = mm(mb[...], rows(x0, x0, x1, x1))

    def z_block(side, j):
        return rem(z + 8 - j, 8) if side == 0 else rem(z + j, 8)

    def z_forward(j):
        for k in range(2):
            rk = pl.ds(128 * k, 128)
            for side, d in both_z:
                blk = gfull.at[z_block(side, j), rk]
                got(blk, zr.at[side, j - 1, k])
                if j < 3 or k == side:
                    send(blk, blk, zs.at[side, j, k], zr.at[side, j, k], at_head(rem(z + d, 8)))

    spots = (q, qm, qp, q2, q2)

    def w_forward(slot):
        for side, row in ((0, pm), (1, pp)):
            if slot < 3:
                blk = wbuf.at[c, row, spots[slot]]
                part = blk.at[top if side == 0 else low]
                on = True
            else:
                blk = part = wbuf.at[c, row, q2, top if slot == 3 else low]
                on = slot == 3 + side
            got(blk, w2r.at[side, slot])
            if on:
                n = min(slot, 3)
                send(part, part, wfs.at[side, n], wfr.at[side, n], second(1 if side == 0 else 3))

    def w_second_of_opposite():
        for n, piece in ((0, top), (1, low)):
            blk = wbuf.at[c, p, q2, piece]
            got(blk, w1r.at[2 + n])
            for side, d in both_4:
                send(blk, blk, w2s.at[side, 3 + n], w2r.at[side, 3 + n], second(d))

    def to_partner(n, i2):
        send(wbuf.at[c, i2], wbuf.at[c, i2], wds.at[n], wdr.at[n], partner)

    def scan(recv, pref, back):
        s = jnp.zeros((8, 256), F32)
        for k in reversed(range(32)) if back else range(32):
            pref[k] = s
            s = s * dec_all[k, :, pl.ds(pl.multiple_of(256 * c, 256), 256)] + recv[k]

    many = pl.ds(0, 31)

    inside(0)
    w_forward(0)
    w_second_of_opposite()
    to_partner(0, p)
    inside(1)
    z_forward(1)
    got(dec_all.at[many], der)
    got(st_recv.at[many], a1r)
    scan(st_recv, st_pref, False)
    to_seq(lambda k: copy(st_pref.at[k], slab(st_in, me), a2s, a2r, at_seq(k)))
    slab(st_in, me)[...] = st_pref[me]
    w_forward(1)
    w_forward(2)
    inside(2)
    inside(3)
    w_forward(3)
    w_forward(4)
    to_partner(1, pm)
    to_partner(2, pp)
    z_forward(2)

    got(st_recv.at[many], a2r)
    s_hi, s_lo = split2(st_in[...])
    cc = lanes(c_ref[...], c_ref[...])
    gain = gain_ref[...]

    def folded(v):
        return v[:, 0:128] + v[:, 128:256] + v[:, 256:384] + v[:, 384:512]

    for r in range(4):
        rs = slice(64 * r, 64 * r + 64)
        v = fr[rs, :] * mm(cc[rs, :], rows(s_hi, s_lo))
        ycs[rs, :] = v
        ybuf[rs, :] = ybuf[rs, :] + v
    for r in range(8):
        rs = slice(32 * r, 32 * r + 32)
        zf = z_ref[rs, :].astype(F32)
        yv = ybuf[rs, :]
        s = 1.0 / (1.0 + jnp.exp(-zf))
        sil = zf * s
        u = yv * sil
        ubuf[rs, :] = u
        silb[rs, :] = sil
        ydb[rs, :] = yv * s * (1.0 + zf * (1.0 - s))
        pprod[rs, 0:128] = folded(u * u)
    sq = jnp.sum(jnp.transpose(pprod[:, 0:128]), axis=0, keepdims=True)
    sq_src[0] = sq
    sq_all[z] = sq
    to_head(lambda k: copy(sq_src.at[0], sq_all.at[z], sqs, sqr, at_head(k)))

    for n in range(4):
        i1 = (q, qm, qp, q2)[n]
        got(wbuf.at[c, p2, i1, top], wfr.at[0, n])
        got(wbuf.at[c, p2, i1, low], wfr.at[1, n])
    to_partner(3, p2)
    z_forward(3)
    for n in range(4):
        got(wbuf.at[oc, p], wdr.at[n])

    gn[...] = jnp.zeros((256, 512), F32)

    def add_block(h):
        yy, xx = div(h, 2), 2 * rem(h, 2)
        rhs = rows(wbuf[0, yy, xx], wbuf[1, xx, yy], wbuf[0, yy, xx + 1], wbuf[1, xx + 1, yy])
        gn[...] = gn[...] + mm(gfull[h], rhs)

    def one_block(d, carry):
        add_block(rem(z + 5 + d, 8))
        return carry

    lax.fori_loop(0, 7, one_block, 0)
    for side in range(2):
        got(gfull.at[z_block(side, 4), pl.ds(128 * side, 128)], zr.at[side, 3, side])
    add_block(rem(z + 4, 8))
    for r in range(8):
        rs = slice(32 * r, 32 * r + 32)
        pprod[rs, 128:256] = folded(gn[rs, :] * gain * ubuf[rs, :])
    cr = jnp.sum(jnp.transpose(pprod[:, 128:256]), axis=0, keepdims=True)
    cr_src[0] = cr
    cr_all[z] = cr
    to_head(lambda k: copy(cr_src.at[0], cr_all.at[z], crs, crr, at_head(k)))

    seven = pl.ds(0, 7)
    got(sq_all.at[seven], sqr)
    inv_row = lax.rsqrt(jnp.sum(sq_all[...], axis=0) / 4096.0 + EPSILON)
    zero7 = jnp.zeros((7, 256), F32)
    colst[:, 0:8] = jnp.transpose(rows(inv_row, zero7))
    gg_acc = jnp.zeros((8, 512), F32)
    for r in range(8):
        rs = slice(32 * r, 32 * r + 32)
        ui = ubuf[rs, :] * colst[rs, 0:1]
        nb[rs, :] = (ui * gain).astype(BF)
        gg_acc = gg_acc + jnp.sum((gn[rs, :] * ui).reshape(4, 8, 512), axis=0)
    ntr[...] = nb[...].T

    for n in range(4):
        i2 = rem(q + ORDER[n], 4)

        def one_chip(i1, carry, i2=i2):
            yy, xx = i2 * c + i1 * oc, i1 * c + i2 * oc
            blk = 2 * yy + div(xx, 2)
            base = rem(xx, 2) * 256
            mine = gfull[blk, :, pl.ds(pl.multiple_of(base + 128 * c, 128), 128)]
            other = gfull[blk, :, pl.ds(pl.multiple_of(base + 128 * oc, 128), 128)]
            both = mm(ntr[...], lanes(mine, other))
            pt_own[yy * oc + xx * c, xx * oc + yy * c] = both[:, 0:128]
            pt_send[i2, i1] = both[:, 128:256].astype(BF)
            return carry

        lax.fori_loop(0, 4, one_chip, 0)
        send(pt_send.at[i2], pt_recv.at[i2], d0s.at[n], d0r.at[n], partner)

    gg_src[0] = jnp.sum(gg_acc, axis=0, keepdims=True)
    gg_all[me] = gg_src[0]
    ab, cd = pl.ds(0, 2), pl.ds(2, 2)
    got(pt_recv.at[p2], d0r.at[0])
    for i in range(4):
        rs_o[i] = (pt_own[p2, i] + pt_recv[p2, i].astype(F32)).astype(BF)
    send(rs_o.at[ab], buf_p, r1s.at[0], r1r.at[0], second(1))
    send(rs_o.at[cd], buf_m, r1s.at[1], r1r.at[1], second(3))

    got(cr_all.at[seven], crr)
    coef_row = inv_row * inv_row * (jnp.sum(cr_all[...], axis=0) / 4096.0)
    colst[:, 8:16] = jnp.transpose(rows(coef_row, zero7))
    for r in range(8):
        rs = slice(32 * r, 32 * r + 32)
        gu = colst[rs, 0:1] * (gn[rs, :] * gain - ubuf[rs, :] * colst[rs, 8:9])
        gz_ref[rs, :] = (gu * ydb[rs, :]).astype(BF)
        e = gu * silb[rs, :]
        hi, lo = split2(e)
        ehi[rs, :] = hi
        elo[rs, :] = lo
        hi, lo = split2(e * fr[rs, :])
        ef2[rs, :] = hi
        ef2[256 + 32 * r : 288 + 32 * r, :] = lo
        hi, lo = split2(e * ycs[rs, :])
        rprod[rs, 0:512] = hi
        rprod[rs, 512:1024] = lo
    ad_send[...] = mm(lanes(ct, ct), ef2[...])
    to_seq(lambda k: copy(slab(ad_send, k), ad_recv.at[me], b1s, b1r, at_seq(k)))
    ad_recv[me] = slab(ad_send, me)[...]
    store(gz_ref, gz_hbm)
    to_seq(lambda k: copy(gg_src.at[0], gg_all.at[me], ggs, ggr, at_seq(k)))

    got(pt_recv.at[pp], d0r.at[1])
    for i in range(4):
        v = pt_own[pp, i] + pt_recv[pp, i].astype(F32)
        if i < 2:
            pt_own[pp, i] = v
        else:
            rs_p[i] = v.astype(BF)
    send(rs_p.at[cd], fin.at[0, cd], r1s.at[2], r1r.at[2], second(1))
    got(pt_recv.at[pm], d0r.at[2])
    for i in range(4):
        v = pt_own[pm, i] + pt_recv[pm, i].astype(F32)
        if i < 2:
            rs_m[i] = v.astype(BF)
        else:
            pt_own[pm, i] = v
    send(rs_m.at[ab], fin.at[1, ab], r1s.at[3], r1r.at[3], second(3))

    mask_t = (iota_j >= iota_i, iota_j >= iota_i + 64)
    mask_b = (iota_j[:, 0:128] >= iota_i[:, 0:128], iota_j[:, 0:128] >= iota_i[:, 0:128] + 64)

    def inside_back(hp):
        ls = slice(128 * hp, 128 * hp + 128)
        mw = mixw.at[hp % 2]
        xp = x_ref[:, ls]
        eh, el = ehi[:, ls], elo[:, ls]
        e2 = lanes(eh, el)
        for k in range(2):
            h = 2 * hp + k
            xk = xp * keep[k]
            x2 = lanes(xk, xk)
            inner_t = nt(x2[0:128], e2)
            inner_b = nt(x2[128:256], e2[128:256])
            racc_l = jnp.zeros((1, 128), F32)
            racc_r = jnp.zeros((1, 128), F32)
            for r in range(4):
                rs = slice(64 * r, 64 * r + 64)
                rr = slice(64 * (r % 2), 64 * (r % 2) + 64)
                cs = slice(0, 256) if r < 2 else slice(128, 256)
                t = jnp.exp(jnp.minimum(lg[h : h + 1, cs] - lgt[rs, h : h + 1], 0.0))
                tab = jnp.where(mask_t[r] if r < 2 else mask_b[r - 2], t, 0.0)
                inner = inner_t[rr] if r < 2 else inner_b[rr]
                st = sct[rs, cs]
                sj = stept[rs, h : h + 1]
                w = tab * inner
                sw = w * sj
                if r < 2:
                    mw[rr, 256 * k : 256 * k + 256] = (tab * st * sj).astype(BF)
                else:
                    mw[128 + 64 * (r - 2) : 192 + 64 * (r - 2), 128 * k : 128 * k + 128] = (tab * st * sj).astype(BF)
                qcol[rs, h : h + 1] = jnp.sum(w * st, axis=1, keepdims=True)
                if h == 0:
                    ws[rs, cs] = sw
                else:
                    ws[rs, cs] = ws[rs, cs] + sw
                rsum = jnp.sum(sw * st, axis=0, keepdims=True)
                if r < 2:
                    racc_l = racc_l + rsum[:, 0:128]
                    racc_r = racc_r + rsum[:, 128:256]
                else:
                    racc_r = racc_r + rsum
            rowp[h : h + 1, 0:128] = racc_l
            rowp[h : h + 1, 128:256] = racc_r
        em0, em1 = lanes(eh * keep[0], el * keep[0]), lanes(eh * keep[1], el * keep[1])
        v = mm(mw[0:128, :], rows(em0, em1))
        gxi[0:128, ls] = v[:, 0:128] + v[:, 128:256]
        v = mm(mw[128:256, 0:256], rows(em0[128:256], em1[128:256]))
        gxi[128:256, ls] = v[:, 0:128] + v[:, 128:256]

    for hp in range(4):
        inside_back(hp)

    got(ad_recv.at[many], b1r)
    scan(ad_recv, ad_pref, True)
    to_seq(lambda k: copy(ad_pref.at[k], slab(ad_in, me), b2s, b2r, at_seq(k)))
    slab(ad_in, me)[...] = ad_pref[me]

    got(buf_p, r1r.at[0])
    for i in range(2):
        rs_p[i] = (pt_own[pp, i] + buf_p[i].astype(F32)).astype(BF)
    send(rs_p.at[ab], fin.at[0, ab], r2s.at[0], r2r.at[0], second(1))
    got(buf_m, r1r.at[1])
    for i in range(2):
        rs_m[2 + i] = (pt_own[pm, 2 + i] + buf_m[i].astype(F32)).astype(BF)
    send(rs_m.at[cd], fin.at[1, cd], r2s.at[1], r2r.at[1], second(3))

    ws[128:256, 0:128] = jnp.zeros((128, 128), F32)
    w_hi, w_lo = split2(jnp.transpose(ws[...]))
    gq = mm(lanes(w_hi, w_lo), rows(b_ref[...], b_ref[...]))
    gq = gq + nt(lanes(ef2[0:256], ef2[256:512], ef2[0:256]), lanes(s_hi, s_hi, s_lo))
    for k in range(8):
        cpart[k] = gq[32 * k : 32 * k + 32]
    crecv[z] = cpart[z]
    to_head(lambda k: copy(cpart.at[k], crecv.at[z], c1s, c1r, at_head(k)))
    w_hi, w_lo = split2(ws[...])
    gk = mm(lanes(w_hi, w_lo), rows(c_ref[...], c_ref[...]))

    got(pt_recv.at[p], d0r.at[3])
    for i in range(4):
        pt_own[p, i] = pt_own[p, i] + pt_recv[p, i].astype(F32)
    e16 = lanes(e8, e8)
    rstate = nt(e16, rprod[...])

    got(ad_recv.at[many], b2r)
    a_hi, a_lo = split2(ad_in[...])
    gk = gk + nt(lanes(xs2[0:256], xs2[256:512], xs2[0:256]), lanes(a_hi, a_hi, a_lo))
    for k in range(8):
        bpart[k] = gk[32 * k : 32 * k + 32].astype(BF)
    brecv[z] = bpart[z]
    to_head(lambda k: copy(bpart.at[k], brecv.at[z], k1s, k1r, at_head(k)))
    got(crecv.at[seven], c1r)
    csum[...] = jnp.sum(crecv[...], axis=0)
    call_[z] = csum[...]
    to_head(lambda k: copy(csum, call_.at[z], c2s, c2r, at_head(k)))

    for r in range(4):
        rs = slice(64 * r, 64 * r + 64)
        ka = mm(lanes(b_ref[rs, :], b_ref[rs, :]), rows(a_hi, a_lo))
        gx_ref[rs, :] = (gxi[rs, :] + stl[rs, :] * ka).astype(BF)
        hi, lo = split2(x_ref[rs, :].astype(F32) * ka)
        pprod[rs, 0:512] = hi.astype(F32)
        pprod[rs, 512:1024] = lo.astype(F32)
    carr = nt(e16, pprod[...].astype(BF))
    store(gx_ref, gx_hbm)
    held = jnp.sum((ad_in[...] * st_in[...]).reshape(16, 8, 512), axis=0)
    h_hi, h_lo = split2(held)
    held8 = jnp.sum(nt(e16, lanes(h_hi, h_lo)), axis=1, keepdims=True)
    logs = lg[...]
    step = step_ref[...]
    rate = rate_c[:, 0:1]
    tail = jnp.exp(logs[:, 255:256] - logs)
    q_in = jnp.transpose(qcol[...])[0:8, :]
    tc = tail * carr
    q_terms = q_in + tc
    drive = rowp[...] + rstate - step * q_terms
    boundary = jnp.exp(logs[:, 255:256]) * held8 + jnp.sum(step * tc, axis=1, keepdims=True)
    tri_l = jnp.where(ia >= ib, 1.0, 0.0).astype(BF)
    v1, v2, v3 = split3(drive)
    log_grad = mm(v1, tri_l) + mm(v2, tri_l) + mm(v3, tri_l) + boundary
    gs_ref[...] = q_terms - rate * log_grad
    rp = -jnp.sum(step * log_grad, axis=1, keepdims=True)
    d0 = lax.broadcasted_iota(jnp.int32, (8, 128), 0)
    d1 = lax.broadcasted_iota(jnp.int32, (8, 128), 1)
    rt_src[0] = jnp.sum(jnp.where(d0 == d1, rp, 0.0), axis=0, keepdims=True)
    rt_all[me] = rt_src[0]
    to_seq(lambda k: copy(rt_src.at[0], rt_all.at[me], rts, rtr, at_seq(k)))
    store(gs_ref, gs_hbm)

    got(fin.at[0, cd], r1r.at[2])
    got(fin.at[1, ab], r1r.at[3])
    got(fin.at[0, ab], r2r.at[0])
    got(fin.at[1, cd], r2r.at[1])

    def total(i):
        return pt_own[p, i] + fin[0, i].astype(F32) + fin[1, i].astype(F32)

    hi_rows, lo_rows = pl.ds(0, 256), pl.ds(256, 256)
    t_o[...] = total(q2).astype(BF)
    send(t_o.at[hi_rows], tbuf_p, r1s.at[4], r1r.at[4], first(1))
    send(t_o.at[lo_rows], tbuf_m, r1s.at[5], r1r.at[5], first(3))
    v = total(qp)
    tot[0] = v[0:256]
    t_p[256:512, :] = v[256:512].astype(BF)
    send(t_p.at[lo_rows], tfin.at[0, lo_rows], r1s.at[6], r1r.at[6], first(1))
    v = total(qm)
    tot[1] = v[256:512]
    t_m[0:256, :] = v[0:256].astype(BF)
    send(t_m.at[hi_rows], tfin.at[1, hi_rows], r1s.at[7], r1r.at[7], first(3))

    got(brecv.at[seven], k1r)
    bsum[...] = jnp.sum(brecv[...].astype(F32), axis=0).astype(BF)
    ball[z] = bsum[...]
    to_head(lambda k: copy(bsum, ball.at[z], k2s, k2r, at_head(k)))

    mine_w = total(q)
    got(tbuf_p, r1r.at[4])
    t_p[0:256, :] = (tot[0] + tbuf_p[...].astype(F32)).astype(BF)
    send(t_p.at[hi_rows], tfin.at[0, hi_rows], r2s.at[2], r2r.at[2], first(1))
    got(tbuf_m, r1r.at[5])
    t_m[256:512, :] = (tot[1] + tbuf_m[...].astype(F32)).astype(BF)
    send(t_m.at[lo_rows], tfin.at[1, lo_rows], r2s.at[3], r2r.at[3], first(3))

    got(gg_all.at[many], ggr)
    gg_ref[...] = jnp.sum(gg_all[...], axis=0)
    store(gg_ref, gg_hbm)
    got(call_.at[seven], c2r)
    for k in range(8):
        gc_ref[32 * k : 32 * k + 32, :] = call_[k]
    store(gc_ref, gc_hbm)
    got(rt_all.at[many], rtr)
    gr_ref[...] = jnp.sum(rt_all[...], axis=0)[:, 0:8]
    store(gr_ref, gr_hbm)

    got(tfin.at[0, lo_rows], r1r.at[6])
    got(tfin.at[1, hi_rows], r1r.at[7])
    got(tfin.at[0, hi_rows], r2r.at[2])
    got(tfin.at[1, lo_rows], r2r.at[3])
    gw_ref[...] = jnp.transpose(mine_w + tfin[0].astype(F32) + tfin[1].astype(F32))
    store(gw_ref, gw_hbm)
    got(ball.at[seven], k2r)
    for k in range(8):
        gb_ref[32 * k : 32 * k + 32, :] = ball[k].astype(F32)
    store(gb_ref, gb_hbm)

    def left(ref, sem):
        copy(ref, ref, sem, sem, partner).wait_send()

    for d in sent:
        d.wait_send()
    for d in stored:
        d.wait()
    for ref, sem in (
        (dec_all, des), (st_recv, a1s), (st_recv, a2s), (ad_recv, b1s), (ad_recv, b2s),
        (gg_all, ggs), (rt_all, rts),
    ):
        left(ref.at[many], sem)
    for ref, sem in ((sq_all, sqs), (cr_all, crs), (crecv, c1s), (call_, c2s), (brecv, k1s), (ball, k2s)):
        left(ref.at[seven], sem)


def hand_over(*refs):
    took = [pltpu.make_async_copy(refs[i], refs[16 + i], refs[24].at[i]) for i in range(8)]
    gave = [pltpu.make_async_copy(refs[16 + i], refs[8 + i], refs[24].at[8 + i]) for i in range(8)]
    for one in took:
        one.start()
    for one, other in zip(took, gave):
        one.wait()
        other.start()
    for one in gave:
        one.wait()


def on_device(
    inputs, gates, b_proj, c_proj, step_size, decay_rate, norm_gain, out_weight, grad_out
):
    V = pltpu.VMEM
    dma = pltpu.SemaphoreType.DMA
    scratch = [
        V((256, 512), BF), V((256, 512), BF), V((256, 128), F32), V((256, 128), F32),
        V((8, 256), F32), V((1, 8), F32), V((1, 512), F32), V((128, 512), F32), dma((8,)),
        V((256, 512), BF), V((256, 512), BF), V((256, 128), BF), V((256, 128), BF),
        V((8, 256), F32), V((1, 8), F32), V((1, 512), F32), V((128, 512), BF), V((256, 512), BF),
        V((8, 256, 512), BF), V((2, 4, 4, 128, 512), BF),
        V((1, 1, 512), F32), V((32, 1, 512), F32),
        V((128, 512), F32), V((32, 8, 256), F32), V((32, 8, 256), F32), V((128, 512), F32),
        V((128, 512), F32), V((32, 8, 256), F32), V((32, 8, 256), F32), V((128, 512), F32),
        V((1, 1, 256), F32), V((8, 1, 256), F32), V((1, 1, 256), F32), V((8, 1, 256), F32),
        V((4, 4, 512, 128), F32), V((4, 4, 512, 128), BF), V((4, 4, 512, 128), BF),
        V((4, 512, 128), BF), V((4, 512, 128), BF), V((4, 512, 128), BF),
        V((2, 512, 128), BF), V((2, 512, 128), BF), V((2, 4, 512, 128), BF),
        V((2, 256, 128), F32), V((512, 128), BF), V((512, 128), BF), V((512, 128), BF),
        V((256, 128), BF), V((256, 128), BF), V((2, 512, 128), BF),
        V((8, 32, 128), F32), V((8, 32, 128), F32), V((32, 128), F32), V((8, 32, 128), F32),
        V((8, 32, 128), BF), V((8, 32, 128), BF), V((32, 128), BF), V((8, 32, 128), BF),
        V((1, 1, 512), F32), V((32, 1, 512), F32), V((1, 1, 128), F32), V((32, 1, 128), F32),
        V((8, 128), F32), V((8, 256), F32), V((256, 128), F32), V((256, 128), F32),
        V((256, 512), F32), V((256, 512), F32), V((512, 512), BF),
        V((256, 256), F32), V((256, 256), F32),
        V((2, 128, 512), BF), V((2, 128, 1024), BF),
        V((256, 512), F32), V((256, 512), F32), V((256, 512), F32),
        V((256, 512), F32), V((256, 512), F32), V((256, 512), F32),
        V((256, 512), BF), V((512, 256), BF),
        V((256, 512), BF), V((256, 512), BF), V((512, 512), BF), V((256, 1024), BF),
        V((256, 128), F32), V((256, 256), F32), V((256, 128), F32), V((8, 256), F32),
        V((256, 512), F32), V((2, 256, 512), BF), V((256, 1024), F32),
        dma((9,)), dma((2, 4, 2)), dma((2, 4, 2)), dma((4,)), dma((4,)), dma((2, 5)), dma((2, 5)),
        dma((2, 4)), dma((2, 4)), dma((4,)), dma((4,)),
        dma, dma, dma, dma, dma, dma, dma, dma, dma, dma, dma, dma, dma, dma,
        dma((4,)), dma((4,)), dma((8,)), dma((8,)), dma((4,)), dma((4,)),
        dma, dma, dma, dma, dma, dma, dma, dma, dma, dma, dma, dma,
    ]
    outs = (
        jax.ShapeDtypeStruct((256, 512), BF),
        jax.ShapeDtypeStruct((256, 512), BF),
        jax.ShapeDtypeStruct((256, 128), F32),
        jax.ShapeDtypeStruct((256, 128), F32),
        jax.ShapeDtypeStruct((8, 256), F32),
        jax.ShapeDtypeStruct((1, 8), F32),
        jax.ShapeDtypeStruct((1, 512), F32),
        jax.ShapeDtypeStruct((128, 512), F32),
    )
    far = pl.BlockSpec(memory_space=pltpu.HBM)
    results = pl.pallas_call(
        kernel,
        out_shape=outs,
        in_specs=[far] * 9,
        out_specs=[far] * 8,
        scratch_shapes=scratch,
        compiler_params=pltpu.CompilerParams(
            collective_id=0, has_side_effects=True, vmem_limit_bytes=60000000
        ),
    )(
        inputs, gates, b_proj, c_proj, step_size, decay_rate.reshape(1, 8),
        norm_gain.reshape(1, 512), out_weight, grad_out,
    )
    gx, gz, gb, gc, gs, gr, gg, gw = pl.pallas_call(
        hand_over,
        out_shape=outs,
        in_specs=[far] * 8,
        out_specs=[far] * 8,
        scratch_shapes=[V(o.shape, o.dtype) for o in outs] + [dma((16,))],
        compiler_params=pltpu.CompilerParams(vmem_limit_bytes=60000000),
    )(*results)
    return gx, gz, gb, gc, gs, gr.reshape(8), gg.reshape(512), gw


def solution(mesh):
    split = Mesh(
        mesh.devices.reshape(4, 4, 2, mesh.shape["head"]), ("seq_0", "seq_1", "seq_2", "head")
    )
    return jax.shard_map(
        on_device,
        mesh=split,
        in_specs=(
            P(SEQ, "head"), P(SEQ, "head"), P(SEQ, None), P(SEQ, None), P("head", SEQ),
            P("head"), P("head"), P(SEQ, "head"), P(SEQ, "head"),
        ),
        out_specs=(
            P(SEQ, "head"), P(SEQ, "head"), P(SEQ, None), P(SEQ, None), P("head", SEQ),
            P("head"), P("head"), P(SEQ, "head"),
        ),
        check_vma=False,
    )
```

```python
import jax
import jax.numpy as jnp
from jax import lax
from jax.experimental import pallas as pl
from jax.experimental.pallas import tpu as pltpu
from jax.sharding import Mesh
from jax.sharding import PartitionSpec as P

SEQ = ("seq_0", "seq_1", "seq_2")
EPSILON = 1e-05
MESH = pl.DeviceIdType.MESH
BF = jnp.bfloat16
F32 = jnp.float32


def mm(a, b):
    return jnp.dot(a, b, preferred_element_type=F32)


def nt(a, b):
    return lax.dot_general(a, b, (((1,), (1,)), ((), ())), preferred_element_type=F32)


def split2(v):
    hi = v.astype(BF)
    return hi, (v - hi.astype(F32)).astype(BF)


def split3(v):
    hi = v.astype(BF)
    rest = v - hi.astype(F32)
    mid = rest.astype(BF)
    return hi, mid, (rest - mid.astype(F32)).astype(BF)


def lanes(*parts):
    return jnp.concatenate(parts, axis=1)


def rows(*parts):
    return jnp.concatenate(parts, axis=0)


ORDER = (2, 1, 3, 0)


def kernel(
    x_hbm, z_hbm, b_hbm, c_hbm, step_hbm, rate_hbm, gain_hbm, w_hbm, g_hbm,
    gx_hbm, gz_hbm, gb_hbm, gc_hbm, gs_hbm, gr_hbm, gg_hbm, gw_hbm,
    gx_ref, gz_ref, gb_ref, gc_ref, gs_ref, gr_ref, gg_ref, gw_ref, outs,
    x_ref, z_ref, b_ref, c_ref, step_ref, rate_ref, gain_ref, w_ref, g_ref,
    gfull, wbuf, dec_src, dec_all, dec_par, st_send, st_recv, st_pref, st_in,
    st_other, st_pair, st_half, st_give,
    ad_send, ad_recv, ad_pref, ad_in, ad_other, ad_pair, ad_half, ad_give, sq_src, sq_all, cr_src, cr_all,
    pt_own, pt_send, pt_recv, rs_o, rs_p, rs_m, buf_p, buf_m, fin,
    tot, t_o, t_p, t_m, tbuf_p, tbuf_m, tfin,
    cpart, crecv, csum, call_, bpart, brecv, bsum, ball,
    gg_src, gg_all, rt_src, rt_all,
    rate_c, lg, lgt, stept, fr, stl, xs2, sc, sct, mix_t, mix_b, ybuf, ycs, gn,
    ubuf, silb, ydb, nb, ntr, ehi, elo, ef2, rprod, colst, ws, qcol, rowp, gxi, mixw, pprod,
    ins, prs, prr, zs, zr, w1s, w1r, w2s, w2r, wfs, wfr, wds, wdr, des, der, a1s, a1r, a2s, a2r,
    b1s, b1r, b2s, b2r, sqs, sqr, crs, crr, d0s, d0r, r1s, r1r, r2s, r2r,
    c1s, c1r, c2s, c2r, k1s, k1r, k2s, k2r, ggs, ggr, rts, rtr,
):
    y = lax.axis_index("seq_0")
    x = lax.axis_index("seq_1")
    c = lax.axis_index("seq_2")
    z = lax.axis_index("head")
    me = (y * 4 + x) * 2 + c
    oc = 1 - c
    q = x * oc + y * c
    p = y * oc + x * c
    rem, div = lax.rem, lax.div

    def at_head(k):
        return (y, x, c, k)

    def first(d):
        return (rem(y + d * c, 4), rem(x + d * oc, 4), c, z)

    def second(d):
        return (rem(y + d * oc, 4), rem(x + d * c, 4), c, z)

    partner = (y, x, oc, z)

    def copy(src, dst, ssem, rsem, dev):
        return pltpu.make_async_remote_copy(
            src_ref=src, dst_ref=dst, send_sem=ssem, recv_sem=rsem,
            device_id=dev, device_id_type=MESH,
        )

    def got(ref, sem):
        copy(ref, ref, sem, sem, partner).wait_recv()

    sent, stored = [], []

    def store(src, dst):
        one = pltpu.make_async_copy(src, dst, outs.at[len(stored)])
        one.start()
        stored.append(one)

    def send(src, dst, ssem, rsem, dev):
        d = copy(src, dst, ssem, rsem, dev)
        d.start()
        sent.append(d)

    far_first = sorted(
        ((dy, dx, dc) for dy in range(4) for dx in range(4) for dc in range(2)),
        key=lambda o: -(min(o[0], 4 - o[0]) + min(o[1], 4 - o[1])) - 0.1 * o[2],
    )
    ys, xs, cs = [rem(y + d, 4) for d in range(4)], [rem(x + d, 4) for d in range(4)], (c, oc)
    peers = [
        ((ys[dy], xs[dx], cs[dc], z), (ys[dy] * 4 + xs[dx]) * 2 + cs[dc])
        for dy, dx, dc in far_first
        if (dy, dx, dc) != (0, 0, 0)
    ]

    chips = [
        ((ys[dy], xs[dx], c, z), ys[dy] * 4 + xs[dx])
        for dy, dx, dc in far_first
        if dc == 0 and (dy, dx) != (0, 0)
    ]
    here = y * 4 + x

    def to_chips(make):
        for dev, k in chips:
            make(dev, k).start()

    def to_seq(make):
        for dev, k in peers:
            make(dev, k).start()

    def to_head(make):
        for d in (4, 3, 5, 2, 6, 1, 7):
            make(rem(z + d, 8)).start()

    barrier = pltpu.get_barrier_semaphore()
    fetches = [
        pltpu.make_async_copy(src, dst, ins.at[i])
        for i, (src, dst) in enumerate((
            (step_hbm, step_ref), (rate_hbm, rate_ref), (gain_hbm, gain_ref), (b_hbm, b_ref),
            (x_hbm, x_ref), (c_hbm, c_ref), (g_hbm, g_ref), (w_hbm, w_ref), (z_hbm, z_ref),
        ))
    ]
    for f in fetches:
        f.start()
    for d in (4, 3, 5, 2, 6, 1, 7):
        pl.semaphore_signal(barrier, inc=1, device_id=at_head(rem(z + d, 8)), device_id_type=MESH)
    for dev, _ in peers:
        pl.semaphore_signal(barrier, inc=1, device_id=dev, device_id_type=MESH)
    for f in fetches[:4]:
        f.wait()

    i8 = lax.broadcasted_iota(jnp.int32, (8, 8), 0)
    j8 = lax.broadcasted_iota(jnp.int32, (8, 8), 1)
    rate = jnp.sum(jnp.where(i8 == j8, jnp.broadcast_to(rate_ref[...], (8, 8)), 0.0), axis=1, keepdims=True)
    rate_c[...] = jnp.broadcast_to(rate, (8, 128))
    step = step_ref[...]
    ia = lax.broadcasted_iota(jnp.int32, (256, 256), 0)
    ib = lax.broadcasted_iota(jnp.int32, (256, 256), 1)
    tri_u = jnp.where(ia <= ib, 1.0, 0.0).astype(BF)
    v1, v2, v3 = split3(rate * step)
    logs = -(mm(v1, tri_u) + mm(v2, tri_u) + mm(v3, tri_u))
    lg[...] = logs
    logs_t = jnp.transpose(logs)
    step_t = jnp.transpose(step)
    lgt[:, 0:8] = logs_t
    stept[:, 0:8] = step_t
    e8 = jnp.where(
        lax.broadcasted_iota(jnp.int32, (8, 512), 0)
        == lax.broadcasted_iota(jnp.int32, (8, 512), 1) // 64, 1.0, 0.0,
    ).astype(BF)

    def spread_heads(v):
        a1, a2, a3 = split3(v)
        return mm(a1, e8) + mm(a2, e8) + mm(a3, e8)

    fr[...] = spread_heads(jnp.exp(logs_t))
    stl[...] = spread_heads(step_t * jnp.exp(logs_t[255:256, :] - logs_t))
    dec_src[0] = fr[255:256, :]
    dec_all[me] = fr[255:256, :]
    bt = b_ref[...].T
    fetches[4].wait()
    for r in range(4):
        rs = slice(64 * r, 64 * r + 64)
        hi, lo = split2(x_ref[rs, :].astype(F32) * stl[rs, :])
        xs2[rs, :] = hi
        xs2[64 * r + 256 : 64 * r + 320, :] = lo
    st_send[...] = mm(lanes(bt, bt), xs2[...])
    for f in fetches[5:]:
        f.wait()

    pl.semaphore_wait(barrier, 38)

    qm, qp, q2 = rem(q + 3, 4), rem(q + 1, 4), rem(q + 2, 4)
    pm, pp, p2 = rem(p + 3, 4), rem(p + 1, 4), rem(p + 2, 4)
    top, low = pl.ds(0, 64), pl.ds(64, 64)
    both_z, both_4 = ((0, 1), (1, 7)), ((0, 1), (1, 3))
    hc = pl.ds(pl.multiple_of(256 * c, 256), 256)
    ho = pl.ds(pl.multiple_of(256 * oc, 256), 256)

    def eight(ref, k):
        return ref.at[pl.ds(pl.multiple_of(8 * k, 8), 8)]

    send(dec_src.at[0], dec_par.at[0], prs.at[4], prr.at[4], partner)
    send(st_send.at[:, ho], st_other, prs.at[0], prr.at[0], partner)
    for n in range(2):
        for side, d in both_z:
            k = n if side == 0 else 1 - n
            rk = pl.ds(128 * k, 128)
            send(g_ref.at[rk], gfull.at[z, rk], zs.at[side, 0, k], zr.at[side, 0, k], at_head(rem(z + d, 8)))
    for side, d in both_4:
        send(w_ref, wbuf.at[c, p, q], w1s.at[side], w1r.at[side], first(d))
    to_seq(lambda dev, k: copy(dec_src.at[0], dec_all.at[me], des, der, dev))

    for side, d in both_4:
        send(w_ref, wbuf.at[c, p, q], w2s.at[side, 0], w2r.at[side, 0], second(d))
    gfull[z] = g_ref[...]
    wbuf[c, p, q] = w_ref[...]

    iota_i = lax.broadcasted_iota(jnp.int32, (64, 256), 0)
    iota_j = lax.broadcasted_iota(jnp.int32, (64, 256), 1)
    ct = c_ref[...].T
    raw = mm(c_ref[...], bt)
    for r in range(4):
        rs = slice(64 * r, 64 * r + 64)
        sc[rs, :] = jnp.where(iota_i + 64 * r >= iota_j, raw[rs, :], 0.0)
    sct[...] = mm(b_ref[...], ct)

    got(dec_par.at[0], prr.at[4])
    d_own, d_par = dec_src[0, :, hc], dec_par[0, :, hc]
    d_0, d_1 = jnp.where(c == 0, d_own, d_par), jnp.where(c == 0, d_par, d_own)
    got(st_other, prr.at[0])
    own, other = st_send[:, hc], st_other[...]
    l_0, l_1 = jnp.where(c == 0, own, other), jnp.where(c == 0, other, own)
    st_pair[...] = l_1 + d_1 * l_0
    to_chips(lambda dev, k: copy(eight(st_pair, k), st_recv.at[here], a1s, a1r, dev))
    st_recv[here] = eight(st_pair, here)[...]

    got(wbuf.at[c, p, qm], w1r.at[0])
    send(wbuf.at[c, p, qm, top], wbuf.at[c, p, qm, top], w1s.at[2], w1r.at[2], first(1))
    for side, d in both_4:
        send(wbuf.at[c, p, qm], wbuf.at[c, p, qm], w2s.at[side, 1], w2r.at[side, 1], second(d))
    got(wbuf.at[c, p, qp], w1r.at[1])
    send(wbuf.at[c, p, qp, low], wbuf.at[c, p, qp, low], w1s.at[3], w1r.at[3], first(3))
    for side, d in both_4:
        send(wbuf.at[c, p, qp], wbuf.at[c, p, qp], w2s.at[side, 2], w2r.at[side, 2], second(d))

    half = lax.broadcasted_iota(jnp.int32, (1, 128), 1)
    keep = (
        jnp.where(half < 64, 1.0, 0.0).astype(BF),
        jnp.where(half < 64, 0.0, 1.0).astype(BF),
    )

    def inside(hp):
        ls = slice(128 * hp, 128 * hp + 128)
        mt, mb = mix_t.at[hp % 2], mix_b.at[hp % 2]
        xp = x_ref[:, ls]
        x0, x1 = xp * keep[0], xp * keep[1]
        for k in range(2):
            h = 2 * hp + k
            for r in range(4):
                rs = slice(64 * r, 64 * r + 64)
                wd = 128 if r < 2 else 256
                t = jnp.exp(jnp.minimum(lgt[rs, h : h + 1] - lg[h : h + 1, 0:wd], 0.0))
                hi, lo = split2(t * (sc[rs, 0:wd] * step_ref[h : h + 1, 0:wd]))
                dst = mt if r < 2 else mb
                rr = slice(64 * (r % 2), 64 * (r % 2) + 64)
                dst[rr, 2 * k * wd : (2 * k + 1) * wd] = hi
                dst[rr, (2 * k + 1) * wd : (2 * k + 2) * wd] = lo
        ybuf[0:128, ls] = mm(mt[...], rows(x0[0:128], x0[0:128], x1[0:128], x1[0:128]))
        ybuf[128:256, ls] = mm(mb[...], rows(x0, x0, x1, x1))

    def z_block(side, j):
        return rem(z + 8 - j, 8) if side == 0 else rem(z + j, 8)

    def z_forward(j, n):
        for side, d in both_z:
            k = n if side == 0 else 1 - n
            blk = gfull.at[z_block(side, j), pl.ds(128 * k, 128)]
            got(blk, zr.at[side, j - 1, k])
            if j < 3 or n == 0:
                send(blk, blk, zs.at[side, j, k], zr.at[side, j, k], at_head(rem(z + d, 8)))

    spots = (q, qm, qp, q2, q2)

    def w_forward(slot):
        for side, row in ((0, pm), (1, pp)):
            if slot < 3:
                blk = wbuf.at[c, row, spots[slot]]
                part = blk.at[top if side == 0 else low]
                on = True
            else:
                blk = part = wbuf.at[c, row, q2, top if slot == 3 else low]
                on = slot == 3 + side
            got(blk, w2r.at[side, slot])
            if on:
                n = min(slot, 3)
                send(part, part, wfs.at[side, n], wfr.at[side, n], second(1 if side == 0 else 3))

    def w_second_of_opposite():
        for n, piece in ((0, top), (1, low)):
            blk = wbuf.at[c, p, q2, piece]
            got(blk, w1r.at[2 + n])
            for side, d in both_4:
                send(blk, blk, w2s.at[side, 3 + n], w2r.at[side, 3 + n], second(d))

    def to_partner(n, i2):
        send(wbuf.at[c, i2], wbuf.at[c, i2], wds.at[n], wdr.at[n], partner)

    def scan(recv, pref, back):
        s = jnp.zeros((8, 256), F32)
        for k in reversed(range(16)) if back else range(16):
            pref[k] = s
            s = s * (dec_all[2 * k, :, hc] * dec_all[2 * k + 1, :, hc]) + recv[k]

    many, few = pl.ds(0, 31), pl.ds(0, 15)

    inside(0)
    w_forward(0)
    w_second_of_opposite()
    to_partner(0, p)
    inside(1)
    z_forward(1, 0)
    z_forward(1, 1)
    got(dec_all.at[many], der)
    got(st_recv.at[few], a1r)
    scan(st_recv, st_pref, False)
    to_chips(lambda dev, k: copy(st_pref.at[k], eight(st_half, here), a2s, a2r, dev))
    eight(st_half, here)[...] = st_pref[here]
    w_forward(1)
    w_forward(2)
    inside(2)
    w_forward(3)
    w_forward(4)
    to_partner(1, pm)
    to_partner(2, pp)
    z_forward(2, 0)
    inside(3)
    z_forward(2, 1)
    z_forward(3, 0)
    for n in range(4):
        i1 = (q, qm, qp, q2)[n]
        got(wbuf.at[c, p2, i1, top], wfr.at[0, n])
        got(wbuf.at[c, p2, i1, low], wfr.at[1, n])
    to_partner(3, p2)

    got(st_recv.at[few], a2r)
    enter = st_half[...]
    later = d_0 * enter + jnp.where(c == 0, st_send[:, hc], st_other[...])
    st_give[...] = jnp.where(c == 0, later, enter)
    send(st_give, st_in.at[:, hc], prs.at[1], prr.at[1], partner)
    st_in[:, hc] = jnp.where(c == 0, enter, later)
    got(st_in.at[:, ho], prr.at[1])
    s_hi, s_lo = split2(st_in[...])
    cc = lanes(c_ref[...], c_ref[...])
    gain = gain_ref[...]

    def folded(v):
        return v[:, 0:128] + v[:, 128:256] + v[:, 256:384] + v[:, 384:512]

    for r in range(4):
        rs = slice(64 * r, 64 * r + 64)
        v = fr[rs, :] * mm(cc[rs, :], rows(s_hi, s_lo))
        ycs[rs, :] = v
        ybuf[rs, :] = ybuf[rs, :] + v
    for r in range(8):
        rs = slice(32 * r, 32 * r + 32)
        zf = z_ref[rs, :].astype(F32)
        yv = ybuf[rs, :]
        s = 1.0 / (1.0 + jnp.exp(-zf))
        sil = zf * s
        u = yv * sil
        ubuf[rs, :] = u
        silb[rs, :] = sil
        ydb[rs, :] = yv * s * (1.0 + zf * (1.0 - s))
        pprod[rs, 0:128] = folded(u * u)
    sq = jnp.sum(jnp.transpose(pprod[:, 0:128]), axis=0, keepdims=True)
    sq_src[0] = sq
    sq_all[z] = sq
    to_head(lambda k: copy(sq_src.at[0], sq_all.at[z], sqs, sqr, at_head(k)))

    z_forward(3, 1)
    for n in range(4):
        got(wbuf.at[oc, p], wdr.at[n])

    gn[...] = jnp.zeros((256, 512), F32)

    def add_block(h):
        yy, xx = div(h, 2), 2 * rem(h, 2)
        rhs = rows(wbuf[0, yy, xx], wbuf[1, xx, yy], wbuf[0, yy, xx + 1], wbuf[1, xx + 1, yy])
        gn[...] = gn[...] + mm(gfull[h], rhs)

    def one_block(d, carry):
        add_block(rem(z + 5 + d, 8))
        return carry

    lax.fori_loop(0, 7, one_block, 0)
    for side in range(2):
        got(gfull.at[z_block(side, 4), pl.ds(128 * side, 128)], zr.at[side, 3, side])
    add_block(rem(z + 4, 8))
    for r in range(8):
        rs = slice(32 * r, 32 * r + 32)
        pprod[rs, 128:256] = folded(gn[rs, :] * gain * ubuf[rs, :])
    cr = jnp.sum(jnp.transpose(pprod[:, 128:256]), axis=0, keepdims=True)
    cr_src[0] = cr
    cr_all[z] = cr
    to_head(lambda k: copy(cr_src.at[0], cr_all.at[z], crs, crr, at_head(k)))

    seven = pl.ds(0, 7)
    got(sq_all.at[seven], sqr)
    inv_row = lax.rsqrt(jnp.sum(sq_all[...], axis=0) / 4096.0 + EPSILON)
    zero7 = jnp.zeros((7, 256), F32)
    colst[:, 0:8] = jnp.transpose(rows(inv_row, zero7))
    gg_acc = jnp.zeros((8, 512), F32)
    for r in range(8):
        rs = slice(32 * r, 32 * r + 32)
        ui = ubuf[rs, :] * colst[rs, 0:1]
        nb[rs, :] = (ui * gain).astype(BF)
        gg_acc = gg_acc + jnp.sum((gn[rs, :] * ui).reshape(4, 8, 512), axis=0)
    ntr[...] = nb[...].T

    for n in range(4):
        i2 = rem(q + ORDER[n], 4)

        def one_chip(i1, carry, i2=i2):
            yy, xx = i2 * c + i1 * oc, i1 * c + i2 * oc
            blk = 2 * yy + div(xx, 2)
            base = rem(xx, 2) * 256
            mine = gfull[blk, :, pl.ds(pl.multiple_of(base + 128 * c, 128), 128)]
            other = gfull[blk, :, pl.ds(pl.multiple_of(base + 128 * oc, 128), 128)]
            both = mm(ntr[...], lanes(mine, other))
            pt_own[yy * oc + xx * c, xx * oc + yy * c] = both[:, 0:128]
            pt_send[i2, i1] = both[:, 128:256].astype(BF)
            return carry

        lax.fori_loop(0, 4, one_chip, 0)
        send(pt_send.at[i2], pt_recv.at[i2], d0s.at[n], d0r.at[n], partner)

    gg_src[0] = jnp.sum(gg_acc, axis=0, keepdims=True)
    gg_all[me] = gg_src[0]
    ab, cd = pl.ds(0, 2), pl.ds(2, 2)
    got(pt_recv.at[p2], d0r.at[0])
    for i in range(4):
        rs_o[i] = (pt_own[p2, i] + pt_recv[p2, i].astype(F32)).astype(BF)
    send(rs_o.at[ab], buf_p, r1s.at[0], r1r.at[0], second(1))
    send(rs_o.at[cd], buf_m, r1s.at[1], r1r.at[1], second(3))

    got(cr_all.at[seven], crr)
    coef_row = inv_row * inv_row * (jnp.sum(cr_all[...], axis=0) / 4096.0)
    colst[:, 8:16] = jnp.transpose(rows(coef_row, zero7))
    for r in range(8):
        rs = slice(32 * r, 32 * r + 32)
        gu = colst[rs, 0:1] * (gn[rs, :] * gain - ubuf[rs, :] * colst[rs, 8:9])
        gz_ref[rs, :] = (gu * ydb[rs, :]).astype(BF)
        e = gu * silb[rs, :]
        hi, lo = split2(e)
        ehi[rs, :] = hi
        elo[rs, :] = lo
        hi, lo = split2(e * fr[rs, :])
        ef2[rs, :] = hi
        ef2[256 + 32 * r : 288 + 32 * r, :] = lo
        hi, lo = split2(e * ycs[rs, :])
        rprod[rs, 0:512] = hi
        rprod[rs, 512:1024] = lo
    ad_send[...] = mm(lanes(ct, ct), ef2[...])
    send(ad_send.at[:, ho], ad_other, prs.at[2], prr.at[2], partner)
    store(gz_ref, gz_hbm)
    to_seq(lambda dev, k: copy(gg_src.at[0], gg_all.at[me], ggs, ggr, dev))

    got(pt_recv.at[pp], d0r.at[1])
    for i in range(4):
        v = pt_own[pp, i] + pt_recv[pp, i].astype(F32)
        if i < 2:
            pt_own[pp, i] = v
        else:
            rs_p[i] = v.astype(BF)
    got(pt_recv.at[pm], d0r.at[2])
    for i in range(4):
        v = pt_own[pm, i] + pt_recv[pm, i].astype(F32)
        if i < 2:
            rs_m[i] = v.astype(BF)
        else:
            pt_own[pm, i] = v
    got(ad_other, prr.at[2])
    own, other = ad_send[:, hc], ad_other[...]
    ad_pair[...] = jnp.where(c == 0, own, other) + d_0 * jnp.where(c == 0, other, own)
    to_chips(lambda dev, k: copy(eight(ad_pair, k), ad_recv.at[here], b1s, b1r, dev))
    ad_recv[here] = eight(ad_pair, here)[...]
    send(rs_p.at[cd], fin.at[0, cd], r1s.at[2], r1r.at[2], second(1))
    send(rs_m.at[ab], fin.at[1, ab], r1s.at[3], r1r.at[3], second(3))

    mask_t = (iota_j >= iota_i, iota_j >= iota_i + 64)
    mask_b = (iota_j[:, 0:128] >= iota_i[:, 0:128], iota_j[:, 0:128] >= iota_i[:, 0:128] + 64)

    def inside_back(hp):
        ls = slice(128 * hp, 128 * hp + 128)
        mw = mixw.at[hp % 2]
        xp = x_ref[:, ls]
        eh, el = ehi[:, ls], elo[:, ls]
        e2 = lanes(eh, el)
        for k in range(2):
            h = 2 * hp + k
            xk = xp * keep[k]
            x2 = lanes(xk, xk)
            inner_t = nt(x2[0:128], e2)
            inner_b = nt(x2[128:256], e2[128:256])
            racc_l = jnp.zeros((1, 128), F32)
            racc_r = jnp.zeros((1, 128), F32)
            for r in range(4):
                rs = slice(64 * r, 64 * r + 64)
                rr = slice(64 * (r % 2), 64 * (r % 2) + 64)
                cs = slice(0, 256) if r < 2 else slice(128, 256)
                t = jnp.exp(jnp.minimum(lg[h : h + 1, cs] - lgt[rs, h : h + 1], 0.0))
                tab = jnp.where(mask_t[r] if r < 2 else mask_b[r - 2], t, 0.0)
                inner = inner_t[rr] if r < 2 else inner_b[rr]
                st = sct[rs, cs]
                sj = stept[rs, h : h + 1]
                w = tab * inner
                sw = w * sj
                if r < 2:
                    mw[rr, 256 * k : 256 * k + 256] = (tab * st * sj).astype(BF)
                else:
                    mw[128 + 64 * (r - 2) : 192 + 64 * (r - 2), 128 * k : 128 * k + 128] = (tab * st * sj).astype(BF)
                qcol[rs, h : h + 1] = jnp.sum(w * st, axis=1, keepdims=True)
                if h == 0:
                    ws[rs, cs] = sw
                else:
                    ws[rs, cs] = ws[rs, cs] + sw
                rsum = jnp.sum(sw * st, axis=0, keepdims=True)
                if r < 2:
                    racc_l = racc_l + rsum[:, 0:128]
                    racc_r = racc_r + rsum[:, 128:256]
                else:
                    racc_r = racc_r + rsum
            rowp[h : h + 1, 0:128] = racc_l
            rowp[h : h + 1, 128:256] = racc_r
        em0, em1 = lanes(eh * keep[0], el * keep[0]), lanes(eh * keep[1], el * keep[1])
        v = mm(mw[0:128, :], rows(em0, em1))
        gxi[0:128, ls] = v[:, 0:128] + v[:, 128:256]
        v = mm(mw[128:256, 0:256], rows(em0[128:256], em1[128:256]))
        gxi[128:256, ls] = v[:, 0:128] + v[:, 128:256]

    for hp in range(4):
        inside_back(hp)

    got(ad_recv.at[few], b1r)
    scan(ad_recv, ad_pref, True)
    to_chips(lambda dev, k: copy(ad_pref.at[k], eight(ad_half, here), b2s, b2r, dev))
    eight(ad_half, here)[...] = ad_pref[here]

    got(buf_p, r1r.at[0])
    for i in range(2):
        rs_p[i] = (pt_own[pp, i] + buf_p[i].astype(F32)).astype(BF)
    send(rs_p.at[ab], fin.at[0, ab], r2s.at[0], r2r.at[0], second(1))
    got(buf_m, r1r.at[1])
    for i in range(2):
        rs_m[2 + i] = (pt_own[pm, 2 + i] + buf_m[i].astype(F32)).astype(BF)
    send(rs_m.at[cd], fin.at[1, cd], r2s.at[1], r2r.at[1], second(3))

    ws[128:256, 0:128] = jnp.zeros((128, 128), F32)
    w_hi, w_lo = split2(jnp.transpose(ws[...]))
    gq = mm(lanes(w_hi, w_lo), rows(b_ref[...], b_ref[...]))
    gq = gq + nt(lanes(ef2[0:256], ef2[256:512], ef2[0:256]), lanes(s_hi, s_hi, s_lo))
    for k in range(8):
        cpart[k] = gq[32 * k : 32 * k + 32]
    crecv[z] = cpart[z]
    to_head(lambda k: copy(cpart.at[k], crecv.at[z], c1s, c1r, at_head(k)))
    w_hi, w_lo = split2(ws[...])
    gk = mm(lanes(w_hi, w_lo), rows(c_ref[...], c_ref[...]))

    got(pt_recv.at[p], d0r.at[3])
    for i in range(4):
        pt_own[p, i] = pt_own[p, i] + pt_recv[p, i].astype(F32)
    e16 = lanes(e8, e8)
    rstate = nt(e16, rprod[...])

    got(ad_recv.at[few], b2r)
    enter = ad_half[...]
    sooner = jnp.where(c == 0, ad_other[...], ad_send[:, hc]) + d_1 * enter
    ad_give[...] = jnp.where(c == 0, enter, sooner)
    send(ad_give, ad_in.at[:, hc], prs.at[3], prr.at[3], partner)
    ad_in[:, hc] = jnp.where(c == 0, sooner, enter)
    got(ad_in.at[:, ho], prr.at[3])
    a_hi, a_lo = split2(ad_in[...])
    gk = gk + nt(lanes(xs2[0:256], xs2[256:512], xs2[0:256]), lanes(a_hi, a_hi, a_lo))
    for k in range(8):
        bpart[k] = gk[32 * k : 32 * k + 32].astype(BF)
    brecv[z] = bpart[z]
    to_head(lambda k: copy(bpart.at[k], brecv.at[z], k1s, k1r, at_head(k)))
    got(crecv.at[seven], c1r)
    csum[...] = jnp.sum(crecv[...], axis=0)
    call_[z] = csum[...]
    to_head(lambda k: copy(csum, call_.at[z], c2s, c2r, at_head(k)))

    for r in range(4):
        rs = slice(64 * r, 64 * r + 64)
        ka = mm(lanes(b_ref[rs, :], b_ref[rs, :]), rows(a_hi, a_lo))
        gx_ref[rs, :] = (gxi[rs, :] + stl[rs, :] * ka).astype(BF)
        hi, lo = split2(x_ref[rs, :].astype(F32) * ka)
        pprod[rs, 0:512] = hi.astype(F32)
        pprod[rs, 512:1024] = lo.astype(F32)
    carr = nt(e16, pprod[...].astype(BF))
    store(gx_ref, gx_hbm)
    held = jnp.sum((ad_in[...] * st_in[...]).reshape(16, 8, 512), axis=0)
    h_hi, h_lo = split2(held)
    held8 = jnp.sum(nt(e16, lanes(h_hi, h_lo)), axis=1, keepdims=True)
    logs = lg[...]
    step = step_ref[...]
    rate = rate_c[:, 0:1]
    tail = jnp.exp(logs[:, 255:256] - logs)
    q_in = jnp.transpose(qcol[...])[0:8, :]
    tc = tail * carr
    q_terms = q_in + tc
    drive = rowp[...] + rstate - step * q_terms
    boundary = jnp.exp(logs[:, 255:256]) * held8 + jnp.sum(step * tc, axis=1, keepdims=True)
    tri_l = jnp.where(ia >= ib, 1.0, 0.0).astype(BF)
    v1, v2, v3 = split3(drive)
    log_grad = mm(v1, tri_l) + mm(v2, tri_l) + mm(v3, tri_l) + boundary
    gs_ref[...] = q_terms - rate * log_grad
    rp = -jnp.sum(step * log_grad, axis=1, keepdims=True)
    d0 = lax.broadcasted_iota(jnp.int32, (8, 128), 0)
    d1 = lax.broadcasted_iota(jnp.int32, (8, 128), 1)
    rt_src[0] = jnp.sum(jnp.where(d0 == d1, rp, 0.0), axis=0, keepdims=True)
    rt_all[me] = rt_src[0]
    to_seq(lambda dev, k: copy(rt_src.at[0], rt_all.at[me], rts, rtr, dev))
    store(gs_ref, gs_hbm)

    got(fin.at[0, cd], r1r.at[2])
    got(fin.at[1, ab], r1r.at[3])
    got(fin.at[0, ab], r2r.at[0])
    got(fin.at[1, cd], r2r.at[1])

    def total(i):
        return pt_own[p, i] + fin[0, i].astype(F32) + fin[1, i].astype(F32)

    hi_rows, lo_rows = pl.ds(0, 256), pl.ds(256, 256)
    t_o[...] = total(q2).astype(BF)
    send(t_o.at[hi_rows], tbuf_p, r1s.at[4], r1r.at[4], first(1))
    send(t_o.at[lo_rows], tbuf_m, r1s.at[5], r1r.at[5], first(3))
    v = total(qp)
    tot[0] = v[0:256]
    t_p[256:512, :] = v[256:512].astype(BF)
    send(t_p.at[lo_rows], tfin.at[0, lo_rows], r1s.at[6], r1r.at[6], first(1))
    v = total(qm)
    tot[1] = v[256:512]
    t_m[0:256, :] = v[0:256].astype(BF)
    send(t_m.at[hi_rows], tfin.at[1, hi_rows], r1s.at[7], r1r.at[7], first(3))

    got(brecv.at[seven], k1r)
    bsum[...] = jnp.sum(brecv[...].astype(F32), axis=0).astype(BF)
    ball[z] = bsum[...]
    to_head(lambda k: copy(bsum, ball.at[z], k2s, k2r, at_head(k)))

    mine_w = total(q)
    got(tbuf_p, r1r.at[4])
    t_p[0:256, :] = (tot[0] + tbuf_p[...].astype(F32)).astype(BF)
    send(t_p.at[hi_rows], tfin.at[0, hi_rows], r2s.at[2], r2r.at[2], first(1))
    got(tbuf_m, r1r.at[5])
    t_m[256:512, :] = (tot[1] + tbuf_m[...].astype(F32)).astype(BF)
    send(t_m.at[lo_rows], tfin.at[1, lo_rows], r2s.at[3], r2r.at[3], first(3))

    got(gg_all.at[many], ggr)
    gg_ref[...] = jnp.sum(gg_all[...], axis=0)
    store(gg_ref, gg_hbm)
    got(call_.at[seven], c2r)
    for k in range(8):
        gc_ref[32 * k : 32 * k + 32, :] = call_[k]
    store(gc_ref, gc_hbm)
    got(rt_all.at[many], rtr)
    gr_ref[...] = jnp.sum(rt_all[...], axis=0)[:, 0:8]
    store(gr_ref, gr_hbm)

    got(tfin.at[0, lo_rows], r1r.at[6])
    got(tfin.at[1, hi_rows], r1r.at[7])
    got(tfin.at[0, hi_rows], r2r.at[2])
    got(tfin.at[1, lo_rows], r2r.at[3])
    gw_ref[...] = jnp.transpose(mine_w + tfin[0].astype(F32) + tfin[1].astype(F32))
    store(gw_ref, gw_hbm)
    got(ball.at[seven], k2r)
    for k in range(8):
        gb_ref[32 * k : 32 * k + 32, :] = ball[k].astype(F32)
    store(gb_ref, gb_hbm)

    def left(ref, sem):
        copy(ref, ref, sem, sem, partner).wait_send()

    for d in sent:
        d.wait_send()
    for d in stored:
        d.wait()
    for ref, sem in [
        (dec_all, des),
        (gg_all, ggs), (rt_all, rts),
    ]:
        left(ref.at[many], sem)
    for ref, sem in [(st_recv, a1s), (st_recv, a2s), (ad_recv, b1s), (ad_recv, b2s)]:
        left(ref.at[few], sem)
    for ref, sem in [(sq_all, sqs), (cr_all, crs), (crecv, c1s), (call_, c2s), (brecv, k1s), (ball, k2s)]:
        left(ref.at[seven], sem)


def hand_over(*refs):
    took = [pltpu.make_async_copy(refs[i], refs[16 + i], refs[24].at[i]) for i in range(8)]
    gave = [pltpu.make_async_copy(refs[16 + i], refs[8 + i], refs[24].at[8 + i]) for i in range(8)]
    for one in took:
        one.start()
    for one, other in zip(took, gave):
        one.wait()
        other.start()
    for one in gave:
        one.wait()


def on_device(
    inputs, gates, b_proj, c_proj, step_size, decay_rate, norm_gain, out_weight, grad_out
):
    V = pltpu.VMEM
    dma = pltpu.SemaphoreType.DMA
    scratch = [
        V((256, 512), BF), V((256, 512), BF), V((256, 128), F32), V((256, 128), F32),
        V((8, 256), F32), V((1, 8), F32), V((1, 512), F32), V((128, 512), F32), dma((8,)),
        V((256, 512), BF), V((256, 512), BF), V((256, 128), BF), V((256, 128), BF),
        V((8, 256), F32), V((1, 8), F32), V((1, 512), F32), V((128, 512), BF), V((256, 512), BF),
        V((8, 256, 512), BF), V((2, 4, 4, 128, 512), BF),
        V((1, 1, 512), F32), V((32, 1, 512), F32), V((1, 1, 512), F32),
        V((128, 512), F32), V((16, 8, 256), F32), V((16, 8, 256), F32), V((128, 512), F32),
        V((128, 256), F32), V((128, 256), F32), V((128, 256), F32), V((128, 256), F32),
        V((128, 512), F32), V((16, 8, 256), F32), V((16, 8, 256), F32), V((128, 512), F32),
        V((128, 256), F32), V((128, 256), F32), V((128, 256), F32), V((128, 256), F32),
        V((1, 1, 256), F32), V((8, 1, 256), F32), V((1, 1, 256), F32), V((8, 1, 256), F32),
        V((4, 4, 512, 128), F32), V((4, 4, 512, 128), BF), V((4, 4, 512, 128), BF),
        V((4, 512, 128), BF), V((4, 512, 128), BF), V((4, 512, 128), BF),
        V((2, 512, 128), BF), V((2, 512, 128), BF), V((2, 4, 512, 128), BF),
        V((2, 256, 128), F32), V((512, 128), BF), V((512, 128), BF), V((512, 128), BF),
        V((256, 128), BF), V((256, 128), BF), V((2, 512, 128), BF),
        V((8, 32, 128), F32), V((8, 32, 128), F32), V((32, 128), F32), V((8, 32, 128), F32),
        V((8, 32, 128), BF), V((8, 32, 128), BF), V((32, 128), BF), V((8, 32, 128), BF),
        V((1, 1, 512), F32), V((32, 1, 512), F32), V((1, 1, 128), F32), V((32, 1, 128), F32),
        V((8, 128), F32), V((8, 256), F32), V((256, 128), F32), V((256, 128), F32),
        V((256, 512), F32), V((256, 512), F32), V((512, 512), BF),
        V((256, 256), F32), V((256, 256), F32),
        V((2, 128, 512), BF), V((2, 128, 1024), BF),
        V((256, 512), F32), V((256, 512), F32), V((256, 512), F32),
        V((256, 512), F32), V((256, 512), F32), V((256, 512), F32),
        V((256, 512), BF), V((512, 256), BF),
        V((256, 512), BF), V((256, 512), BF), V((512, 512), BF), V((256, 1024), BF),
        V((256, 128), F32), V((256, 256), F32), V((256, 128), F32), V((8, 256), F32),
        V((256, 512), F32), V((2, 256, 512), BF), V((256, 1024), F32),
        dma((9,)), dma((5,)), dma((5,)), dma((2, 4, 2)), dma((2, 4, 2)), dma((4,)), dma((4,)), dma((2, 5)), dma((2, 5)),
        dma((2, 4)), dma((2, 4)), dma((4,)), dma((4,)),
        dma, dma, dma, dma, dma, dma, dma, dma, dma, dma, dma, dma, dma, dma,
        dma((4,)), dma((4,)), dma((8,)), dma((8,)), dma((4,)), dma((4,)),
        dma, dma, dma, dma, dma, dma, dma, dma, dma, dma, dma, dma,
    ]
    outs = (
        jax.ShapeDtypeStruct((256, 512), BF),
        jax.ShapeDtypeStruct((256, 512), BF),
        jax.ShapeDtypeStruct((256, 128), F32),
        jax.ShapeDtypeStruct((256, 128), F32),
        jax.ShapeDtypeStruct((8, 256), F32),
        jax.ShapeDtypeStruct((1, 8), F32),
        jax.ShapeDtypeStruct((1, 512), F32),
        jax.ShapeDtypeStruct((128, 512), F32),
    )
    far = pl.BlockSpec(memory_space=pltpu.HBM)
    results = pl.pallas_call(
        kernel,
        out_shape=outs,
        in_specs=[far] * 9,
        out_specs=[far] * 8,
        scratch_shapes=scratch,
        compiler_params=pltpu.CompilerParams(
            collective_id=0, has_side_effects=True, vmem_limit_bytes=60000000
        ),
    )(
        inputs, gates, b_proj, c_proj, step_size, decay_rate.reshape(1, 8),
        norm_gain.reshape(1, 512), out_weight, grad_out,
    )
    gx, gz, gb, gc, gs, gr, gg, gw = pl.pallas_call(
        hand_over,
        out_shape=outs,
        in_specs=[far] * 8,
        out_specs=[far] * 8,
        scratch_shapes=[V(o.shape, o.dtype) for o in outs] + [dma((16,))],
        compiler_params=pltpu.CompilerParams(vmem_limit_bytes=60000000),
    )(*results)
    return gx, gz, gb, gc, gs, gr.reshape(8), gg.reshape(512), gw


def solution(mesh):
    split = Mesh(
        mesh.devices.reshape(4, 4, 2, mesh.shape["head"]), ("seq_0", "seq_1", "seq_2", "head")
    )
    return jax.shard_map(
        on_device,
        mesh=split,
        in_specs=(
            P(SEQ, "head"), P(SEQ, "head"), P(SEQ, None), P(SEQ, None), P("head", SEQ),
            P("head"), P("head"), P(SEQ, "head"), P(SEQ, "head"),
        ),
        out_specs=(
            P(SEQ, "head"), P(SEQ, "head"), P(SEQ, None), P(SEQ, None), P("head", SEQ),
            P("head"), P("head"), P(SEQ, "head"),
        ),
        check_vma=False,
    )
```

```python
import jax
import jax.numpy as jnp
from jax import lax
from jax.experimental import pallas as pl
from jax.experimental.pallas import tpu as pltpu
from jax.sharding import Mesh
from jax.sharding import PartitionSpec as P

SEQ = ("seq_0", "seq_1", "seq_2")
EPSILON = 1e-05
MESH = pl.DeviceIdType.MESH
BF = jnp.bfloat16
F32 = jnp.float32


def mm(a, b):
    return jnp.dot(a, b, preferred_element_type=F32)


def nt(a, b):
    return lax.dot_general(a, b, (((1,), (1,)), ((), ())), preferred_element_type=F32)


def split2(v):
    hi = v.astype(BF)
    return hi, (v - hi.astype(F32)).astype(BF)


def split3(v):
    hi = v.astype(BF)
    rest = v - hi.astype(F32)
    mid = rest.astype(BF)
    return hi, mid, (rest - mid.astype(F32)).astype(BF)


def lanes(*parts):
    return jnp.concatenate(parts, axis=1)


def rows(*parts):
    return jnp.concatenate(parts, axis=0)


ORDER = (2, 1, 3, 0)


def kernel(
    x_hbm, z_hbm, b_hbm, c_hbm, step_hbm, rate_hbm, gain_hbm, w_hbm, g_hbm,
    gx_hbm, gz_hbm, gb_hbm, gc_hbm, gs_hbm, gr_hbm, gg_hbm, gw_hbm,
    gx_ref, gz_ref, gb_ref, gc_ref, gs_ref, gr_ref, gg_ref, gw_ref, outs,
    x_ref, z_ref, b_ref, c_ref, step_ref, rate_ref, gain_ref, w_ref, g_ref,
    gfull, wbuf, dec_src, dec_all, dec_par, dec_two, st_send, st_recv, st_pref, st_in,
    st_other, st_pair, st_half, st_give,
    ad_send, ad_recv, ad_pref, ad_in, ad_other, ad_pair, ad_half, ad_give, sq_src, sq_all, cr_src, cr_all,
    pt_own, pt_send, pt_recv, rs_o, rs_p, rs_m, buf_p, buf_m, fin,
    tot, t_o, t_p, t_m, tbuf_p, tbuf_m, tfin,
    cpart, crecv, csum, call_, bpart, brecv, bsum, ball,
    gg_src, gg_all, rt_src, rt_all,
    rate_c, lg, lgt, stept, fr, stl, xs2, sc, sct, mix_t, mix_b, ybuf, ycs, gn,
    ubuf, silb, ydb, nb, ntr, ehi, elo, ef2, rprod, colst, ws, qcol, rowp, gxi, mixw, pprod,
    kx, ky, kyy, kc, kz1, kz2, kz3, ins, prs, prr, zs, zr, w1s, w1r, w2s, w2r, wfs, wfr, wds, wdr, des, der, a1s, a1r, a2s, a2r,
    b1s, b1r, b2s, b2r, sqs, sqr, crs, crr, d0s, d0r, r1s, r1r, r2s, r2r,
    c1s, c1r, c2s, c2r, k1s, k1r, k2s, k2r, ggs, ggr, rts, rtr,
):
    y = lax.axis_index("seq_0")
    x = lax.axis_index("seq_1")
    c = lax.axis_index("seq_2")
    z = lax.axis_index("head")
    me = (y * 4 + x) * 2 + c
    oc = 1 - c
    q = x * oc + y * c
    p = y * oc + x * c
    rem, div = lax.rem, lax.div

    def at_head(k):
        return (y, x, c, k)

    def first(d):
        return (rem(y + d * c, 4), rem(x + d * oc, 4), c, z)

    def second(d):
        return (rem(y + d * oc, 4), rem(x + d * c, 4), c, z)

    partner = (y, x, oc, z)

    def copy(src, dst, ssem, rsem, dev):
        return pltpu.make_async_remote_copy(
            src_ref=src, dst_ref=dst, send_sem=ssem, recv_sem=rsem,
            device_id=dev, device_id_type=MESH,
        )

    def got(ref, sem):
        copy(ref, ref, sem, sem, partner).wait_recv()

    sent, stored = [], []

    def store(src, dst):
        one = pltpu.make_async_copy(src, dst, outs.at[len(stored)])
        one.start()
        stored.append(one)

    def send(src, dst, ssem, rsem, dev):
        d = copy(src, dst, ssem, rsem, dev)
        d.start()
        sent.append(d)

    far_first = sorted(
        ((dy, dx, dc) for dy in range(4) for dx in range(4) for dc in range(2)),
        key=lambda o: -(min(o[0], 4 - o[0]) + min(o[1], 4 - o[1])) - 0.1 * o[2],
    )
    ys, xs, cs = [rem(y + d, 4) for d in range(4)], [rem(x + d, 4) for d in range(4)], (c, oc)
    peers = [
        ((ys[dy], xs[dx], cs[dc], z), (ys[dy] * 4 + xs[dx]) * 2 + cs[dc])
        for dy, dx, dc in far_first
        if (dy, dx, dc) != (0, 0, 0)
    ]

    chips = [
        ((ys[dy], xs[dx], c, z), ys[dy] * 4 + xs[dx])
        for dy, dx, dc in far_first
        if dc == 0 and (dy, dx) != (0, 0)
    ]
    here = y * 4 + x

    def to_chips(make):
        for dev, k in chips:
            make(dev, k).start()

    def to_seq(make):
        for dev, k in peers:
            make(dev, k).start()

    def to_head(make):
        for d in (4, 3, 5, 2, 6, 1, 7):
            make(rem(z + d, 8)).start()

    near_x = [(y, rem(x + d, 4), c, z) for d in (1, 3)]
    near_y = [(rem(y + d, 4), x, c, z) for d in (1, 3)]
    near_z = [(y, x, c, rem(z + d, 8)) for d in (1, 7)]

    def tell(sem, devices):
        for dev in devices:
            pl.semaphore_signal(sem, inc=1, device_id=dev, device_id_type=MESH)

    barrier = pltpu.get_barrier_semaphore()
    fetches = [
        pltpu.make_async_copy(src, dst, ins.at[i])
        for i, (src, dst) in enumerate((
            (g_hbm, g_ref), (w_hbm, w_ref), (step_hbm, step_ref), (rate_hbm, rate_ref),
            (b_hbm, b_ref), (x_hbm, x_ref), (c_hbm, c_ref), (gain_hbm, gain_ref), (z_hbm, z_ref),
        ))
    ]
    for f in fetches:
        f.start()
    tell(barrier, near_z + near_x + near_y + [partner])
    for f in fetches[:2]:
        f.wait()
    pl.semaphore_wait(barrier, 7)
    tell(kx, near_x)
    tell(kz1, near_z)

    qm, qp, q2 = rem(q + 3, 4), rem(q + 1, 4), rem(q + 2, 4)
    pm, pp, p2 = rem(p + 3, 4), rem(p + 1, 4), rem(p + 2, 4)
    top, low = pl.ds(0, 64), pl.ds(64, 64)
    both_z, both_4 = ((0, 1), (1, 7)), ((0, 1), (1, 3))
    for n in range(2):
        for side, d in both_z:
            k = n if side == 0 else 1 - n
            rk = pl.ds(128 * k, 128)
            send(g_ref.at[rk], gfull.at[z, rk], zs.at[side, 0, k], zr.at[side, 0, k], at_head(rem(z + d, 8)))
    for side, d in both_4:
        send(w_ref, wbuf.at[c, p, q], w1s.at[side], w1r.at[side], first(d))
    for side, d in both_4:
        send(w_ref, wbuf.at[c, p, q], w2s.at[side, 0], w2r.at[side, 0], second(d))
    gfull[z] = g_ref[...]
    wbuf[c, p, q] = w_ref[...]

    for f in fetches[2:5]:
        f.wait()

    i8 = lax.broadcasted_iota(jnp.int32, (8, 8), 0)
    j8 = lax.broadcasted_iota(jnp.int32, (8, 8), 1)
    rate = jnp.sum(jnp.where(i8 == j8, jnp.broadcast_to(rate_ref[...], (8, 8)), 0.0), axis=1, keepdims=True)
    rate_c[...] = jnp.broadcast_to(rate, (8, 128))
    step = step_ref[...]
    ia = lax.broadcasted_iota(jnp.int32, (256, 256), 0)
    ib = lax.broadcasted_iota(jnp.int32, (256, 256), 1)
    tri_u = jnp.where(ia <= ib, 1.0, 0.0).astype(BF)
    v1, v2, v3 = split3(rate * step)
    logs = -(mm(v1, tri_u) + mm(v2, tri_u) + mm(v3, tri_u))
    lg[...] = logs
    logs_t = jnp.transpose(logs)
    step_t = jnp.transpose(step)
    lgt[:, 0:8] = logs_t
    stept[:, 0:8] = step_t
    e8 = jnp.where(
        lax.broadcasted_iota(jnp.int32, (8, 512), 0)
        == lax.broadcasted_iota(jnp.int32, (8, 512), 1) // 64, 1.0, 0.0,
    ).astype(BF)

    def spread_heads(v):
        a1, a2, a3 = split3(v)
        return mm(a1, e8) + mm(a2, e8) + mm(a3, e8)

    fr[...] = spread_heads(jnp.exp(logs_t))
    stl[...] = spread_heads(step_t * jnp.exp(logs_t[255:256, :] - logs_t))
    dec_src[0] = fr[255:256, :]
    bt = b_ref[...].T
    fetches[5].wait()
    pl.semaphore_wait(kx, 2)
    tell(ky, near_y)
    for r in range(4):
        rs = slice(64 * r, 64 * r + 64)
        hi, lo = split2(x_ref[rs, :].astype(F32) * stl[rs, :])
        xs2[rs, :] = hi
        xs2[64 * r + 256 : 64 * r + 320, :] = lo
    st_send[...] = mm(lanes(bt, bt), xs2[...])
    for f in fetches[6:]:
        f.wait()

    hc = pl.ds(pl.multiple_of(256 * c, 256), 256)
    ho = pl.ds(pl.multiple_of(256 * oc, 256), 256)

    def eight(ref, k):
        return ref.at[pl.ds(pl.multiple_of(8 * k, 8), 8)]

    send(dec_src.at[0], dec_par.at[0], prs.at[4], prr.at[4], partner)
    send(st_send.at[:, ho], st_other, prs.at[0], prr.at[0], partner)
    iota_i = lax.broadcasted_iota(jnp.int32, (64, 256), 0)
    iota_j = lax.broadcasted_iota(jnp.int32, (64, 256), 1)
    ct = c_ref[...].T
    raw = mm(c_ref[...], bt)
    for r in range(4):
        rs = slice(64 * r, 64 * r + 64)
        sc[rs, :] = jnp.where(iota_i + 64 * r >= iota_j, raw[rs, :], 0.0)
    sct[...] = mm(b_ref[...], ct)

    pl.semaphore_wait(ky, 2)
    tell(kyy, near_y)
    got(dec_par.at[0], prr.at[4])
    d_own, d_par = dec_src[0, :, hc], dec_par[0, :, hc]
    d_0, d_1 = jnp.where(c == 0, d_own, d_par), jnp.where(c == 0, d_par, d_own)
    got(st_other, prr.at[0])
    own, other = st_send[:, hc], st_other[...]
    l_0, l_1 = jnp.where(c == 0, own, other), jnp.where(c == 0, other, own)
    st_pair[...] = l_1 + d_1 * l_0
    dec_two[0] = dec_src[0] * dec_par[0]
    dec_all[here] = dec_two[0]
    pl.semaphore_wait(kyy, 2)
    tell(kc, [partner])
    to_chips(lambda dev, k: copy(dec_two.at[0], dec_all.at[here], des, der, dev))
    to_chips(lambda dev, k: copy(eight(st_pair, k), st_recv.at[here], a1s, a1r, dev))
    st_recv[here] = eight(st_pair, here)[...]

    got(wbuf.at[c, p, qm], w1r.at[0])
    send(wbuf.at[c, p, qm, top], wbuf.at[c, p, qm, top], w1s.at[2], w1r.at[2], first(1))
    for side, d in both_4:
        send(wbuf.at[c, p, qm], wbuf.at[c, p, qm], w2s.at[side, 1], w2r.at[side, 1], second(d))
    got(wbuf.at[c, p, qp], w1r.at[1])
    send(wbuf.at[c, p, qp, low], wbuf.at[c, p, qp, low], w1s.at[3], w1r.at[3], first(3))
    for side, d in both_4:
        send(wbuf.at[c, p, qp], wbuf.at[c, p, qp], w2s.at[side, 2], w2r.at[side, 2], second(d))

    half = lax.broadcasted_iota(jnp.int32, (1, 128), 1)
    keep = (
        jnp.where(half < 64, 1.0, 0.0).astype(BF),
        jnp.where(half < 64, 0.0, 1.0).astype(BF),
    )

    def inside(hp):
        ls = slice(128 * hp, 128 * hp + 128)
        mt, mb = mix_t.at[hp % 2], mix_b.at[hp % 2]
        xp = x_ref[:, ls]
        x0, x1 = xp * keep[0], xp * keep[1]
        for k in range(2):
            h = 2 * hp + k
            for r in range(4):
                rs = slice(64 * r, 64 * r + 64)
                wd = 128 if r < 2 else 256
                t = jnp.exp(jnp.minimum(lgt[rs, h : h + 1] - lg[h : h + 1, 0:wd], 0.0))
                hi, lo = split2(t * (sc[rs, 0:wd] * step_ref[h : h + 1, 0:wd]))
                dst = mt if r < 2 else mb
                rr = slice(64 * (r % 2), 64 * (r % 2) + 64)
                dst[rr, 2 * k * wd : (2 * k + 1) * wd] = hi
                dst[rr, (2 * k + 1) * wd : (2 * k + 2) * wd] = lo
        ybuf[0:128, ls] = mm(mt[...], rows(x0[0:128], x0[0:128], x1[0:128], x1[0:128]))
        ybuf[128:256, ls] = mm(mb[...], rows(x0, x0, x1, x1))

    def z_block(side, j):
        return rem(z + 8 - j, 8) if side == 0 else rem(z + j, 8)

    def z_forward(j, n):
        for side, d in both_z:
            k = n if side == 0 else 1 - n
            blk = gfull.at[z_block(side, j), pl.ds(128 * k, 128)]
            got(blk, zr.at[side, j - 1, k])
            if j < 3 or n == 0:
                send(blk, blk, zs.at[side, j, k], zr.at[side, j, k], at_head(rem(z + d, 8)))

    spots = (q, qm, qp, q2, q2)

    def w_forward(slot):
        for side, row in ((0, pm), (1, pp)):
            if slot < 3:
                blk = wbuf.at[c, row, spots[slot]]
                part = blk.at[top if side == 0 else low]
                on = True
            else:
                blk = part = wbuf.at[c, row, q2, top if slot == 3 else low]
                on = slot == 3 + side
            got(blk, w2r.at[side, slot])
            if on:
                n = min(slot, 3)
                send(part, part, wfs.at[side, n], wfr.at[side, n], second(1 if side == 0 else 3))

    def w_second_of_opposite():
        for n, piece in ((0, top), (1, low)):
            blk = wbuf.at[c, p, q2, piece]
            got(blk, w1r.at[2 + n])
            for side, d in both_4:
                send(blk, blk, w2s.at[side, 3 + n], w2r.at[side, 3 + n], second(d))

    def to_partner(n, i2):
        send(wbuf.at[c, i2], wbuf.at[c, i2], wds.at[n], wdr.at[n], partner)

    def scan(recv, pref, back):
        s = jnp.zeros((8, 256), F32)
        for k in reversed(range(16)) if back else range(16):
            pref[k] = s
            s = s * dec_all[k, :, hc] + recv[k]

    many, few = pl.ds(0, 31), pl.ds(0, 15)

    inside(0)
    w_forward(0)
    w_second_of_opposite()
    to_partner(0, p)
    inside(1)
    pl.semaphore_wait(kz1, 2)
    tell(kz2, near_z)
    z_forward(1, 0)
    z_forward(1, 1)
    got(dec_all.at[few], der)
    got(st_recv.at[few], a1r)
    scan(st_recv, st_pref, False)
    to_chips(lambda dev, k: copy(st_pref.at[k], eight(st_half, here), a2s, a2r, dev))
    eight(st_half, here)[...] = st_pref[here]
    w_forward(1)
    w_forward(2)
    inside(2)
    w_forward(3)
    w_forward(4)
    to_partner(1, pm)
    to_partner(2, pp)
    pl.semaphore_wait(kz2, 2)
    tell(kz3, near_z)
    z_forward(2, 0)
    inside(3)
    z_forward(2, 1)
    z_forward(3, 0)
    for n in range(4):
        i1 = (q, qm, qp, q2)[n]
        got(wbuf.at[c, p2, i1, top], wfr.at[0, n])
        got(wbuf.at[c, p2, i1, low], wfr.at[1, n])
    to_partner(3, p2)

    got(st_recv.at[few], a2r)
    enter = st_half[...]
    later = d_0 * enter + jnp.where(c == 0, st_send[:, hc], st_other[...])
    st_give[...] = jnp.where(c == 0, later, enter)
    send(st_give, st_in.at[:, hc], prs.at[1], prr.at[1], partner)
    st_in[:, hc] = jnp.where(c == 0, enter, later)
    got(st_in.at[:, ho], prr.at[1])
    s_hi, s_lo = split2(st_in[...])
    cc = lanes(c_ref[...], c_ref[...])
    gain = gain_ref[...]

    def folded(v):
        return v[:, 0:128] + v[:, 128:256] + v[:, 256:384] + v[:, 384:512]

    for r in range(4):
        rs = slice(64 * r, 64 * r + 64)
        v = fr[rs, :] * mm(cc[rs, :], rows(s_hi, s_lo))
        ycs[rs, :] = v
        ybuf[rs, :] = ybuf[rs, :] + v
    for r in range(8):
        rs = slice(32 * r, 32 * r + 32)
        zf = z_ref[rs, :].astype(F32)
        yv = ybuf[rs, :]
        s = 1.0 / (1.0 + jnp.exp(-zf))
        sil = zf * s
        u = yv * sil
        ubuf[rs, :] = u
        silb[rs, :] = sil
        ydb[rs, :] = yv * s * (1.0 + zf * (1.0 - s))
        pprod[rs, 0:128] = folded(u * u)
    sq = jnp.sum(jnp.transpose(pprod[:, 0:128]), axis=0, keepdims=True)
    sq_src[0] = sq
    sq_all[z] = sq
    pl.semaphore_wait(kz3, 2)
    to_head(lambda k: copy(sq_src.at[0], sq_all.at[z], sqs, sqr, at_head(k)))

    z_forward(3, 1)
    for n in range(4):
        got(wbuf.at[oc, p], wdr.at[n])

    gn[...] = jnp.zeros((256, 512), F32)

    def add_block(h):
        yy, xx = div(h, 2), 2 * rem(h, 2)
        rhs = rows(wbuf[0, yy, xx], wbuf[1, xx, yy], wbuf[0, yy, xx + 1], wbuf[1, xx + 1, yy])
        gn[...] = gn[...] + mm(gfull[h], rhs)

    def one_block(d, carry):
        add_block(rem(z + 5 + d, 8))
        return carry

    lax.fori_loop(0, 7, one_block, 0)
    for side in range(2):
        got(gfull.at[z_block(side, 4), pl.ds(128 * side, 128)], zr.at[side, 3, side])
    add_block(rem(z + 4, 8))
    for r in range(8):
        rs = slice(32 * r, 32 * r + 32)
        pprod[rs, 128:256] = folded(gn[rs, :] * gain * ubuf[rs, :])
    cr = jnp.sum(jnp.transpose(pprod[:, 128:256]), axis=0, keepdims=True)
    cr_src[0] = cr
    cr_all[z] = cr
    to_head(lambda k: copy(cr_src.at[0], cr_all.at[z], crs, crr, at_head(k)))

    seven = pl.ds(0, 7)
    got(sq_all.at[seven], sqr)
    inv_row = lax.rsqrt(jnp.sum(sq_all[...], axis=0) / 4096.0 + EPSILON)
    zero7 = jnp.zeros((7, 256), F32)
    colst[:, 0:8] = jnp.transpose(rows(inv_row, zero7))
    gg_acc = jnp.zeros((8, 512), F32)
    for r in range(8):
        rs = slice(32 * r, 32 * r + 32)
        ui = ubuf[rs, :] * colst[rs, 0:1]
        nb[rs, :] = (ui * gain).astype(BF)
        gg_acc = gg_acc + jnp.sum((gn[rs, :] * ui).reshape(4, 8, 512), axis=0)
    ntr[...] = nb[...].T

    for n in range(4):
        i2 = rem(q + ORDER[n], 4)

        def one_chip(i1, carry, i2=i2):
            yy, xx = i2 * c + i1 * oc, i1 * c + i2 * oc
            blk = 2 * yy + div(xx, 2)
            base = rem(xx, 2) * 256
            mine = gfull[blk, :, pl.ds(pl.multiple_of(base + 128 * c, 128), 128)]
            other = gfull[blk, :, pl.ds(pl.multiple_of(base + 128 * oc, 128), 128)]
            both = mm(ntr[...], lanes(mine, other))
            pt_own[yy * oc + xx * c, xx * oc + yy * c] = both[:, 0:128]
            pt_send[i2, i1] = both[:, 128:256].astype(BF)
            return carry

        lax.fori_loop(0, 4, one_chip, 0)
        send(pt_send.at[i2], pt_recv.at[i2], d0s.at[n], d0r.at[n], partner)

    gg_src[0] = jnp.sum(gg_acc, axis=0, keepdims=True)
    gg_all[me] = gg_src[0]
    ab, cd = pl.ds(0, 2), pl.ds(2, 2)
    got(pt_recv.at[p2], d0r.at[0])
    for i in range(4):
        rs_o[i] = (pt_own[p2, i] + pt_recv[p2, i].astype(F32)).astype(BF)
    send(rs_o.at[ab], buf_p, r1s.at[0], r1r.at[0], second(1))
    send(rs_o.at[cd], buf_m, r1s.at[1], r1r.at[1], second(3))

    got(cr_all.at[seven], crr)
    coef_row = inv_row * inv_row * (jnp.sum(cr_all[...], axis=0) / 4096.0)
    colst[:, 8:16] = jnp.transpose(rows(coef_row, zero7))
    for r in range(8):
        rs = slice(32 * r, 32 * r + 32)
        gu = colst[rs, 0:1] * (gn[rs, :] * gain - ubuf[rs, :] * colst[rs, 8:9])
        gz_ref[rs, :] = (gu * ydb[rs, :]).astype(BF)
        e = gu * silb[rs, :]
        hi, lo = split2(e)
        ehi[rs, :] = hi
        elo[rs, :] = lo
        hi, lo = split2(e * fr[rs, :])
        ef2[rs, :] = hi
        ef2[256 + 32 * r : 288 + 32 * r, :] = lo
        hi, lo = split2(e * ycs[rs, :])
        rprod[rs, 0:512] = hi
        rprod[rs, 512:1024] = lo
    ad_send[...] = mm(lanes(ct, ct), ef2[...])
    send(ad_send.at[:, ho], ad_other, prs.at[2], prr.at[2], partner)
    store(gz_ref, gz_hbm)
    pl.semaphore_wait(kc, 1)
    to_seq(lambda dev, k: copy(gg_src.at[0], gg_all.at[me], ggs, ggr, dev))

    got(pt_recv.at[pp], d0r.at[1])
    for i in range(4):
        v = pt_own[pp, i] + pt_recv[pp, i].astype(F32)
        if i < 2:
            pt_own[pp, i] = v
        else:
            rs_p[i] = v.astype(BF)
    got(pt_recv.at[pm], d0r.at[2])
    for i in range(4):
        v = pt_own[pm, i] + pt_recv[pm, i].astype(F32)
        if i < 2:
            rs_m[i] = v.astype(BF)
        else:
            pt_own[pm, i] = v
    got(ad_other, prr.at[2])
    own, other = ad_send[:, hc], ad_other[...]
    ad_pair[...] = jnp.where(c == 0, own, other) + d_0 * jnp.where(c == 0, other, own)
    to_chips(lambda dev, k: copy(eight(ad_pair, k), ad_recv.at[here], b1s, b1r, dev))
    ad_recv[here] = eight(ad_pair, here)[...]
    send(rs_p.at[cd], fin.at[0, cd], r1s.at[2], r1r.at[2], second(1))
    send(rs_m.at[ab], fin.at[1, ab], r1s.at[3], r1r.at[3], second(3))

    mask_t = (iota_j >= iota_i, iota_j >= iota_i + 64)
    mask_b = (iota_j[:, 0:128] >= iota_i[:, 0:128], iota_j[:, 0:128] >= iota_i[:, 0:128] + 64)

    def inside_back(hp):
        ls = slice(128 * hp, 128 * hp + 128)
        mw = mixw.at[hp % 2]
        xp = x_ref[:, ls]
        eh, el = ehi[:, ls], elo[:, ls]
        e2 = lanes(eh, el)
        for k in range(2):
            h = 2 * hp + k
            xk = xp * keep[k]
            x2 = lanes(xk, xk)
            inner_t = nt(x2[0:128], e2)
            inner_b = nt(x2[128:256], e2[128:256])
            racc_l = jnp.zeros((1, 128), F32)
            racc_r = jnp.zeros((1, 128), F32)
            for r in range(4):
                rs = slice(64 * r, 64 * r + 64)
                rr = slice(64 * (r % 2), 64 * (r % 2) + 64)
                cs = slice(0, 256) if r < 2 else slice(128, 256)
                t = jnp.exp(jnp.minimum(lg[h : h + 1, cs] - lgt[rs, h : h + 1], 0.0))
                tab = jnp.where(mask_t[r] if r < 2 else mask_b[r - 2], t, 0.0)
                inner = inner_t[rr] if r < 2 else inner_b[rr]
                st = sct[rs, cs]
                sj = stept[rs, h : h + 1]
                w = tab * inner
                sw = w * sj
                if r < 2:
                    mw[rr, 256 * k : 256 * k + 256] = (tab * st * sj).astype(BF)
                else:
                    mw[128 + 64 * (r - 2) : 192 + 64 * (r - 2), 128 * k : 128 * k + 128] = (tab * st * sj).astype(BF)
                qcol[rs, h : h + 1] = jnp.sum(w * st, axis=1, keepdims=True)
                if h == 0:
                    ws[rs, cs] = sw
                else:
                    ws[rs, cs] = ws[rs, cs] + sw
                rsum = jnp.sum(sw * st, axis=0, keepdims=True)
                if r < 2:
                    racc_l = racc_l + rsum[:, 0:128]
                    racc_r = racc_r + rsum[:, 128:256]
                else:
                    racc_r = racc_r + rsum
            rowp[h : h + 1, 0:128] = racc_l
            rowp[h : h + 1, 128:256] = racc_r
        em0, em1 = lanes(eh * keep[0], el * keep[0]), lanes(eh * keep[1], el * keep[1])
        v = mm(mw[0:128, :], rows(em0, em1))
        gxi[0:128, ls] = v[:, 0:128] + v[:, 128:256]
        v = mm(mw[128:256, 0:256], rows(em0[128:256], em1[128:256]))
        gxi[128:256, ls] = v[:, 0:128] + v[:, 128:256]

    for hp in range(4):
        inside_back(hp)

    got(ad_recv.at[few], b1r)
    scan(ad_recv, ad_pref, True)
    to_chips(lambda dev, k: copy(ad_pref.at[k], eight(ad_half, here), b2s, b2r, dev))
    eight(ad_half, here)[...] = ad_pref[here]

    got(buf_p, r1r.at[0])
    for i in range(2):
        rs_p[i] = (pt_own[pp, i] + buf_p[i].astype(F32)).astype(BF)
    send(rs_p.at[ab], fin.at[0, ab], r2s.at[0], r2r.at[0], second(1))
    got(buf_m, r1r.at[1])
    for i in range(2):
        rs_m[2 + i] = (pt_own[pm, 2 + i] + buf_m[i].astype(F32)).astype(BF)
    send(rs_m.at[cd], fin.at[1, cd], r2s.at[1], r2r.at[1], second(3))

    ws[128:256, 0:128] = jnp.zeros((128, 128), F32)
    w_hi, w_lo = split2(jnp.transpose(ws[...]))
    gq = mm(lanes(w_hi, w_lo), rows(b_ref[...], b_ref[...]))
    gq = gq + nt(lanes(ef2[0:256], ef2[256:512], ef2[0:256]), lanes(s_hi, s_hi, s_lo))
    for k in range(8):
        cpart[k] = gq[32 * k : 32 * k + 32]
    crecv[z] = cpart[z]
    to_head(lambda k: copy(cpart.at[k], crecv.at[z], c1s, c1r, at_head(k)))
    w_hi, w_lo = split2(ws[...])
    gk = mm(lanes(w_hi, w_lo), rows(c_ref[...], c_ref[...]))

    got(pt_recv.at[p], d0r.at[3])
    for i in range(4):
        pt_own[p, i] = pt_own[p, i] + pt_recv[p, i].astype(F32)
    e16 = lanes(e8, e8)
    rstate = nt(e16, rprod[...])

    got(ad_recv.at[few], b2r)
    enter = ad_half[...]
    sooner = jnp.where(c == 0, ad_other[...], ad_send[:, hc]) + d_1 * enter
    ad_give[...] = jnp.where(c == 0, enter, sooner)
    send(ad_give, ad_in.at[:, hc], prs.at[3], prr.at[3], partner)
    ad_in[:, hc] = jnp.where(c == 0, sooner, enter)
    got(ad_in.at[:, ho], prr.at[3])
    a_hi, a_lo = split2(ad_in[...])
    gk = gk + nt(lanes(xs2[0:256], xs2[256:512], xs2[0:256]), lanes(a_hi, a_hi, a_lo))
    for k in range(8):
        bpart[k] = gk[32 * k : 32 * k + 32].astype(BF)
    brecv[z] = bpart[z]
    to_head(lambda k: copy(bpart.at[k], brecv.at[z], k1s, k1r, at_head(k)))
    got(crecv.at[seven], c1r)
    csum[...] = jnp.sum(crecv[...], axis=0)
    call_[z] = csum[...]
    to_head(lambda k: copy(csum, call_.at[z], c2s, c2r, at_head(k)))

    for r in range(4):
        rs = slice(64 * r, 64 * r + 64)
        ka = mm(lanes(b_ref[rs, :], b_ref[rs, :]), rows(a_hi, a_lo))
        gx_ref[rs, :] = (gxi[rs, :] + stl[rs, :] * ka).astype(BF)
        hi, lo = split2(x_ref[rs, :].astype(F32) * ka)
        pprod[rs, 0:512] = hi.astype(F32)
        pprod[rs, 512:1024] = lo.astype(F32)
    carr = nt(e16, pprod[...].astype(BF))
    store(gx_ref, gx_hbm)
    held = jnp.sum((ad_in[...] * st_in[...]).reshape(16, 8, 512), axis=0)
    h_hi, h_lo = split2(held)
    held8 = jnp.sum(nt(e16, lanes(h_hi, h_lo)), axis=1, keepdims=True)
    logs = lg[...]
    step = step_ref[...]
    rate = rate_c[:, 0:1]
    tail = jnp.exp(logs[:, 255:256] - logs)
    q_in = jnp.transpose(qcol[...])[0:8, :]
    tc = tail * carr
    q_terms = q_in + tc
    drive = rowp[...] + rstate - step * q_terms
    boundary = jnp.exp(logs[:, 255:256]) * held8 + jnp.sum(step * tc, axis=1, keepdims=True)
    tri_l = jnp.where(ia >= ib, 1.0, 0.0).astype(BF)
    v1, v2, v3 = split3(drive)
    log_grad = mm(v1, tri_l) + mm(v2, tri_l) + mm(v3, tri_l) + boundary
    gs_ref[...] = q_terms - rate * log_grad
    rp = -jnp.sum(step * log_grad, axis=1, keepdims=True)
    d0 = lax.broadcasted_iota(jnp.int32, (8, 128), 0)
    d1 = lax.broadcasted_iota(jnp.int32, (8, 128), 1)
    rt_src[0] = jnp.sum(jnp.where(d0 == d1, rp, 0.0), axis=0, keepdims=True)
    rt_all[me] = rt_src[0]
    to_seq(lambda dev, k: copy(rt_src.at[0], rt_all.at[me], rts, rtr, dev))
    store(gs_ref, gs_hbm)

    got(fin.at[0, cd], r1r.at[2])
    got(fin.at[1, ab], r1r.at[3])
    got(fin.at[0, ab], r2r.at[0])
    got(fin.at[1, cd], r2r.at[1])

    def total(i):
        return pt_own[p, i] + fin[0, i].astype(F32) + fin[1, i].astype(F32)

    hi_rows, lo_rows = pl.ds(0, 256), pl.ds(256, 256)
    t_o[...] = total(q2).astype(BF)
    send(t_o.at[hi_rows], tbuf_p, r1s.at[4], r1r.at[4], first(1))
    send(t_o.at[lo_rows], tbuf_m, r1s.at[5], r1r.at[5], first(3))
    v = total(qp)
    tot[0] = v[0:256]
    t_p[256:512, :] = v[256:512].astype(BF)
    send(t_p.at[lo_rows], tfin.at[0, lo_rows], r1s.at[6], r1r.at[6], first(1))
    v = total(qm)
    tot[1] = v[256:512]
    t_m[0:256, :] = v[0:256].astype(BF)
    send(t_m.at[hi_rows], tfin.at[1, hi_rows], r1s.at[7], r1r.at[7], first(3))

    got(brecv.at[seven], k1r)
    bsum[...] = jnp.sum(brecv[...].astype(F32), axis=0).astype(BF)
    ball[z] = bsum[...]
    to_head(lambda k: copy(bsum, ball.at[z], k2s, k2r, at_head(k)))

    mine_w = total(q)
    got(tbuf_p, r1r.at[4])
    t_p[0:256, :] = (tot[0] + tbuf_p[...].astype(F32)).astype(BF)
    send(t_p.at[hi_rows], tfin.at[0, hi_rows], r2s.at[2], r2r.at[2], first(1))
    got(tbuf_m, r1r.at[5])
    t_m[256:512, :] = (tot[1] + tbuf_m[...].astype(F32)).astype(BF)
    send(t_m.at[lo_rows], tfin.at[1, lo_rows], r2s.at[3], r2r.at[3], first(3))

    got(gg_all.at[many], ggr)
    gg_ref[...] = jnp.sum(gg_all[...], axis=0)
    store(gg_ref, gg_hbm)
    got(call_.at[seven], c2r)
    for k in range(8):
        gc_ref[32 * k : 32 * k + 32, :] = call_[k]
    store(gc_ref, gc_hbm)
    got(rt_all.at[many], rtr)
    gr_ref[...] = jnp.sum(rt_all[...], axis=0)[:, 0:8]
    store(gr_ref, gr_hbm)

    got(tfin.at[0, lo_rows], r1r.at[6])
    got(tfin.at[1, hi_rows], r1r.at[7])
    got(tfin.at[0, hi_rows], r2r.at[2])
    got(tfin.at[1, lo_rows], r2r.at[3])
    gw_ref[...] = jnp.transpose(mine_w + tfin[0].astype(F32) + tfin[1].astype(F32))
    store(gw_ref, gw_hbm)
    got(ball.at[seven], k2r)
    for k in range(8):
        gb_ref[32 * k : 32 * k + 32, :] = ball[k].astype(F32)
    store(gb_ref, gb_hbm)

    def left(ref, sem):
        copy(ref, ref, sem, sem, partner).wait_send()

    for d in sent:
        d.wait_send()
    for d in stored:
        d.wait()
    for ref, sem in [
        (gg_all, ggs), (rt_all, rts),
    ]:
        left(ref.at[many], sem)
    for ref, sem in [(dec_all, des), (st_recv, a1s), (st_recv, a2s), (ad_recv, b1s), (ad_recv, b2s)]:
        left(ref.at[few], sem)
    for ref, sem in [(sq_all, sqs), (cr_all, crs), (crecv, c1s), (call_, c2s), (brecv, k1s), (ball, k2s)]:
        left(ref.at[seven], sem)


def hand_over(*refs):
    took = [pltpu.make_async_copy(refs[i], refs[16 + i], refs[24].at[i]) for i in range(8)]
    gave = [pltpu.make_async_copy(refs[16 + i], refs[8 + i], refs[24].at[8 + i]) for i in range(8)]
    for one in took:
        one.start()
    for one, other in zip(took, gave):
        one.wait()
        other.start()
    for one in gave:
        one.wait()


def on_device(
    inputs, gates, b_proj, c_proj, step_size, decay_rate, norm_gain, out_weight, grad_out
):
    V = pltpu.VMEM
    dma, reg = pltpu.SemaphoreType.DMA, pltpu.SemaphoreType.REGULAR
    scratch = [
        V((256, 512), BF), V((256, 512), BF), V((256, 128), F32), V((256, 128), F32),
        V((8, 256), F32), V((1, 8), F32), V((1, 512), F32), V((128, 512), F32), dma((8,)),
        V((256, 512), BF), V((256, 512), BF), V((256, 128), BF), V((256, 128), BF),
        V((8, 256), F32), V((1, 8), F32), V((1, 512), F32), V((128, 512), BF), V((256, 512), BF),
        V((8, 256, 512), BF), V((2, 4, 4, 128, 512), BF),
        V((1, 1, 512), F32), V((16, 1, 512), F32), V((1, 1, 512), F32), V((1, 1, 512), F32),
        V((128, 512), F32), V((16, 8, 256), F32), V((16, 8, 256), F32), V((128, 512), F32),
        V((128, 256), F32), V((128, 256), F32), V((128, 256), F32), V((128, 256), F32),
        V((128, 512), F32), V((16, 8, 256), F32), V((16, 8, 256), F32), V((128, 512), F32),
        V((128, 256), F32), V((128, 256), F32), V((128, 256), F32), V((128, 256), F32),
        V((1, 1, 256), F32), V((8, 1, 256), F32), V((1, 1, 256), F32), V((8, 1, 256), F32),
        V((4, 4, 512, 128), F32), V((4, 4, 512, 128), BF), V((4, 4, 512, 128), BF),
        V((4, 512, 128), BF), V((4, 512, 128), BF), V((4, 512, 128), BF),
        V((2, 512, 128), BF), V((2, 512, 128), BF), V((2, 4, 512, 128), BF),
        V((2, 256, 128), F32), V((512, 128), BF), V((512, 128), BF), V((512, 128), BF),
        V((256, 128), BF), V((256, 128), BF), V((2, 512, 128), BF),
        V((8, 32, 128), F32), V((8, 32, 128), F32), V((32, 128), F32), V((8, 32, 128), F32),
        V((8, 32, 128), BF), V((8, 32, 128), BF), V((32, 128), BF), V((8, 32, 128), BF),
        V((1, 1, 512), F32), V((32, 1, 512), F32), V((1, 1, 128), F32), V((32, 1, 128), F32),
        V((8, 128), F32), V((8, 256), F32), V((256, 128), F32), V((256, 128), F32),
        V((256, 512), F32), V((256, 512), F32), V((512, 512), BF),
        V((256, 256), F32), V((256, 256), F32),
        V((2, 128, 512), BF), V((2, 128, 1024), BF),
        V((256, 512), F32), V((256, 512), F32), V((256, 512), F32),
        V((256, 512), F32), V((256, 512), F32), V((256, 512), F32),
        V((256, 512), BF), V((512, 256), BF),
        V((256, 512), BF), V((256, 512), BF), V((512, 512), BF), V((256, 1024), BF),
        V((256, 128), F32), V((256, 256), F32), V((256, 128), F32), V((8, 256), F32),
        V((256, 512), F32), V((2, 256, 512), BF), V((256, 1024), F32),
        reg, reg, reg, reg, reg, reg, reg, dma((9,)), dma((5,)), dma((5,)), dma((2, 4, 2)), dma((2, 4, 2)), dma((4,)), dma((4,)), dma((2, 5)), dma((2, 5)),
        dma((2, 4)), dma((2, 4)), dma((4,)), dma((4,)),
        dma, dma, dma, dma, dma, dma, dma, dma, dma, dma, dma, dma, dma, dma,
        dma((4,)), dma((4,)), dma((8,)), dma((8,)), dma((4,)), dma((4,)),
        dma, dma, dma, dma, dma, dma, dma, dma, dma, dma, dma, dma,
    ]
    outs = (
        jax.ShapeDtypeStruct((256, 512), BF),
        jax.ShapeDtypeStruct((256, 512), BF),
        jax.ShapeDtypeStruct((256, 128), F32),
        jax.ShapeDtypeStruct((256, 128), F32),
        jax.ShapeDtypeStruct((8, 256), F32),
        jax.ShapeDtypeStruct((1, 8), F32),
        jax.ShapeDtypeStruct((1, 512), F32),
        jax.ShapeDtypeStruct((128, 512), F32),
    )
    far = pl.BlockSpec(memory_space=pltpu.HBM)
    results = pl.pallas_call(
        kernel,
        out_shape=outs,
        in_specs=[far] * 9,
        out_specs=[far] * 8,
        scratch_shapes=scratch,
        compiler_params=pltpu.CompilerParams(
            collective_id=0, has_side_effects=True, vmem_limit_bytes=60000000
        ),
    )(
        inputs, gates, b_proj, c_proj, step_size, decay_rate.reshape(1, 8),
        norm_gain.reshape(1, 512), out_weight, grad_out,
    )
    gx, gz, gb, gc, gs, gr, gg, gw = pl.pallas_call(
        hand_over,
        out_shape=outs,
        in_specs=[far] * 8,
        out_specs=[far] * 8,
        scratch_shapes=[V(o.shape, o.dtype) for o in outs] + [dma((16,))],
        compiler_params=pltpu.CompilerParams(vmem_limit_bytes=60000000),
    )(*results)
    return gx, gz, gb, gc, gs, gr.reshape(8), gg.reshape(512), gw


def solution(mesh):
    split = Mesh(
        mesh.devices.reshape(4, 4, 2, mesh.shape["head"]), ("seq_0", "seq_1", "seq_2", "head")
    )
    return jax.shard_map(
        on_device,
        mesh=split,
        in_specs=(
            P(SEQ, "head"), P(SEQ, "head"), P(SEQ, None), P(SEQ, None), P("head", SEQ),
            P("head"), P("head"), P(SEQ, "head"), P(SEQ, "head"),
        ),
        out_specs=(
            P(SEQ, "head"), P(SEQ, "head"), P(SEQ, None), P(SEQ, None), P("head", SEQ),
            P("head"), P("head"), P(SEQ, "head"),
        ),
        check_vma=False,
    )
```

```python
import jax
import jax.numpy as jnp
from jax import lax
from jax.experimental import pallas as pl
from jax.experimental.pallas import tpu as pltpu
from jax.sharding import Mesh
from jax.sharding import PartitionSpec as P

SEQ = ("seq_0", "seq_1", "seq_2")
EPSILON = 1e-05
MESH = pl.DeviceIdType.MESH
BF = jnp.bfloat16
F32 = jnp.float32


def mm(a, b):
    return jnp.dot(a, b, preferred_element_type=F32)


def nt(a, b):
    return lax.dot_general(a, b, (((1,), (1,)), ((), ())), preferred_element_type=F32)


def split2(v):
    hi = v.astype(BF)
    return hi, (v - hi.astype(F32)).astype(BF)


def split3(v):
    hi = v.astype(BF)
    rest = v - hi.astype(F32)
    mid = rest.astype(BF)
    return hi, mid, (rest - mid.astype(F32)).astype(BF)


def lanes(*parts):
    return jnp.concatenate(parts, axis=1)


def rows(*parts):
    return jnp.concatenate(parts, axis=0)


ORDER = (2, 1, 3, 0)


def kernel(
    x_hbm, z_hbm, b_hbm, c_hbm, step_hbm, rate_hbm, gain_hbm, w_hbm, g_hbm,
    gx_hbm, gz_hbm, gb_hbm, gc_hbm, gs_hbm, gr_hbm, gg_hbm, gw_hbm,
    gx_ref, gz_ref, gb_ref, gc_ref, gs_ref, gr_ref, gg_ref, gw_ref, outs,
    x_ref, z_ref, b_ref, c_ref, step_ref, rate_ref, gain_ref, w_ref, g_ref,
    gfull, wbuf, dec_src, dec_all, dec_par, dec_two, st_send, st_recv, st_pref, st_in,
    st_other, st_pair, st_half, st_give,
    ad_send, ad_recv, ad_pref, ad_in, ad_other, ad_pair, ad_half, ad_give, sq_src, sq_all, cr_src, cr_all,
    pt_own, pt_send, pt_recv, rs_o, rs_p, rs_m, buf_p, buf_m, fin,
    tot, t_o, t_p, t_m, tbuf_p, tbuf_m, tfin,
    cpart, crecv, csum, call_, bpart, brecv, bsum, ball,
    gg_src, gg_all, rt_src, rt_all,
    rate_c, lg, lgt, stept, fr, stl, xs2, sc, sct, mix_t, mix_b, ybuf, ycs, gn,
    ubuf, silb, ydb, nb, ntr, ehi, elo, ef2, rprod, colst, ws, qcol, rowp, gxi, mixw, pprod,
    kx, ky, kyy, kc, kz1, kz2, kz3, ins, prs, prr, zs, zr, w1s, w1r, w2s, w2r, wfs, wfr, wds, wdr, des, der, a1s, a1r, a2s, a2r,
    b1s, b1r, b2s, b2r, sqs, sqr, crs, crr, d0s, d0r, r1s, r1r, r2s, r2r,
    c1s, c1r, c2s, c2r, k1s, k1r, k2s, k2r, ggs, ggr, rts, rtr,
):
    y = lax.axis_index("seq_0")
    x = lax.axis_index("seq_1")
    c = lax.axis_index("seq_2")
    z = lax.axis_index("head")
    me = (y * 4 + x) * 2 + c
    oc = 1 - c
    q = x * oc + y * c
    p = y * oc + x * c
    rem, div = lax.rem, lax.div

    def at_head(k):
        return (y, x, c, k)

    def first(d):
        return (rem(y + d * c, 4), rem(x + d * oc, 4), c, z)

    def second(d):
        return (rem(y + d * oc, 4), rem(x + d * c, 4), c, z)

    partner = (y, x, oc, z)

    def copy(src, dst, ssem, rsem, dev):
        return pltpu.make_async_remote_copy(
            src_ref=src, dst_ref=dst, send_sem=ssem, recv_sem=rsem,
            device_id=dev, device_id_type=MESH,
        )

    def got(ref, sem):
        copy(ref, ref, sem, sem, partner).wait_recv()

    sent, stored = [], []

    def store(src, dst):
        one = pltpu.make_async_copy(src, dst, outs.at[len(stored)])
        one.start()
        stored.append(one)

    def send(src, dst, ssem, rsem, dev):
        d = copy(src, dst, ssem, rsem, dev)
        d.start()
        sent.append(d)

    far_first = sorted(
        ((dy, dx, dc) for dy in range(4) for dx in range(4) for dc in range(2)),
        key=lambda o: -(min(o[0], 4 - o[0]) + min(o[1], 4 - o[1])) - 0.1 * o[2],
    )
    ys, xs, cs = [rem(y + d, 4) for d in range(4)], [rem(x + d, 4) for d in range(4)], (c, oc)
    peers = [
        ((ys[dy], xs[dx], cs[dc], z), (ys[dy] * 4 + xs[dx]) * 2 + cs[dc])
        for dy, dx, dc in far_first
        if (dy, dx, dc) != (0, 0, 0)
    ]

    chips = [
        ((ys[dy], xs[dx], c, z), ys[dy] * 4 + xs[dx])
        for dy, dx, dc in far_first
        if dc == 0 and (dy, dx) != (0, 0)
    ]
    here = y * 4 + x

    def to_chips(make):
        for dev, k in chips:
            make(dev, k).start()

    def to_seq(make):
        for dev, k in peers:
            make(dev, k).start()

    def to_head(make):
        for d in (4, 3, 5, 2, 6, 1, 7):
            make(rem(z + d, 8)).start()

    near_x = [(y, rem(x + d, 4), c, z) for d in (1, 3)]
    near_y = [(rem(y + d, 4), x, c, z) for d in (1, 3)]
    near_z = [(y, x, c, rem(z + d, 8)) for d in (1, 7)]

    def tell(sem, devices):
        for dev in devices:
            pl.semaphore_signal(sem, inc=1, device_id=dev, device_id_type=MESH)

    barrier = pltpu.get_barrier_semaphore()
    fetches = [
        pltpu.make_async_copy(src, dst, ins.at[i])
        for i, (src, dst) in enumerate((
            (g_hbm, g_ref), (w_hbm, w_ref), (step_hbm, step_ref), (rate_hbm, rate_ref),
            (b_hbm, b_ref), (x_hbm, x_ref), (c_hbm, c_ref), (gain_hbm, gain_ref), (z_hbm, z_ref),
        ))
    ]
    for f in fetches:
        f.start()
    tell(barrier, near_z + near_x + near_y + [partner])
    for f in fetches[:2]:
        f.wait()
    pl.semaphore_wait(barrier, 7)
    tell(kx, near_x)
    tell(kz1, near_z)

    qm, qp, q2 = rem(q + 3, 4), rem(q + 1, 4), rem(q + 2, 4)
    pm, pp, p2 = rem(p + 3, 4), rem(p + 1, 4), rem(p + 2, 4)
    top, low = pl.ds(0, 64), pl.ds(64, 64)
    both_z, both_4 = ((0, 1), (1, 7)), ((0, 1), (1, 3))
    for n in range(2):
        for side, d in both_z:
            k = n if side == 0 else 1 - n
            rk = pl.ds(128 * k, 128)
            send(g_ref.at[rk], gfull.at[z, rk], zs.at[side, 0, k], zr.at[side, 0, k], at_head(rem(z + d, 8)))
    for side, d in both_4:
        send(w_ref, wbuf.at[c, p, q], w1s.at[side], w1r.at[side], first(d))
    for side, d in both_4:
        send(w_ref, wbuf.at[c, p, q], w2s.at[side, 0], w2r.at[side, 0], second(d))
    gfull[z] = g_ref[...]
    wbuf[c, p, q] = w_ref[...]

    for f in fetches[2:5]:
        f.wait()

    i8 = lax.broadcasted_iota(jnp.int32, (8, 8), 0)
    j8 = lax.broadcasted_iota(jnp.int32, (8, 8), 1)
    rate = jnp.sum(jnp.where(i8 == j8, jnp.broadcast_to(rate_ref[...], (8, 8)), 0.0), axis=1, keepdims=True)
    rate_c[...] = jnp.broadcast_to(rate, (8, 128))
    step = step_ref[...]
    ia = lax.broadcasted_iota(jnp.int32, (256, 256), 0)
    ib = lax.broadcasted_iota(jnp.int32, (256, 256), 1)
    tri_u = jnp.where(ia <= ib, 1.0, 0.0).astype(BF)
    v1, v2, v3 = split3(rate * step)
    logs = -(mm(v1, tri_u) + mm(v2, tri_u) + mm(v3, tri_u))
    lg[...] = logs
    logs_t = jnp.transpose(logs)
    step_t = jnp.transpose(step)
    lgt[:, 0:8] = logs_t
    stept[:, 0:8] = step_t
    e8 = jnp.where(
        lax.broadcasted_iota(jnp.int32, (8, 512), 0)
        == lax.broadcasted_iota(jnp.int32, (8, 512), 1) // 64, 1.0, 0.0,
    ).astype(BF)

    def spread_heads(v):
        a1, a2, a3 = split3(v)
        return mm(a1, e8) + mm(a2, e8) + mm(a3, e8)

    fr[...] = spread_heads(jnp.exp(logs_t))
    stl[...] = spread_heads(step_t * jnp.exp(logs_t[255:256, :] - logs_t))
    dec_src[0] = fr[255:256, :]
    bt = b_ref[...].T
    fetches[5].wait()
    pl.semaphore_wait(kx, 2)
    tell(ky, near_y)
    for r in range(4):
        rs = slice(64 * r, 64 * r + 64)
        hi, lo = split2(x_ref[rs, :].astype(F32) * stl[rs, :])
        xs2[rs, :] = hi
        xs2[64 * r + 256 : 64 * r + 320, :] = lo
    st_send[...] = mm(lanes(bt, bt), xs2[...])
    for f in fetches[6:]:
        f.wait()

    hc = pl.ds(pl.multiple_of(256 * c, 256), 256)
    ho = pl.ds(pl.multiple_of(256 * oc, 256), 256)

    def eight(ref, k):
        return ref.at[pl.ds(pl.multiple_of(8 * k, 8), 8)]

    send(dec_src.at[0], dec_par.at[0], prs.at[4], prr.at[4], partner)
    send(st_send.at[:, ho], st_other, prs.at[0], prr.at[0], partner)
    iota_i = lax.broadcasted_iota(jnp.int32, (64, 256), 0)
    iota_j = lax.broadcasted_iota(jnp.int32, (64, 256), 1)
    ct = c_ref[...].T
    raw = mm(c_ref[...], bt)
    for r in range(4):
        rs = slice(64 * r, 64 * r + 64)
        sc[rs, :] = jnp.where(iota_i + 64 * r >= iota_j, raw[rs, :], 0.0)
    sct[...] = mm(b_ref[...], ct)

    got(wbuf.at[c, p, qm], w1r.at[0])
    send(wbuf.at[c, p, qm, top], wbuf.at[c, p, qm, top], w1s.at[2], w1r.at[2], first(1))
    for side, d in both_4:
        send(wbuf.at[c, p, qm], wbuf.at[c, p, qm], w2s.at[side, 1], w2r.at[side, 1], second(d))
    got(wbuf.at[c, p, qp], w1r.at[1])
    send(wbuf.at[c, p, qp, low], wbuf.at[c, p, qp, low], w1s.at[3], w1r.at[3], first(3))
    for side, d in both_4:
        send(wbuf.at[c, p, qp], wbuf.at[c, p, qp], w2s.at[side, 2], w2r.at[side, 2], second(d))

    pl.semaphore_wait(ky, 2)
    tell(kyy, near_y)
    got(dec_par.at[0], prr.at[4])
    d_own, d_par = dec_src[0, :, hc], dec_par[0, :, hc]
    d_0, d_1 = jnp.where(c == 0, d_own, d_par), jnp.where(c == 0, d_par, d_own)
    got(st_other, prr.at[0])
    own, other = st_send[:, hc], st_other[...]
    l_0, l_1 = jnp.where(c == 0, own, other), jnp.where(c == 0, other, own)
    st_pair[...] = l_1 + d_1 * l_0
    dec_two[0] = dec_src[0] * dec_par[0]
    dec_all[here] = dec_two[0]
    pl.semaphore_wait(kyy, 2)
    tell(kc, [partner])
    to_chips(lambda dev, k: copy(dec_two.at[0], dec_all.at[here], des, der, dev))
    to_chips(lambda dev, k: copy(eight(st_pair, k), st_recv.at[here], a1s, a1r, dev))
    st_recv[here] = eight(st_pair, here)[...]

    half = lax.broadcasted_iota(jnp.int32, (1, 128), 1)
    keep = (
        jnp.where(half < 64, 1.0, 0.0).astype(BF),
        jnp.where(half < 64, 0.0, 1.0).astype(BF),
    )

    def inside(hp):
        ls = slice(128 * hp, 128 * hp + 128)
        mt, mb = mix_t.at[hp % 2], mix_b.at[hp % 2]
        xp = x_ref[:, ls]
        x0, x1 = xp * keep[0], xp * keep[1]
        for k in range(2):
            h = 2 * hp + k
            for r in range(4):
                rs = slice(64 * r, 64 * r + 64)
                wd = 128 if r < 2 else 256
                t = jnp.exp(jnp.minimum(lgt[rs, h : h + 1] - lg[h : h + 1, 0:wd], 0.0))
                hi, lo = split2(t * (sc[rs, 0:wd] * step_ref[h : h + 1, 0:wd]))
                dst = mt if r < 2 else mb
                rr = slice(64 * (r % 2), 64 * (r % 2) + 64)
                dst[rr, 2 * k * wd : (2 * k + 1) * wd] = hi
                dst[rr, (2 * k + 1) * wd : (2 * k + 2) * wd] = lo
        ybuf[0:128, ls] = mm(mt[...], rows(x0[0:128], x0[0:128], x1[0:128], x1[0:128]))
        ybuf[128:256, ls] = mm(mb[...], rows(x0, x0, x1, x1))

    def z_block(side, j):
        return rem(z + 8 - j, 8) if side == 0 else rem(z + j, 8)

    def z_forward(j, n):
        for side, d in both_z:
            k = n if side == 0 else 1 - n
            blk = gfull.at[z_block(side, j), pl.ds(128 * k, 128)]
            got(blk, zr.at[side, j - 1, k])
            if j < 3 or n == 0:
                send(blk, blk, zs.at[side, j, k], zr.at[side, j, k], at_head(rem(z + d, 8)))

    spots = (q, qm, qp, q2, q2)

    def w_forward(slot):
        for side, row in ((0, pm), (1, pp)):
            if slot < 3:
                blk = wbuf.at[c, row, spots[slot]]
                part = blk.at[top if side == 0 else low]
                on = True
            else:
                blk = part = wbuf.at[c, row, q2, top if slot == 3 else low]
                on = slot == 3 + side
            got(blk, w2r.at[side, slot])
            if on:
                n = min(slot, 3)
                send(part, part, wfs.at[side, n], wfr.at[side, n], second(1 if side == 0 else 3))

    def w_second_of_opposite():
        for n, piece in ((0, top), (1, low)):
            blk = wbuf.at[c, p, q2, piece]
            got(blk, w1r.at[2 + n])
            for side, d in both_4:
                send(blk, blk, w2s.at[side, 3 + n], w2r.at[side, 3 + n], second(d))

    def to_partner(n, i2):
        send(wbuf.at[c, i2], wbuf.at[c, i2], wds.at[n], wdr.at[n], partner)

    def scan(recv, pref, back):
        s = jnp.zeros((8, 256), F32)
        for k in reversed(range(16)) if back else range(16):
            pref[k] = s
            s = s * dec_all[k, :, hc] + recv[k]

    many, few = pl.ds(0, 31), pl.ds(0, 15)

    inside(0)
    w_forward(0)
    pl.semaphore_wait(kz1, 2)
    tell(kz2, near_z)
    z_forward(1, 0)
    w_second_of_opposite()
    to_partner(0, p)
    inside(1)
    z_forward(1, 1)
    got(dec_all.at[few], der)
    got(st_recv.at[few], a1r)
    scan(st_recv, st_pref, False)
    to_chips(lambda dev, k: copy(st_pref.at[k], eight(st_half, here), a2s, a2r, dev))
    eight(st_half, here)[...] = st_pref[here]
    w_forward(1)
    w_forward(2)
    inside(2)
    pl.semaphore_wait(kz2, 2)
    tell(kz3, near_z)
    z_forward(2, 0)
    w_forward(3)
    w_forward(4)
    to_partner(1, pm)
    to_partner(2, pp)
    inside(3)
    z_forward(2, 1)
    z_forward(3, 0)
    for n in range(4):
        i1 = (q, qm, qp, q2)[n]
        got(wbuf.at[c, p2, i1, top], wfr.at[0, n])
        got(wbuf.at[c, p2, i1, low], wfr.at[1, n])
        blk = wbuf.at[c, p2, i1]
        send(blk, blk, wds.at[3 + n], wdr.at[3 + n], partner)

    got(st_recv.at[few], a2r)
    enter = st_half[...]
    later = d_0 * enter + jnp.where(c == 0, st_send[:, hc], st_other[...])
    st_give[...] = jnp.where(c == 0, later, enter)
    send(st_give, st_in.at[:, hc], prs.at[1], prr.at[1], partner)
    st_in[:, hc] = jnp.where(c == 0, enter, later)
    got(st_in.at[:, ho], prr.at[1])
    s_hi, s_lo = split2(st_in[...])
    cc = lanes(c_ref[...], c_ref[...])
    gain = gain_ref[...]

    def folded(v):
        return v[:, 0:128] + v[:, 128:256] + v[:, 256:384] + v[:, 384:512]

    for r in range(4):
        rs = slice(64 * r, 64 * r + 64)
        v = fr[rs, :] * mm(cc[rs, :], rows(s_hi, s_lo))
        ycs[rs, :] = v
        ybuf[rs, :] = ybuf[rs, :] + v
    for r in range(8):
        rs = slice(32 * r, 32 * r + 32)
        zf = z_ref[rs, :].astype(F32)
        yv = ybuf[rs, :]
        s = 1.0 / (1.0 + jnp.exp(-zf))
        sil = zf * s
        u = yv * sil
        ubuf[rs, :] = u
        silb[rs, :] = sil
        ydb[rs, :] = yv * s * (1.0 + zf * (1.0 - s))
        pprod[rs, 0:128] = folded(u * u)
    sq = jnp.sum(jnp.transpose(pprod[:, 0:128]), axis=0, keepdims=True)
    sq_src[0] = sq
    sq_all[z] = sq
    pl.semaphore_wait(kz3, 2)
    to_head(lambda k: copy(sq_src.at[0], sq_all.at[z], sqs, sqr, at_head(k)))

    z_forward(3, 1)
    for n in range(3):
        got(wbuf.at[oc, p], wdr.at[n])
    for n in range(4):
        got(wbuf.at[oc, p, q], wdr.at[3 + n])

    gn[...] = jnp.zeros((256, 512), F32)

    def add_block(h):
        yy, xx = div(h, 2), 2 * rem(h, 2)
        rhs = rows(wbuf[0, yy, xx], wbuf[1, xx, yy], wbuf[0, yy, xx + 1], wbuf[1, xx + 1, yy])
        gn[...] = gn[...] + mm(gfull[h], rhs)

    def one_block(d, carry):
        add_block(rem(z + 5 + d, 8))
        return carry

    lax.fori_loop(0, 7, one_block, 0)
    for side in range(2):
        got(gfull.at[z_block(side, 4), pl.ds(128 * side, 128)], zr.at[side, 3, side])
    add_block(rem(z + 4, 8))
    for r in range(8):
        rs = slice(32 * r, 32 * r + 32)
        pprod[rs, 128:256] = folded(gn[rs, :] * gain * ubuf[rs, :])
    cr = jnp.sum(jnp.transpose(pprod[:, 128:256]), axis=0, keepdims=True)
    cr_src[0] = cr
    cr_all[z] = cr
    to_head(lambda k: copy(cr_src.at[0], cr_all.at[z], crs, crr, at_head(k)))

    seven = pl.ds(0, 7)
    got(sq_all.at[seven], sqr)
    inv_row = lax.rsqrt(jnp.sum(sq_all[...], axis=0) / 4096.0 + EPSILON)
    zero7 = jnp.zeros((7, 256), F32)
    colst[:, 0:8] = jnp.transpose(rows(inv_row, zero7))
    gg_acc = jnp.zeros((8, 512), F32)
    for r in range(8):
        rs = slice(32 * r, 32 * r + 32)
        ui = ubuf[rs, :] * colst[rs, 0:1]
        nb[rs, :] = (ui * gain).astype(BF)
        gg_acc = gg_acc + jnp.sum((gn[rs, :] * ui).reshape(4, 8, 512), axis=0)
    ntr[...] = nb[...].T

    for n in range(4):
        i2 = rem(q + ORDER[n], 4)

        def one_chip(i1, carry, i2=i2):
            yy, xx = i2 * c + i1 * oc, i1 * c + i2 * oc
            blk = 2 * yy + div(xx, 2)
            base = rem(xx, 2) * 256
            mine = gfull[blk, :, pl.ds(pl.multiple_of(base + 128 * c, 128), 128)]
            other = gfull[blk, :, pl.ds(pl.multiple_of(base + 128 * oc, 128), 128)]
            both = mm(ntr[...], lanes(mine, other))
            pt_own[yy * oc + xx * c, xx * oc + yy * c] = both[:, 0:128]
            pt_send[i2, i1] = both[:, 128:256].astype(BF)
            return carry

        lax.fori_loop(0, 4, one_chip, 0)
        send(pt_send.at[i2], pt_recv.at[i2], d0s.at[n], d0r.at[n], partner)

    gg_src[0] = jnp.sum(gg_acc, axis=0, keepdims=True)
    gg_all[me] = gg_src[0]
    ab, cd = pl.ds(0, 2), pl.ds(2, 2)
    got(pt_recv.at[p2], d0r.at[0])
    for i in range(4):
        rs_o[i] = (pt_own[p2, i] + pt_recv[p2, i].astype(F32)).astype(BF)
    send(rs_o.at[ab], buf_p, r1s.at[0], r1r.at[0], second(1))
    send(rs_o.at[cd], buf_m, r1s.at[1], r1r.at[1], second(3))

    got(cr_all.at[seven], crr)
    coef_row = inv_row * inv_row * (jnp.sum(cr_all[...], axis=0) / 4096.0)
    colst[:, 8:16] = jnp.transpose(rows(coef_row, zero7))
    for r in range(8):
        rs = slice(32 * r, 32 * r + 32)
        gu = colst[rs, 0:1] * (gn[rs, :] * gain - ubuf[rs, :] * colst[rs, 8:9])
        gz_ref[rs, :] = (gu * ydb[rs, :]).astype(BF)
        e = gu * silb[rs, :]
        hi, lo = split2(e)
        ehi[rs, :] = hi
        elo[rs, :] = lo
        hi, lo = split2(e * fr[rs, :])
        ef2[rs, :] = hi
        ef2[256 + 32 * r : 288 + 32 * r, :] = lo
        hi, lo = split2(e * ycs[rs, :])
        rprod[rs, 0:512] = hi
        rprod[rs, 512:1024] = lo
    ad_send[...] = mm(lanes(ct, ct), ef2[...])
    send(ad_send.at[:, ho], ad_other, prs.at[2], prr.at[2], partner)
    store(gz_ref, gz_hbm)
    got(pt_recv.at[pp], d0r.at[1])
    for i in range(4):
        v = pt_own[pp, i] + pt_recv[pp, i].astype(F32)
        if i < 2:
            pt_own[pp, i] = v
        else:
            rs_p[i] = v.astype(BF)
    got(pt_recv.at[pm], d0r.at[2])
    for i in range(4):
        v = pt_own[pm, i] + pt_recv[pm, i].astype(F32)
        if i < 2:
            rs_m[i] = v.astype(BF)
        else:
            pt_own[pm, i] = v
    got(ad_other, prr.at[2])
    own, other = ad_send[:, hc], ad_other[...]
    ad_pair[...] = jnp.where(c == 0, own, other) + d_0 * jnp.where(c == 0, other, own)
    to_chips(lambda dev, k: copy(eight(ad_pair, k), ad_recv.at[here], b1s, b1r, dev))
    ad_recv[here] = eight(ad_pair, here)[...]
    pl.semaphore_wait(kc, 1)
    to_seq(lambda dev, k: copy(gg_src.at[0], gg_all.at[me], ggs, ggr, dev))
    send(rs_p.at[cd], fin.at[0, cd], r1s.at[2], r1r.at[2], second(1))
    send(rs_m.at[ab], fin.at[1, ab], r1s.at[3], r1r.at[3], second(3))

    mask_t = (iota_j >= iota_i, iota_j >= iota_i + 64)
    mask_b = (iota_j[:, 0:128] >= iota_i[:, 0:128], iota_j[:, 0:128] >= iota_i[:, 0:128] + 64)

    def inside_back(hp):
        ls = slice(128 * hp, 128 * hp + 128)
        mw = mixw.at[hp % 2]
        xp = x_ref[:, ls]
        eh, el = ehi[:, ls], elo[:, ls]
        e2 = lanes(eh, el)
        for k in range(2):
            h = 2 * hp + k
            xk = xp * keep[k]
            x2 = lanes(xk, xk)
            inner_t = nt(x2[0:128], e2)
            inner_b = nt(x2[128:256], e2[128:256])
            racc_l = jnp.zeros((1, 128), F32)
            racc_r = jnp.zeros((1, 128), F32)
            for r in range(4):
                rs = slice(64 * r, 64 * r + 64)
                rr = slice(64 * (r % 2), 64 * (r % 2) + 64)
                cs = slice(0, 256) if r < 2 else slice(128, 256)
                t = jnp.exp(jnp.minimum(lg[h : h + 1, cs] - lgt[rs, h : h + 1], 0.0))
                tab = jnp.where(mask_t[r] if r < 2 else mask_b[r - 2], t, 0.0)
                inner = inner_t[rr] if r < 2 else inner_b[rr]
                st = sct[rs, cs]
                sj = stept[rs, h : h + 1]
                w = tab * inner
                sw = w * sj
                if r < 2:
                    mw[rr, 256 * k : 256 * k + 256] = (tab * st * sj).astype(BF)
                else:
                    mw[128 + 64 * (r - 2) : 192 + 64 * (r - 2), 128 * k : 128 * k + 128] = (tab * st * sj).astype(BF)
                qcol[rs, h : h + 1] = jnp.sum(w * st, axis=1, keepdims=True)
                if h == 0:
                    ws[rs, cs] = sw
                else:
                    ws[rs, cs] = ws[rs, cs] + sw
                rsum = jnp.sum(sw * st, axis=0, keepdims=True)
                if r < 2:
                    racc_l = racc_l + rsum[:, 0:128]
                    racc_r = racc_r + rsum[:, 128:256]
                else:
                    racc_r = racc_r + rsum
            rowp[h : h + 1, 0:128] = racc_l
            rowp[h : h + 1, 128:256] = racc_r
        em0, em1 = lanes(eh * keep[0], el * keep[0]), lanes(eh * keep[1], el * keep[1])
        v = mm(mw[0:128, :], rows(em0, em1))
        gxi[0:128, ls] = v[:, 0:128] + v[:, 128:256]
        v = mm(mw[128:256, 0:256], rows(em0[128:256], em1[128:256]))
        gxi[128:256, ls] = v[:, 0:128] + v[:, 128:256]

    for hp in range(4):
        inside_back(hp)

    got(ad_recv.at[few], b1r)
    scan(ad_recv, ad_pref, True)
    to_chips(lambda dev, k: copy(ad_pref.at[k], eight(ad_half, here), b2s, b2r, dev))
    eight(ad_half, here)[...] = ad_pref[here]

    got(buf_p, r1r.at[0])
    for i in range(2):
        rs_p[i] = (pt_own[pp, i] + buf_p[i].astype(F32)).astype(BF)
    send(rs_p.at[ab], fin.at[0, ab], r2s.at[0], r2r.at[0], second(1))
    got(buf_m, r1r.at[1])
    for i in range(2):
        rs_m[2 + i] = (pt_own[pm, 2 + i] + buf_m[i].astype(F32)).astype(BF)
    send(rs_m.at[cd], fin.at[1, cd], r2s.at[1], r2r.at[1], second(3))

    ws[128:256, 0:128] = jnp.zeros((128, 128), F32)
    w_hi, w_lo = split2(jnp.transpose(ws[...]))
    gq = mm(lanes(w_hi, w_lo), rows(b_ref[...], b_ref[...]))
    gq = gq + nt(lanes(ef2[0:256], ef2[256:512], ef2[0:256]), lanes(s_hi, s_hi, s_lo))
    for k in range(8):
        cpart[k] = gq[32 * k : 32 * k + 32]
    crecv[z] = cpart[z]
    to_head(lambda k: copy(cpart.at[k], crecv.at[z], c1s, c1r, at_head(k)))
    w_hi, w_lo = split2(ws[...])
    gk = mm(lanes(w_hi, w_lo), rows(c_ref[...], c_ref[...]))

    got(pt_recv.at[p], d0r.at[3])
    for i in range(4):
        pt_own[p, i] = pt_own[p, i] + pt_recv[p, i].astype(F32)
    e16 = lanes(e8, e8)
    rstate = nt(e16, rprod[...])

    got(ad_recv.at[few], b2r)
    enter = ad_half[...]
    sooner = jnp.where(c == 0, ad_other[...], ad_send[:, hc]) + d_1 * enter
    ad_give[...] = jnp.where(c == 0, enter, sooner)
    send(ad_give, ad_in.at[:, hc], prs.at[3], prr.at[3], partner)
    ad_in[:, hc] = jnp.where(c == 0, sooner, enter)
    got(ad_in.at[:, ho], prr.at[3])
    a_hi, a_lo = split2(ad_in[...])
    gk = gk + nt(lanes(xs2[0:256], xs2[256:512], xs2[0:256]), lanes(a_hi, a_hi, a_lo))
    for k in range(8):
        bpart[k] = gk[32 * k : 32 * k + 32].astype(BF)
    brecv[z] = bpart[z]
    to_head(lambda k: copy(bpart.at[k], brecv.at[z], k1s, k1r, at_head(k)))
    got(crecv.at[seven], c1r)
    csum[...] = jnp.sum(crecv[...], axis=0)
    call_[z] = csum[...]
    to_head(lambda k: copy(csum, call_.at[z], c2s, c2r, at_head(k)))

    for r in range(4):
        rs = slice(64 * r, 64 * r + 64)
        ka = mm(lanes(b_ref[rs, :], b_ref[rs, :]), rows(a_hi, a_lo))
        gx_ref[rs, :] = (gxi[rs, :] + stl[rs, :] * ka).astype(BF)
        hi, lo = split2(x_ref[rs, :].astype(F32) * ka)
        pprod[rs, 0:512] = hi.astype(F32)
        pprod[rs, 512:1024] = lo.astype(F32)
    carr = nt(e16, pprod[...].astype(BF))
    store(gx_ref, gx_hbm)
    held = jnp.sum((ad_in[...] * st_in[...]).reshape(16, 8, 512), axis=0)
    h_hi, h_lo = split2(held)
    held8 = jnp.sum(nt(e16, lanes(h_hi, h_lo)), axis=1, keepdims=True)
    logs = lg[...]
    step = step_ref[...]
    rate = rate_c[:, 0:1]
    tail = jnp.exp(logs[:, 255:256] - logs)
    q_in = jnp.transpose(qcol[...])[0:8, :]
    tc = tail * carr
    q_terms = q_in + tc
    drive = rowp[...] + rstate - step * q_terms
    boundary = jnp.exp(logs[:, 255:256]) * held8 + jnp.sum(step * tc, axis=1, keepdims=True)
    tri_l = jnp.where(ia >= ib, 1.0, 0.0).astype(BF)
    v1, v2, v3 = split3(drive)
    log_grad = mm(v1, tri_l) + mm(v2, tri_l) + mm(v3, tri_l) + boundary
    gs_ref[...] = q_terms - rate * log_grad
    rp = -jnp.sum(step * log_grad, axis=1, keepdims=True)
    d0 = lax.broadcasted_iota(jnp.int32, (8, 128), 0)
    d1 = lax.broadcasted_iota(jnp.int32, (8, 128), 1)
    rt_src[0] = jnp.sum(jnp.where(d0 == d1, rp, 0.0), axis=0, keepdims=True)
    rt_all[me] = rt_src[0]
    to_seq(lambda dev, k: copy(rt_src.at[0], rt_all.at[me], rts, rtr, dev))
    store(gs_ref, gs_hbm)

    got(fin.at[0, cd], r1r.at[2])
    got(fin.at[1, ab], r1r.at[3])
    got(fin.at[0, ab], r2r.at[0])
    got(fin.at[1, cd], r2r.at[1])

    def total(i):
        return pt_own[p, i] + fin[0, i].astype(F32) + fin[1, i].astype(F32)

    hi_rows, lo_rows = pl.ds(0, 256), pl.ds(256, 256)
    t_o[...] = total(q2).astype(BF)
    send(t_o.at[hi_rows], tbuf_p, r1s.at[4], r1r.at[4], first(1))
    send(t_o.at[lo_rows], tbuf_m, r1s.at[5], r1r.at[5], first(3))
    v = total(qp)
    tot[0] = v[0:256]
    t_p[256:512, :] = v[256:512].astype(BF)
    send(t_p.at[lo_rows], tfin.at[0, lo_rows], r1s.at[6], r1r.at[6], first(1))
    v = total(qm)
    tot[1] = v[256:512]
    t_m[0:256, :] = v[0:256].astype(BF)
    send(t_m.at[hi_rows], tfin.at[1, hi_rows], r1s.at[7], r1r.at[7], first(3))

    got(brecv.at[seven], k1r)
    bsum[...] = jnp.sum(brecv[...].astype(F32), axis=0).astype(BF)
    ball[z] = bsum[...]
    to_head(lambda k: copy(bsum, ball.at[z], k2s, k2r, at_head(k)))

    mine_w = total(q)
    got(tbuf_p, r1r.at[4])
    t_p[0:256, :] = (tot[0] + tbuf_p[...].astype(F32)).astype(BF)
    send(t_p.at[hi_rows], tfin.at[0, hi_rows], r2s.at[2], r2r.at[2], first(1))
    got(tbuf_m, r1r.at[5])
    t_m[256:512, :] = (tot[1] + tbuf_m[...].astype(F32)).astype(BF)
    send(t_m.at[lo_rows], tfin.at[1, lo_rows], r2s.at[3], r2r.at[3], first(3))

    got(gg_all.at[many], ggr)
    gg_ref[...] = jnp.sum(gg_all[...], axis=0)
    store(gg_ref, gg_hbm)
    got(call_.at[seven], c2r)
    for k in range(8):
        gc_ref[32 * k : 32 * k + 32, :] = call_[k]
    store(gc_ref, gc_hbm)
    got(rt_all.at[many], rtr)
    gr_ref[...] = jnp.sum(rt_all[...], axis=0)[:, 0:8]
    store(gr_ref, gr_hbm)

    got(tfin.at[0, lo_rows], r1r.at[6])
    got(tfin.at[1, hi_rows], r1r.at[7])
    got(tfin.at[0, hi_rows], r2r.at[2])
    got(tfin.at[1, lo_rows], r2r.at[3])
    gw_ref[...] = jnp.transpose(mine_w + tfin[0].astype(F32) + tfin[1].astype(F32))
    store(gw_ref, gw_hbm)
    got(ball.at[seven], k2r)
    for k in range(8):
        gb_ref[32 * k : 32 * k + 32, :] = ball[k].astype(F32)
    store(gb_ref, gb_hbm)

    def left(ref, sem):
        copy(ref, ref, sem, sem, partner).wait_send()

    for d in sent:
        d.wait_send()
    for d in stored:
        d.wait()
    for ref, sem in [
        (gg_all, ggs), (rt_all, rts),
    ]:
        left(ref.at[many], sem)
    for ref, sem in [(dec_all, des), (st_recv, a1s), (st_recv, a2s), (ad_recv, b1s), (ad_recv, b2s)]:
        left(ref.at[few], sem)
    for ref, sem in [(sq_all, sqs), (cr_all, crs), (crecv, c1s), (call_, c2s), (brecv, k1s), (ball, k2s)]:
        left(ref.at[seven], sem)


def hand_over(*refs):
    took = [pltpu.make_async_copy(refs[i], refs[16 + i], refs[24].at[i]) for i in range(8)]
    gave = [pltpu.make_async_copy(refs[16 + i], refs[8 + i], refs[24].at[8 + i]) for i in range(8)]
    for one in took:
        one.start()
    for one, other in zip(took, gave):
        one.wait()
        other.start()
    for one in gave:
        one.wait()


def on_device(
    inputs, gates, b_proj, c_proj, step_size, decay_rate, norm_gain, out_weight, grad_out
):
    V = pltpu.VMEM
    dma, reg = pltpu.SemaphoreType.DMA, pltpu.SemaphoreType.REGULAR
    scratch = [
        V((256, 512), BF), V((256, 512), BF), V((256, 128), F32), V((256, 128), F32),
        V((8, 256), F32), V((1, 8), F32), V((1, 512), F32), V((128, 512), F32), dma((8,)),
        V((256, 512), BF), V((256, 512), BF), V((256, 128), BF), V((256, 128), BF),
        V((8, 256), F32), V((1, 8), F32), V((1, 512), F32), V((128, 512), BF), V((256, 512), BF),
        V((8, 256, 512), BF), V((2, 4, 4, 128, 512), BF),
        V((1, 1, 512), F32), V((16, 1, 512), F32), V((1, 1, 512), F32), V((1, 1, 512), F32),
        V((128, 512), F32), V((16, 8, 256), F32), V((16, 8, 256), F32), V((128, 512), F32),
        V((128, 256), F32), V((128, 256), F32), V((128, 256), F32), V((128, 256), F32),
        V((128, 512), F32), V((16, 8, 256), F32), V((16, 8, 256), F32), V((128, 512), F32),
        V((128, 256), F32), V((128, 256), F32), V((128, 256), F32), V((128, 256), F32),
        V((1, 1, 256), F32), V((8, 1, 256), F32), V((1, 1, 256), F32), V((8, 1, 256), F32),
        V((4, 4, 512, 128), F32), V((4, 4, 512, 128), BF), V((4, 4, 512, 128), BF),
        V((4, 512, 128), BF), V((4, 512, 128), BF), V((4, 512, 128), BF),
        V((2, 512, 128), BF), V((2, 512, 128), BF), V((2, 4, 512, 128), BF),
        V((2, 256, 128), F32), V((512, 128), BF), V((512, 128), BF), V((512, 128), BF),
        V((256, 128), BF), V((256, 128), BF), V((2, 512, 128), BF),
        V((8, 32, 128), F32), V((8, 32, 128), F32), V((32, 128), F32), V((8, 32, 128), F32),
        V((8, 32, 128), BF), V((8, 32, 128), BF), V((32, 128), BF), V((8, 32, 128), BF),
        V((1, 1, 512), F32), V((32, 1, 512), F32), V((1, 1, 128), F32), V((32, 1, 128), F32),
        V((8, 128), F32), V((8, 256), F32), V((256, 128), F32), V((256, 128), F32),
        V((256, 512), F32), V((256, 512), F32), V((512, 512), BF),
        V((256, 256), F32), V((256, 256), F32),
        V((2, 128, 512), BF), V((2, 128, 1024), BF),
        V((256, 512), F32), V((256, 512), F32), V((256, 512), F32),
        V((256, 512), F32), V((256, 512), F32), V((256, 512), F32),
        V((256, 512), BF), V((512, 256), BF),
        V((256, 512), BF), V((256, 512), BF), V((512, 512), BF), V((256, 1024), BF),
        V((256, 128), F32), V((256, 256), F32), V((256, 128), F32), V((8, 256), F32),
        V((256, 512), F32), V((2, 256, 512), BF), V((256, 1024), F32),
        reg, reg, reg, reg, reg, reg, reg, dma((9,)), dma((5,)), dma((5,)), dma((2, 4, 2)), dma((2, 4, 2)), dma((4,)), dma((4,)), dma((2, 5)), dma((2, 5)),
        dma((2, 4)), dma((2, 4)), dma((7,)), dma((7,)),
        dma, dma, dma, dma, dma, dma, dma, dma, dma, dma, dma, dma, dma, dma,
        dma((4,)), dma((4,)), dma((8,)), dma((8,)), dma((4,)), dma((4,)),
        dma, dma, dma, dma, dma, dma, dma, dma, dma, dma, dma, dma,
    ]
    outs = (
        jax.ShapeDtypeStruct((256, 512), BF),
        jax.ShapeDtypeStruct((256, 512), BF),
        jax.ShapeDtypeStruct((256, 128), F32),
        jax.ShapeDtypeStruct((256, 128), F32),
        jax.ShapeDtypeStruct((8, 256), F32),
        jax.ShapeDtypeStruct((1, 8), F32),
        jax.ShapeDtypeStruct((1, 512), F32),
        jax.ShapeDtypeStruct((128, 512), F32),
    )
    far = pl.BlockSpec(memory_space=pltpu.HBM)
    results = pl.pallas_call(
        kernel,
        out_shape=outs,
        in_specs=[far] * 9,
        out_specs=[far] * 8,
        scratch_shapes=scratch,
        compiler_params=pltpu.CompilerParams(
            collective_id=0, has_side_effects=True, vmem_limit_bytes=60000000
        ),
    )(
        inputs, gates, b_proj, c_proj, step_size, decay_rate.reshape(1, 8),
        norm_gain.reshape(1, 512), out_weight, grad_out,
    )
    gx, gz, gb, gc, gs, gr, gg, gw = pl.pallas_call(
        hand_over,
        out_shape=outs,
        in_specs=[far] * 8,
        out_specs=[far] * 8,
        scratch_shapes=[V(o.shape, o.dtype) for o in outs] + [dma((16,))],
        compiler_params=pltpu.CompilerParams(vmem_limit_bytes=60000000),
    )(*results)
    return gx, gz, gb, gc, gs, gr.reshape(8), gg.reshape(512), gw


def solution(mesh):
    split = Mesh(
        mesh.devices.reshape(4, 4, 2, mesh.shape["head"]), ("seq_0", "seq_1", "seq_2", "head")
    )
    return jax.shard_map(
        on_device,
        mesh=split,
        in_specs=(
            P(SEQ, "head"), P(SEQ, "head"), P(SEQ, None), P(SEQ, None), P("head", SEQ),
            P("head"), P("head"), P(SEQ, "head"), P(SEQ, "head"),
        ),
        out_specs=(
            P(SEQ, "head"), P(SEQ, "head"), P(SEQ, None), P(SEQ, None), P("head", SEQ),
            P("head"), P("head"), P(SEQ, "head"),
        ),
        check_vma=False,
    )
```

```python
import jax
import jax.numpy as jnp
from jax import lax
from jax.experimental import pallas as pl
from jax.experimental.pallas import tpu as pltpu
from jax.sharding import Mesh
from jax.sharding import PartitionSpec as P

SEQ = ("seq_0", "seq_1", "seq_2")
EPSILON = 1e-05
MESH = pl.DeviceIdType.MESH
BF = jnp.bfloat16
F32 = jnp.float32


def mm(a, b):
    return jnp.dot(a, b, preferred_element_type=F32)


def nt(a, b):
    return lax.dot_general(a, b, (((1,), (1,)), ((), ())), preferred_element_type=F32)


def split2(v):
    hi = v.astype(BF)
    return hi, (v - hi.astype(F32)).astype(BF)


def split3(v):
    hi = v.astype(BF)
    rest = v - hi.astype(F32)
    mid = rest.astype(BF)
    return hi, mid, (rest - mid.astype(F32)).astype(BF)


def lanes(*parts):
    return jnp.concatenate(parts, axis=1)


def rows(*parts):
    return jnp.concatenate(parts, axis=0)


ORDER = (2, 1, 3, 0)


def kernel(
    x_hbm, z_hbm, b_hbm, c_hbm, step_hbm, rate_hbm, gain_hbm, w_hbm, g_hbm,
    gx_hbm, gz_hbm, gb_hbm, gc_hbm, gs_hbm, gr_hbm, gg_hbm, gw_hbm,
    gx_ref, gz_ref, gb_ref, gc_ref, gs_ref, gr_ref, gg_ref, gw_ref, outs,
    x_ref, z_ref, b_ref, c_ref, step_ref, rate_ref, gain_ref, w_ref, g_ref,
    gfull, wbuf, dec_src, dec_all, dec_par, dec_two, st_send, st_recv, st_pref, st_in,
    st_other, st_pair, st_half, st_give,
    ad_send, ad_recv, ad_pref, ad_in, ad_other, ad_pair, ad_half, ad_give, sq_src, sq_all, cr_src, cr_all,
    pt_own, pt_send, pt_recv, rs_o, rs_p, rs_m, buf_p, buf_m, fin,
    tot, t_o, t_p, t_m, tbuf_p, tbuf_m, tfin,
    cpart, crecv, csum, call_, bpart, brecv, bsum, ball,
    gg_src, gg_all, rt_src, rt_all,
    rate_c, lg, lgt, stept, fr, stl, xs2, sc, sct, mix_t, mix_b, ybuf, ycs, gn,
    ubuf, silb, ydb, nb, ntr, ehi, elo, ef2, rprod, colst, ws, qcol, rowp, gxi, mixw, pprod,
    kx, ky, kyy, kc, kz1, kz2, kz3, ins, prs, prr, zs, zr, w1s, w1r, w2s, w2r, wfs, wfr, wds, wdr, des, der, a1s, a1r, a2s, a2r,
    b1s, b1r, b2s, b2r, sqs, sqr, crs, crr, d0s, d0r, r1s, r1r, r2s, r2r,
    c1s, c1r, c2s, c2r, k1s, k1r, k2s, k2r, ggs, ggr, rts, rtr,
):
    y = lax.axis_index("seq_0")
    x = lax.axis_index("seq_1")
    c = lax.axis_index("seq_2")
    z = lax.axis_index("head")
    me = (y * 4 + x) * 2 + c
    oc = 1 - c
    q = x * oc + y * c
    p = y * oc + x * c
    rem, div = lax.rem, lax.div

    def at_head(k):
        return (y, x, c, k)

    def first(d):
        return (rem(y + d * c, 4), rem(x + d * oc, 4), c, z)

    def second(d):
        return (rem(y + d * oc, 4), rem(x + d * c, 4), c, z)

    partner = (y, x, oc, z)

    def copy(src, dst, ssem, rsem, dev):
        return pltpu.make_async_remote_copy(
            src_ref=src, dst_ref=dst, send_sem=ssem, recv_sem=rsem,
            device_id=dev, device_id_type=MESH,
        )

    def got(ref, sem):
        copy(ref, ref, sem, sem, partner).wait_recv()

    sent, stored = [], []

    def store(src, dst):
        one = pltpu.make_async_copy(src, dst, outs.at[len(stored)])
        one.start()
        stored.append(one)

    def send(src, dst, ssem, rsem, dev):
        d = copy(src, dst, ssem, rsem, dev)
        d.start()
        sent.append(d)

    far_first = sorted(
        ((dy, dx, dc) for dy in range(4) for dx in range(4) for dc in range(2)),
        key=lambda o: -(min(o[0], 4 - o[0]) + min(o[1], 4 - o[1])) - 0.1 * o[2],
    )
    ys, xs, cs = [rem(y + d, 4) for d in range(4)], [rem(x + d, 4) for d in range(4)], (c, oc)
    peers = [
        ((ys[dy], xs[dx], cs[dc], z), (ys[dy] * 4 + xs[dx]) * 2 + cs[dc])
        for dy, dx, dc in far_first
        if (dy, dx, dc) != (0, 0, 0)
    ]

    chips = [
        ((ys[dy], xs[dx], c, z), ys[dy] * 4 + xs[dx])
        for dy, dx, dc in far_first
        if dc == 0 and (dy, dx) != (0, 0)
    ]
    here = y * 4 + x

    def to_chips(make):
        for dev, k in chips:
            make(dev, k).start()

    def to_seq(make):
        for dev, k in peers:
            make(dev, k).start()

    def to_head(make):
        for d in (4, 3, 5, 2, 6, 1, 7):
            make(rem(z + d, 8)).start()

    near_x = [(y, rem(x + d, 4), c, z) for d in (1, 3)]
    near_y = [(rem(y + d, 4), x, c, z) for d in (1, 3)]
    near_z = [(y, x, c, rem(z + d, 8)) for d in (1, 7)]

    def tell(sem, devices):
        for dev in devices:
            pl.semaphore_signal(sem, inc=1, device_id=dev, device_id_type=MESH)

    barrier = pltpu.get_barrier_semaphore()
    fetches = [
        pltpu.make_async_copy(src, dst, ins.at[i])
        for i, (src, dst) in enumerate((
            (g_hbm, g_ref), (w_hbm, w_ref), (step_hbm, step_ref), (rate_hbm, rate_ref),
            (b_hbm, b_ref), (x_hbm, x_ref), (c_hbm, c_ref), (gain_hbm, gain_ref), (z_hbm, z_ref),
        ))
    ]
    for f in fetches:
        f.start()
    tell(barrier, near_z + near_x + near_y + [partner])
    for f in fetches[:2]:
        f.wait()
    pl.semaphore_wait(barrier, 7)
    tell(kx, near_x)
    tell(kz1, near_z)

    qm, qp, q2 = rem(q + 3, 4), rem(q + 1, 4), rem(q + 2, 4)
    pm, pp, p2 = rem(p + 3, 4), rem(p + 1, 4), rem(p + 2, 4)
    top, low = pl.ds(0, 64), pl.ds(64, 64)
    both_z, both_4 = ((0, 1), (1, 7)), ((0, 1), (1, 3))
    for n in range(2):
        for side, d in both_z:
            k = n if side == 0 else 1 - n
            rk = pl.ds(128 * k, 128)
            send(g_ref.at[rk], gfull.at[z, rk], zs.at[side, 0, k], zr.at[side, 0, k], at_head(rem(z + d, 8)))
    for side, d in both_4:
        send(w_ref, wbuf.at[c, p, q], w1s.at[side], w1r.at[side], first(d))
    for side, d in both_4:
        send(w_ref, wbuf.at[c, p, q], w2s.at[side, 0], w2r.at[side, 0], second(d))
    gfull[z] = g_ref[...]
    wbuf[c, p, q] = w_ref[...]

    for f in fetches[2:5]:
        f.wait()

    i8 = lax.broadcasted_iota(jnp.int32, (8, 8), 0)
    j8 = lax.broadcasted_iota(jnp.int32, (8, 8), 1)
    rate = jnp.sum(jnp.where(i8 == j8, jnp.broadcast_to(rate_ref[...], (8, 8)), 0.0), axis=1, keepdims=True)
    rate_c[...] = jnp.broadcast_to(rate, (8, 128))
    step = step_ref[...]
    ia = lax.broadcasted_iota(jnp.int32, (256, 256), 0)
    ib = lax.broadcasted_iota(jnp.int32, (256, 256), 1)
    tri_u = jnp.where(ia <= ib, 1.0, 0.0).astype(BF)
    v1, v2, v3 = split3(rate * step)
    logs = -(mm(v1, tri_u) + mm(v2, tri_u) + mm(v3, tri_u))
    lg[...] = logs
    logs_t = jnp.transpose(logs)
    step_t = jnp.transpose(step)
    lgt[:, 0:8] = logs_t
    stept[:, 0:8] = step_t
    e8 = jnp.where(
        lax.broadcasted_iota(jnp.int32, (8, 512), 0)
        == lax.broadcasted_iota(jnp.int32, (8, 512), 1) // 64, 1.0, 0.0,
    ).astype(BF)

    def spread_heads(v):
        a1, a2, a3 = split3(v)
        return mm(a1, e8) + mm(a2, e8) + mm(a3, e8)

    fr[...] = spread_heads(jnp.exp(logs_t))
    stl[...] = spread_heads(step_t * jnp.exp(logs_t[255:256, :] - logs_t))
    dec_src[0] = fr[255:256, :]
    bt = b_ref[...].T
    fetches[5].wait()
    pl.semaphore_wait(kx, 2)
    tell(ky, near_y)
    for r in range(4):
        rs = slice(64 * r, 64 * r + 64)
        hi, lo = split2(x_ref[rs, :].astype(F32) * stl[rs, :])
        xs2[rs, :] = hi
        xs2[64 * r + 256 : 64 * r + 320, :] = lo
    st_send[...] = mm(lanes(bt, bt), xs2[...])
    for f in fetches[6:]:
        f.wait()

    hc = pl.ds(pl.multiple_of(256 * c, 256), 256)
    ho = pl.ds(pl.multiple_of(256 * oc, 256), 256)

    def eight(ref, k):
        return ref.at[pl.ds(pl.multiple_of(8 * k, 8), 8)]

    send(dec_src.at[0], dec_par.at[0], prs.at[4], prr.at[4], partner)
    send(st_send.at[:, ho], st_other, prs.at[0], prr.at[0], partner)
    iota_i = lax.broadcasted_iota(jnp.int32, (64, 256), 0)
    iota_j = lax.broadcasted_iota(jnp.int32, (64, 256), 1)
    ct = c_ref[...].T
    raw = mm(c_ref[...], bt)
    for r in range(4):
        rs = slice(64 * r, 64 * r + 64)
        sc[rs, :] = jnp.where(iota_i + 64 * r >= iota_j, raw[rs, :], 0.0)
    sct[...] = mm(b_ref[...], ct)

    got(wbuf.at[c, p, qm], w1r.at[0])
    send(wbuf.at[c, p, qm, top], wbuf.at[c, p, qm, top], w1s.at[2], w1r.at[2], first(1))
    for side, d in both_4:
        send(wbuf.at[c, p, qm], wbuf.at[c, p, qm], w2s.at[side, 1], w2r.at[side, 1], second(d))
    got(wbuf.at[c, p, qp], w1r.at[1])
    send(wbuf.at[c, p, qp, low], wbuf.at[c, p, qp, low], w1s.at[3], w1r.at[3], first(3))
    for side, d in both_4:
        send(wbuf.at[c, p, qp], wbuf.at[c, p, qp], w2s.at[side, 2], w2r.at[side, 2], second(d))

    pl.semaphore_wait(ky, 2)
    tell(kyy, near_y)
    got(dec_par.at[0], prr.at[4])
    d_own, d_par = dec_src[0, :, hc], dec_par[0, :, hc]
    d_0, d_1 = jnp.where(c == 0, d_own, d_par), jnp.where(c == 0, d_par, d_own)
    got(st_other, prr.at[0])
    own, other = st_send[:, hc], st_other[...]
    l_0, l_1 = jnp.where(c == 0, own, other), jnp.where(c == 0, other, own)
    st_pair[...] = l_1 + d_1 * l_0
    dec_two[0] = dec_src[0] * dec_par[0]
    dec_all[here] = dec_two[0]
    pl.semaphore_wait(kyy, 2)
    tell(kc, [partner])
    to_chips(lambda dev, k: copy(dec_two.at[0], dec_all.at[here], des, der, dev))
    to_chips(lambda dev, k: copy(eight(st_pair, k), st_recv.at[here], a1s, a1r, dev))
    st_recv[here] = eight(st_pair, here)[...]

    half = lax.broadcasted_iota(jnp.int32, (1, 128), 1)
    keep = (
        jnp.where(half < 64, 1.0, 0.0).astype(BF),
        jnp.where(half < 64, 0.0, 1.0).astype(BF),
    )

    def inside(hp):
        ls = slice(128 * hp, 128 * hp + 128)
        mt, mb = mix_t.at[hp % 2], mix_b.at[hp % 2]
        xp = x_ref[:, ls]
        x0, x1 = xp * keep[0], xp * keep[1]
        for k in range(2):
            h = 2 * hp + k
            for r in range(4):
                rs = slice(64 * r, 64 * r + 64)
                wd = 128 if r < 2 else 256
                t = jnp.exp(jnp.minimum(lgt[rs, h : h + 1] - lg[h : h + 1, 0:wd], 0.0))
                hi, lo = split2(t * (sc[rs, 0:wd] * step_ref[h : h + 1, 0:wd]))
                dst = mt if r < 2 else mb
                rr = slice(64 * (r % 2), 64 * (r % 2) + 64)
                dst[rr, 2 * k * wd : (2 * k + 1) * wd] = hi
                dst[rr, (2 * k + 1) * wd : (2 * k + 2) * wd] = lo
        ybuf[0:128, ls] = mm(mt[...], rows(x0[0:128], x0[0:128], x1[0:128], x1[0:128]))
        ybuf[128:256, ls] = mm(mb[...], rows(x0, x0, x1, x1))

    def z_block(side, j):
        return rem(z + 8 - j, 8) if side == 0 else rem(z + j, 8)

    def z_forward(j, n):
        for side, d in both_z:
            k = n if side == 0 else 1 - n
            blk = gfull.at[z_block(side, j), pl.ds(128 * k, 128)]
            got(blk, zr.at[side, j - 1, k])
            if j < 3 or n == 0:
                send(blk, blk, zs.at[side, j, k], zr.at[side, j, k], at_head(rem(z + d, 8)))

    spots = (q, qm, qp, q2, q2)

    def w_forward(slot):
        for side, row in ((0, pm), (1, pp)):
            if slot < 3:
                blk = wbuf.at[c, row, spots[slot]]
                part = blk.at[top if side == 0 else low]
                on = True
            else:
                blk = part = wbuf.at[c, row, q2, top if slot == 3 else low]
                on = slot == 3 + side
            got(blk, w2r.at[side, slot])
            if on:
                n = min(slot, 3)
                send(part, part, wfs.at[side, n], wfr.at[side, n], second(1 if side == 0 else 3))

    def w_second_of_opposite():
        for n, piece in ((0, top), (1, low)):
            blk = wbuf.at[c, p, q2, piece]
            got(blk, w1r.at[2 + n])
            for side, d in both_4:
                send(blk, blk, w2s.at[side, 3 + n], w2r.at[side, 3 + n], second(d))

    def to_partner(n, i2):
        send(wbuf.at[c, i2], wbuf.at[c, i2], wds.at[n], wdr.at[n], partner)

    def scan(recv, pref, back):
        s = jnp.zeros((8, 256), F32)
        for k in reversed(range(16)) if back else range(16):
            pref[k] = s
            s = s * dec_all[k, :, hc] + recv[k]

    many, few = pl.ds(0, 31), pl.ds(0, 15)

    inside(0)
    w_forward(0)
    pl.semaphore_wait(kz1, 2)
    tell(kz2, near_z)
    z_forward(1, 0)
    w_second_of_opposite()
    to_partner(0, p)
    inside(1)
    z_forward(1, 1)
    got(dec_all.at[few], der)
    got(st_recv.at[few], a1r)
    scan(st_recv, st_pref, False)
    to_chips(lambda dev, k: copy(st_pref.at[k], eight(st_half, here), a2s, a2r, dev))
    eight(st_half, here)[...] = st_pref[here]
    w_forward(1)
    w_forward(2)
    inside(2)
    pl.semaphore_wait(kz2, 2)
    tell(kz3, near_z)
    z_forward(2, 0)
    w_forward(3)
    w_forward(4)
    to_partner(1, pm)
    to_partner(2, pp)
    inside(3)
    z_forward(2, 1)
    z_forward(3, 0)
    for n in range(4):
        i1 = (q, qm, qp, q2)[n]
        got(wbuf.at[c, p2, i1, top], wfr.at[0, n])
        got(wbuf.at[c, p2, i1, low], wfr.at[1, n])
        blk = wbuf.at[c, p2, i1]
        send(blk, blk, wds.at[3 + n], wdr.at[3 + n], partner)

    got(st_recv.at[few], a2r)
    enter = st_half[...]
    later = d_0 * enter + jnp.where(c == 0, st_send[:, hc], st_other[...])
    st_give[...] = jnp.where(c == 0, later, enter)
    send(st_give, st_in.at[:, hc], prs.at[1], prr.at[1], partner)
    st_in[:, hc] = jnp.where(c == 0, enter, later)
    got(st_in.at[:, ho], prr.at[1])
    s_hi, s_lo = split2(st_in[...])
    cc = lanes(c_ref[...], c_ref[...])
    gain = gain_ref[...]

    def folded(v):
        return v[:, 0:128] + v[:, 128:256] + v[:, 256:384] + v[:, 384:512]

    for r in range(4):
        rs = slice(64 * r, 64 * r + 64)
        v = fr[rs, :] * mm(cc[rs, :], rows(s_hi, s_lo))
        ycs[rs, :] = v
        ybuf[rs, :] = ybuf[rs, :] + v
    for r in range(8):
        rs = slice(32 * r, 32 * r + 32)
        zf = z_ref[rs, :].astype(F32)
        yv = ybuf[rs, :]
        s = 1.0 / (1.0 + jnp.exp(-zf))
        sil = zf * s
        u = yv * sil
        ubuf[rs, :] = u
        silb[rs, :] = sil
        ydb[rs, :] = yv * s * (1.0 + zf * (1.0 - s))
        pprod[rs, 0:128] = folded(u * u)
    sq = jnp.sum(jnp.transpose(pprod[:, 0:128]), axis=0, keepdims=True)
    sq_src[0] = sq
    sq_all[z] = sq
    pl.semaphore_wait(kz3, 2)
    to_head(lambda k: copy(sq_src.at[0], sq_all.at[z], sqs, sqr, at_head(k)))

    z_forward(3, 1)
    for n in range(3):
        got(wbuf.at[oc, p], wdr.at[n])
    for n in range(4):
        got(wbuf.at[oc, p, q], wdr.at[3 + n])

    gn[...] = jnp.zeros((256, 512), F32)

    def add_block(h):
        yy, xx = div(h, 2), 2 * rem(h, 2)
        rhs = rows(wbuf[0, yy, xx], wbuf[1, xx, yy], wbuf[0, yy, xx + 1], wbuf[1, xx + 1, yy])
        gn[...] = gn[...] + mm(gfull[h], rhs)

    def one_block(d, carry):
        add_block(rem(z + 5 + d, 8))
        return carry

    lax.fori_loop(0, 7, one_block, 0)
    for side in range(2):
        got(gfull.at[z_block(side, 4), pl.ds(128 * side, 128)], zr.at[side, 3, side])
    add_block(rem(z + 4, 8))
    for r in range(8):
        rs = slice(32 * r, 32 * r + 32)
        pprod[rs, 128:256] = folded(gn[rs, :] * gain * ubuf[rs, :])
    cr = jnp.sum(jnp.transpose(pprod[:, 128:256]), axis=0, keepdims=True)
    cr_src[0] = cr
    cr_all[z] = cr
    to_head(lambda k: copy(cr_src.at[0], cr_all.at[z], crs, crr, at_head(k)))

    seven = pl.ds(0, 7)
    got(sq_all.at[seven], sqr)
    inv_row = lax.rsqrt(jnp.sum(sq_all[...], axis=0) / 4096.0 + EPSILON)
    zero7 = jnp.zeros((7, 256), F32)
    colst[:, 0:8] = jnp.transpose(rows(inv_row, zero7))
    gg_acc = jnp.zeros((8, 512), F32)
    for r in range(8):
        rs = slice(32 * r, 32 * r + 32)
        ui = ubuf[rs, :] * colst[rs, 0:1]
        nb[rs, :] = (ui * gain).astype(BF)
        gg_acc = gg_acc + jnp.sum((gn[rs, :] * ui).reshape(4, 8, 512), axis=0)
    ntr[...] = nb[...].T

    for n in range(4):
        i2 = rem(q + ORDER[n], 4)

        def one_chip(i1, carry, i2=i2):
            yy, xx = i2 * c + i1 * oc, i1 * c + i2 * oc
            blk = 2 * yy + div(xx, 2)
            base = rem(xx, 2) * 256
            mine = gfull[blk, :, pl.ds(pl.multiple_of(base + 128 * c, 128), 128)]
            other = gfull[blk, :, pl.ds(pl.multiple_of(base + 128 * oc, 128), 128)]
            both = mm(ntr[...], lanes(mine, other))
            pt_own[yy * oc + xx * c, xx * oc + yy * c] = both[:, 0:128]
            pt_send[i2, i1] = both[:, 128:256].astype(BF)
            return carry

        lax.fori_loop(0, 4, one_chip, 0)
        send(pt_send.at[i2], pt_recv.at[i2], d0s.at[n], d0r.at[n], partner)

    gg_src[0] = jnp.sum(gg_acc, axis=0, keepdims=True)
    gg_all[me] = gg_src[0]
    ab, cd = pl.ds(0, 2), pl.ds(2, 2)
    got(pt_recv.at[p2], d0r.at[0])
    for i in range(4):
        rs_o[i] = (pt_own[p2, i] + pt_recv[p2, i].astype(F32)).astype(BF)
    send(rs_o.at[ab], buf_p, r1s.at[0], r1r.at[0], second(1))
    send(rs_o.at[cd], buf_m, r1s.at[1], r1r.at[1], second(3))

    got(cr_all.at[seven], crr)
    coef_row = inv_row * inv_row * (jnp.sum(cr_all[...], axis=0) / 4096.0)
    colst[:, 8:16] = jnp.transpose(rows(coef_row, zero7))
    for r in range(8):
        rs = slice(32 * r, 32 * r + 32)
        gu = colst[rs, 0:1] * (gn[rs, :] * gain - ubuf[rs, :] * colst[rs, 8:9])
        gz_ref[rs, :] = (gu * ydb[rs, :]).astype(BF)
        e = gu * silb[rs, :]
        hi, lo = split2(e)
        ehi[rs, :] = hi
        elo[rs, :] = lo
        hi, lo = split2(e * fr[rs, :])
        ef2[rs, :] = hi
        ef2[256 + 32 * r : 288 + 32 * r, :] = lo
        hi, lo = split2(e * ycs[rs, :])
        rprod[rs, 0:512] = hi
        rprod[rs, 512:1024] = lo
    ad_send[...] = mm(lanes(ct, ct), ef2[...])
    send(ad_send.at[:, ho], ad_other, prs.at[2], prr.at[2], partner)
    store(gz_ref, gz_hbm)
    got(pt_recv.at[pp], d0r.at[1])
    for i in range(4):
        v = pt_own[pp, i] + pt_recv[pp, i].astype(F32)
        if i < 2:
            pt_own[pp, i] = v
        else:
            rs_p[i] = v.astype(BF)
    got(pt_recv.at[pm], d0r.at[2])
    for i in range(4):
        v = pt_own[pm, i] + pt_recv[pm, i].astype(F32)
        if i < 2:
            rs_m[i] = v.astype(BF)
        else:
            pt_own[pm, i] = v
    got(ad_other, prr.at[2])
    own, other = ad_send[:, hc], ad_other[...]
    ad_pair[...] = jnp.where(c == 0, own, other) + d_0 * jnp.where(c == 0, other, own)
    to_chips(lambda dev, k: copy(eight(ad_pair, k), ad_recv.at[here], b1s, b1r, dev))
    ad_recv[here] = eight(ad_pair, here)[...]
    pl.semaphore_wait(kc, 1)
    to_seq(lambda dev, k: copy(gg_src.at[0], gg_all.at[me], ggs, ggr, dev))
    send(rs_p.at[cd], fin.at[0, cd], r1s.at[2], r1r.at[2], second(1))
    send(rs_m.at[ab], fin.at[1, ab], r1s.at[3], r1r.at[3], second(3))

    mask_t = (iota_j >= iota_i, iota_j >= iota_i + 64)
    mask_b = (iota_j[:, 0:128] >= iota_i[:, 0:128], iota_j[:, 0:128] >= iota_i[:, 0:128] + 64)

    def inside_back(hp):
        ls = slice(128 * hp, 128 * hp + 128)
        mw = mixw.at[hp % 2]
        xp = x_ref[:, ls]
        eh, el = ehi[:, ls], elo[:, ls]
        e2 = lanes(eh, el)
        for k in range(2):
            h = 2 * hp + k
            xk = xp * keep[k]
            x2 = lanes(xk, xk)
            inner_t = nt(x2[0:128], e2)
            inner_b = nt(x2[128:256], e2[128:256])
            racc_l = jnp.zeros((1, 128), F32)
            racc_r = jnp.zeros((1, 128), F32)
            for r in range(4):
                rs = slice(64 * r, 64 * r + 64)
                rr = slice(64 * (r % 2), 64 * (r % 2) + 64)
                cs = slice(0, 256) if r < 2 else slice(128, 256)
                t = jnp.exp(jnp.minimum(lg[h : h + 1, cs] - lgt[rs, h : h + 1], 0.0))
                tab = jnp.where(mask_t[r] if r < 2 else mask_b[r - 2], t, 0.0)
                inner = inner_t[rr] if r < 2 else inner_b[rr]
                st = sct[rs, cs]
                sj = stept[rs, h : h + 1]
                w = tab * inner
                sw = w * sj
                if r < 2:
                    mw[rr, 256 * k : 256 * k + 256] = (tab * st * sj).astype(BF)
                else:
                    mw[128 + 64 * (r - 2) : 192 + 64 * (r - 2), 128 * k : 128 * k + 128] = (tab * st * sj).astype(BF)
                qcol[rs, h : h + 1] = jnp.sum(w * st, axis=1, keepdims=True)
                if h == 0:
                    ws[rs, cs] = sw
                else:
                    ws[rs, cs] = ws[rs, cs] + sw
                rsum = jnp.sum(sw * st, axis=0, keepdims=True)
                if r < 2:
                    racc_l = racc_l + rsum[:, 0:128]
                    racc_r = racc_r + rsum[:, 128:256]
                else:
                    racc_r = racc_r + rsum
            rowp[h : h + 1, 0:128] = racc_l
            rowp[h : h + 1, 128:256] = racc_r
        em0, em1 = lanes(eh * keep[0], el * keep[0]), lanes(eh * keep[1], el * keep[1])
        v = mm(mw[0:128, :], rows(em0, em1))
        gxi[0:128, ls] = v[:, 0:128] + v[:, 128:256]
        v = mm(mw[128:256, 0:256], rows(em0[128:256], em1[128:256]))
        gxi[128:256, ls] = v[:, 0:128] + v[:, 128:256]

    for hp in range(4):
        inside_back(hp)

    ws[128:256, 0:128] = jnp.zeros((128, 128), F32)
    w_hi, w_lo = split2(jnp.transpose(ws[...]))
    gq = mm(lanes(w_hi, w_lo), rows(b_ref[...], b_ref[...]))
    gq = gq + nt(lanes(ef2[0:256], ef2[256:512], ef2[0:256]), lanes(s_hi, s_hi, s_lo))
    for k in range(8):
        cpart[k] = gq[32 * k : 32 * k + 32]
    crecv[z] = cpart[z]
    to_head(lambda k: copy(cpart.at[k], crecv.at[z], c1s, c1r, at_head(k)))
    w_hi, w_lo = split2(ws[...])
    gk = mm(lanes(w_hi, w_lo), rows(c_ref[...], c_ref[...]))

    got(ad_recv.at[few], b1r)
    scan(ad_recv, ad_pref, True)
    to_chips(lambda dev, k: copy(ad_pref.at[k], eight(ad_half, here), b2s, b2r, dev))
    eight(ad_half, here)[...] = ad_pref[here]

    got(buf_p, r1r.at[0])
    for i in range(2):
        rs_p[i] = (pt_own[pp, i] + buf_p[i].astype(F32)).astype(BF)
    send(rs_p.at[ab], fin.at[0, ab], r2s.at[0], r2r.at[0], second(1))
    got(buf_m, r1r.at[1])
    for i in range(2):
        rs_m[2 + i] = (pt_own[pm, 2 + i] + buf_m[i].astype(F32)).astype(BF)
    send(rs_m.at[cd], fin.at[1, cd], r2s.at[1], r2r.at[1], second(3))

    got(pt_recv.at[p], d0r.at[3])
    for i in range(4):
        pt_own[p, i] = pt_own[p, i] + pt_recv[p, i].astype(F32)
    e16 = lanes(e8, e8)
    rstate = nt(e16, rprod[...])

    got(ad_recv.at[few], b2r)
    enter = ad_half[...]
    sooner = jnp.where(c == 0, ad_other[...], ad_send[:, hc]) + d_1 * enter
    ad_give[...] = jnp.where(c == 0, enter, sooner)
    send(ad_give, ad_in.at[:, hc], prs.at[3], prr.at[3], partner)
    ad_in[:, hc] = jnp.where(c == 0, sooner, enter)
    got(ad_in.at[:, ho], prr.at[3])
    a_hi, a_lo = split2(ad_in[...])
    gk = gk + nt(lanes(xs2[0:256], xs2[256:512], xs2[0:256]), lanes(a_hi, a_hi, a_lo))
    for k in range(8):
        bpart[k] = gk[32 * k : 32 * k + 32].astype(BF)
    brecv[z] = bpart[z]
    to_head(lambda k: copy(bpart.at[k], brecv.at[z], k1s, k1r, at_head(k)))
    got(crecv.at[seven], c1r)
    csum[...] = jnp.sum(crecv[...], axis=0)
    call_[z] = csum[...]
    to_head(lambda k: copy(csum, call_.at[z], c2s, c2r, at_head(k)))

    for r in range(4):
        rs = slice(64 * r, 64 * r + 64)
        ka = mm(lanes(b_ref[rs, :], b_ref[rs, :]), rows(a_hi, a_lo))
        gx_ref[rs, :] = (gxi[rs, :] + stl[rs, :] * ka).astype(BF)
        hi, lo = split2(x_ref[rs, :].astype(F32) * ka)
        pprod[rs, 0:512] = hi.astype(F32)
        pprod[rs, 512:1024] = lo.astype(F32)
    carr = nt(e16, pprod[...].astype(BF))
    store(gx_ref, gx_hbm)
    held = jnp.sum((ad_in[...] * st_in[...]).reshape(16, 8, 512), axis=0)
    h_hi, h_lo = split2(held)
    held8 = jnp.sum(nt(e16, lanes(h_hi, h_lo)), axis=1, keepdims=True)
    logs = lg[...]
    step = step_ref[...]
    rate = rate_c[:, 0:1]
    tail = jnp.exp(logs[:, 255:256] - logs)
    q_in = jnp.transpose(qcol[...])[0:8, :]
    tc = tail * carr
    q_terms = q_in + tc
    drive = rowp[...] + rstate - step * q_terms
    boundary = jnp.exp(logs[:, 255:256]) * held8 + jnp.sum(step * tc, axis=1, keepdims=True)
    tri_l = jnp.where(ia >= ib, 1.0, 0.0).astype(BF)
    v1, v2, v3 = split3(drive)
    log_grad = mm(v1, tri_l) + mm(v2, tri_l) + mm(v3, tri_l) + boundary
    gs_ref[...] = q_terms - rate * log_grad
    rp = -jnp.sum(step * log_grad, axis=1, keepdims=True)
    d0 = lax.broadcasted_iota(jnp.int32, (8, 128), 0)
    d1 = lax.broadcasted_iota(jnp.int32, (8, 128), 1)
    rt_src[0] = jnp.sum(jnp.where(d0 == d1, rp, 0.0), axis=0, keepdims=True)
    rt_all[me] = rt_src[0]
    to_seq(lambda dev, k: copy(rt_src.at[0], rt_all.at[me], rts, rtr, dev))
    store(gs_ref, gs_hbm)

    got(fin.at[0, cd], r1r.at[2])
    got(fin.at[1, ab], r1r.at[3])
    got(fin.at[0, ab], r2r.at[0])
    got(fin.at[1, cd], r2r.at[1])

    def total(i):
        return pt_own[p, i] + fin[0, i].astype(F32) + fin[1, i].astype(F32)

    hi_rows, lo_rows = pl.ds(0, 256), pl.ds(256, 256)
    t_o[...] = total(q2).astype(BF)
    send(t_o.at[hi_rows], tbuf_p, r1s.at[4], r1r.at[4], first(1))
    send(t_o.at[lo_rows], tbuf_m, r1s.at[5], r1r.at[5], first(3))
    v = total(qp)
    tot[0] = v[0:256]
    t_p[256:512, :] = v[256:512].astype(BF)
    send(t_p.at[lo_rows], tfin.at[0, lo_rows], r1s.at[6], r1r.at[6], first(1))
    v = total(qm)
    tot[1] = v[256:512]
    t_m[0:256, :] = v[0:256].astype(BF)
    send(t_m.at[hi_rows], tfin.at[1, hi_rows], r1s.at[7], r1r.at[7], first(3))

    got(brecv.at[seven], k1r)
    bsum[...] = jnp.sum(brecv[...].astype(F32), axis=0).astype(BF)
    ball[z] = bsum[...]
    to_head(lambda k: copy(bsum, ball.at[z], k2s, k2r, at_head(k)))

    mine_w = total(q)
    got(tbuf_p, r1r.at[4])
    t_p[0:256, :] = (tot[0] + tbuf_p[...].astype(F32)).astype(BF)
    send(t_p.at[hi_rows], tfin.at[0, hi_rows], r2s.at[2], r2r.at[2], first(1))
    got(tbuf_m, r1r.at[5])
    t_m[256:512, :] = (tot[1] + tbuf_m[...].astype(F32)).astype(BF)
    send(t_m.at[lo_rows], tfin.at[1, lo_rows], r2s.at[3], r2r.at[3], first(3))

    got(gg_all.at[many], ggr)
    gg_ref[...] = jnp.sum(gg_all[...], axis=0)
    store(gg_ref, gg_hbm)
    got(call_.at[seven], c2r)
    for k in range(8):
        gc_ref[32 * k : 32 * k + 32, :] = call_[k]
    store(gc_ref, gc_hbm)
    got(rt_all.at[many], rtr)
    gr_ref[...] = jnp.sum(rt_all[...], axis=0)[:, 0:8]
    store(gr_ref, gr_hbm)

    got(tfin.at[0, lo_rows], r1r.at[6])
    got(tfin.at[1, hi_rows], r1r.at[7])
    got(tfin.at[0, hi_rows], r2r.at[2])
    got(tfin.at[1, lo_rows], r2r.at[3])
    gw_ref[...] = jnp.transpose(mine_w + tfin[0].astype(F32) + tfin[1].astype(F32))
    store(gw_ref, gw_hbm)
    got(ball.at[seven], k2r)
    for k in range(8):
        gb_ref[32 * k : 32 * k + 32, :] = ball[k].astype(F32)
    store(gb_ref, gb_hbm)

    def left(ref, sem):
        copy(ref, ref, sem, sem, partner).wait_send()

    for d in sent:
        d.wait_send()
    for d in stored:
        d.wait()
    for ref, sem in [
        (gg_all, ggs), (rt_all, rts),
    ]:
        left(ref.at[many], sem)
    for ref, sem in [(dec_all, des), (st_recv, a1s), (st_recv, a2s), (ad_recv, b1s), (ad_recv, b2s)]:
        left(ref.at[few], sem)
    for ref, sem in [(sq_all, sqs), (cr_all, crs), (crecv, c1s), (call_, c2s), (brecv, k1s), (ball, k2s)]:
        left(ref.at[seven], sem)


def hand_over(*refs):
    took = [pltpu.make_async_copy(refs[i], refs[16 + i], refs[24].at[i]) for i in range(8)]
    gave = [pltpu.make_async_copy(refs[16 + i], refs[8 + i], refs[24].at[8 + i]) for i in range(8)]
    for one in took:
        one.start()
    for one, other in zip(took, gave):
        one.wait()
        other.start()
    for one in gave:
        one.wait()


def on_device(
    inputs, gates, b_proj, c_proj, step_size, decay_rate, norm_gain, out_weight, grad_out
):
    V = pltpu.VMEM
    dma, reg = pltpu.SemaphoreType.DMA, pltpu.SemaphoreType.REGULAR
    scratch = [
        V((256, 512), BF), V((256, 512), BF), V((256, 128), F32), V((256, 128), F32),
        V((8, 256), F32), V((1, 8), F32), V((1, 512), F32), V((128, 512), F32), dma((8,)),
        V((256, 512), BF), V((256, 512), BF), V((256, 128), BF), V((256, 128), BF),
        V((8, 256), F32), V((1, 8), F32), V((1, 512), F32), V((128, 512), BF), V((256, 512), BF),
        V((8, 256, 512), BF), V((2, 4, 4, 128, 512), BF),
        V((1, 1, 512), F32), V((16, 1, 512), F32), V((1, 1, 512), F32), V((1, 1, 512), F32),
        V((128, 512), F32), V((16, 8, 256), F32), V((16, 8, 256), F32), V((128, 512), F32),
        V((128, 256), F32), V((128, 256), F32), V((128, 256), F32), V((128, 256), F32),
        V((128, 512), F32), V((16, 8, 256), F32), V((16, 8, 256), F32), V((128, 512), F32),
        V((128, 256), F32), V((128, 256), F32), V((128, 256), F32), V((128, 256), F32),
        V((1, 1, 256), F32), V((8, 1, 256), F32), V((1, 1, 256), F32), V((8, 1, 256), F32),
        V((4, 4, 512, 128), F32), V((4, 4, 512, 128), BF), V((4, 4, 512, 128), BF),
        V((4, 512, 128), BF), V((4, 512, 128), BF), V((4, 512, 128), BF),
        V((2, 512, 128), BF), V((2, 512, 128), BF), V((2, 4, 512, 128), BF),
        V((2, 256, 128), F32), V((512, 128), BF), V((512, 128), BF), V((512, 128), BF),
        V((256, 128), BF), V((256, 128), BF), V((2, 512, 128), BF),
        V((8, 32, 128), F32), V((8, 32, 128), F32), V((32, 128), F32), V((8, 32, 128), F32),
        V((8, 32, 128), BF), V((8, 32, 128), BF), V((32, 128), BF), V((8, 32, 128), BF),
        V((1, 1, 512), F32), V((32, 1, 512), F32), V((1, 1, 128), F32), V((32, 1, 128), F32),
        V((8, 128), F32), V((8, 256), F32), V((256, 128), F32), V((256, 128), F32),
        V((256, 512), F32), V((256, 512), F32), V((512, 512), BF),
        V((256, 256), F32), V((256, 256), F32),
        V((2, 128, 512), BF), V((2, 128, 1024), BF),
        V((256, 512), F32), V((256, 512), F32), V((256, 512), F32),
        V((256, 512), F32), V((256, 512), F32), V((256, 512), F32),
        V((256, 512), BF), V((512, 256), BF),
        V((256, 512), BF), V((256, 512), BF), V((512, 512), BF), V((256, 1024), BF),
        V((256, 128), F32), V((256, 256), F32), V((256, 128), F32), V((8, 256), F32),
        V((256, 512), F32), V((2, 256, 512), BF), V((256, 1024), F32),
        reg, reg, reg, reg, reg, reg, reg, dma((9,)), dma((5,)), dma((5,)), dma((2, 4, 2)), dma((2, 4, 2)), dma((4,)), dma((4,)), dma((2, 5)), dma((2, 5)),
        dma((2, 4)), dma((2, 4)), dma((7,)), dma((7,)),
        dma, dma, dma, dma, dma, dma, dma, dma, dma, dma, dma, dma, dma, dma,
        dma((4,)), dma((4,)), dma((8,)), dma((8,)), dma((4,)), dma((4,)),
        dma, dma, dma, dma, dma, dma, dma, dma, dma, dma, dma, dma,
    ]
    outs = (
        jax.ShapeDtypeStruct((256, 512), BF),
        jax.ShapeDtypeStruct((256, 512), BF),
        jax.ShapeDtypeStruct((256, 128), F32),
        jax.ShapeDtypeStruct((256, 128), F32),
        jax.ShapeDtypeStruct((8, 256), F32),
        jax.ShapeDtypeStruct((1, 8), F32),
        jax.ShapeDtypeStruct((1, 512), F32),
        jax.ShapeDtypeStruct((128, 512), F32),
    )
    far = pl.BlockSpec(memory_space=pltpu.HBM)
    results = pl.pallas_call(
        kernel,
        out_shape=outs,
        in_specs=[far] * 9,
        out_specs=[far] * 8,
        scratch_shapes=scratch,
        compiler_params=pltpu.CompilerParams(
            collective_id=0, has_side_effects=True, vmem_limit_bytes=60000000
        ),
    )(
        inputs, gates, b_proj, c_proj, step_size, decay_rate.reshape(1, 8),
        norm_gain.reshape(1, 512), out_weight, grad_out,
    )
    gx, gz, gb, gc, gs, gr, gg, gw = pl.pallas_call(
        hand_over,
        out_shape=outs,
        in_specs=[far] * 8,
        out_specs=[far] * 8,
        scratch_shapes=[V(o.shape, o.dtype) for o in outs] + [dma((16,))],
        compiler_params=pltpu.CompilerParams(vmem_limit_bytes=60000000),
    )(*results)
    return gx, gz, gb, gc, gs, gr.reshape(8), gg.reshape(512), gw


def solution(mesh):
    split = Mesh(
        mesh.devices.reshape(4, 4, 2, mesh.shape["head"]), ("seq_0", "seq_1", "seq_2", "head")
    )
    return jax.shard_map(
        on_device,
        mesh=split,
        in_specs=(
            P(SEQ, "head"), P(SEQ, "head"), P(SEQ, None), P(SEQ, None), P("head", SEQ),
            P("head"), P("head"), P(SEQ, "head"), P(SEQ, "head"),
        ),
        out_specs=(
            P(SEQ, "head"), P(SEQ, "head"), P(SEQ, None), P(SEQ, None), P("head", SEQ),
            P("head"), P("head"), P(SEQ, "head"),
        ),
        check_vma=False,
    )
```
